32 devices in a mesh: cons: 4 (over y, x), blk: 8 (over z, core).
Axes of the slice: x: 2, y: 2, z: 4, core: 2. Of those that a mesh axis runs over, the one named last changes fastest.
Arguments:
- elevation: bfloat16 [16, 320, 6144], P('cons', 'blk'), may hold values from -6 to 6
- legendre: bfloat16 [320, 768, 768], P('blk', 'cons'), may hold values from -5 to 5, as said below
- cycle_weight: float32 [320], P('blk'), may hold values from 0.0003565902 to 0.0028527216
- love_factor: float32 [768], replicated, may hold values from 0.000390625 to 0.0052083335
- assignment: int32 [16], replicated, may hold values from 0 to 15, each once
Outputs:
- loading: float32 [16, 320, 6144], P('cons', 'blk')
The draws below stay inside these ranges and needn't reach their ends.
Inputs may be any that keep to these rules, and one draw needn't show every extreme that they name: `legendre`: fully normalized associated Legendre functions (the square integrates to 1 over [-1, 1]) of each cycle's latitude, every cycle within 26 degrees of the equator; zero where the degree is below the order.
All inputs are finite; a program needn't handle non-finite values.
Results may differ from the reference program's by a relative error of at most 0.02.
Values may be sent and summed in bfloat16 or wider, within the bound.
A program may use at most 128 MiB of HBM per device.

```python
import math
import jax
import jax.numpy as jnp
from jax import lax

FIELDS = 16
DEGREES = 768
ORDERS = 768
LONS = 6144
CYCLE_DEV = 40
CYCLES = 320
N_BLK = 8


def draw_legendre(key, part):
    cosine_vals = jax.random.uniform(jax.random.fold_in(key, 11), (CYCLES,), jnp.float32, -0.43, 0.43)
    sine_vals = jnp.sqrt(1.0 - cosine_vals * cosine_vals)
    order_vals = jnp.arange(ORDERS).astype(jnp.float32)
    growth = 0.5 * jnp.log((2.0 * order_vals + 1.0) / jnp.maximum(2.0 * order_vals, 1.0))
    log_steps = jnp.where(order_vals[None, :] > 0.0, growth[None, :] + jnp.log(sine_vals)[:, None], 0.0)
    diagonal = jnp.exp(0.5 * jnp.log(0.5) + jnp.cumsum(log_steps, axis=1))
    order_sq = order_vals[None, :] * order_vals[None, :]

    def advance(state, degree):
        previous, earlier = state
        level = degree.astype(jnp.float32)
        coef_now = jnp.sqrt((4.0 * level * level - 1.0) / jnp.maximum(level * level - order_sq, 1.0))
        lower = level - 1.0
        coef_before = jnp.sqrt(jnp.maximum(4.0 * lower * lower - 1.0, 1.0) / jnp.maximum(lower * lower - order_sq, 1.0))
        generic = coef_now * (cosine_vals[:, None] * previous - earlier / coef_before)
        first_up = jnp.sqrt(2.0 * order_vals[None, :] + 3.0) * cosine_vals[:, None] * previous
        values = jnp.where(level == order_vals[None, :], diagonal, jnp.where(level == order_vals[None, :] + 1.0, first_up, jnp.where(level > order_vals[None, :] + 1.0, generic, 0.0)))
        return ((values, previous), values)
    zeros = jnp.zeros((CYCLES, ORDERS), jnp.float32)
    _, table = lax.scan(advance, (zeros, zeros), jnp.arange(DEGREES, dtype=jnp.int32))
    return jnp.transpose(table, (1, 2, 0)).astype(jnp.bfloat16)


def level_of(own_key, dims, shards, smallest, high):
    def one(dim, shards_of):
        steps = jax.random.uniform(jax.random.fold_in(jax.random.fold_in(own_key, 6), dim), (shards_of,), jnp.float32, smallest / len(shards), high / len(shards))
        return jnp.repeat(jnp.exp(steps), dims[dim] // shards_of).reshape((-1,) + (1,) * (len(dims) - dim - 1))

    level = one(*shards[0])
    for cut in shards[1:]:
        level = level * one(*cut)
    return level


def normal_values(own_key, dims, deviation, bound, split=(), kind=jnp.bfloat16):
    entries = jax.random.normal(own_key, dims, jnp.float32) * deviation
    if len(split) > 0:
        entries = level_of(own_key, dims, split, -0.22, 0.18) * entries
    return jnp.clip(entries, min=-bound, max=bound).astype(kind)


def setup_inputs(seed: int = 0) -> dict:
    keys = jax.random.split(jax.random.key(seed), 6)
    return {
        "elevation": normal_values(keys[0], (FIELDS, CYCLES, LONS), 1.0, 6.0, ((0, 4), (1, 8))),
        "legendre": draw_legendre(jax.random.fold_in(keys[5], 71), 0),
        "cycle_weight": jnp.clip(jnp.exp(math.log(0.0028527216) - 2.0794415 * jax.random.uniform(keys[2], (CYCLES,), jnp.float32) ** level_of(keys[2], (CYCLES,), ((0, 8),), -0.2, 0.2)), 0.0003565902, 0.0028527216),
        "love_factor": jnp.clip(jnp.exp(jax.random.uniform(keys[3], (DEGREES,), jnp.float32, math.log(0.000390625), math.log(0.0052083335))), 0.000390625, 0.0052083335),
        "assignment": jax.random.permutation(keys[4], FIELDS).astype(jnp.int32),
    }


def fourier_block(offset, length, period, orders):
    lon_index = offset + jnp.arange(length, dtype=jnp.int32)
    order_index = jnp.arange(orders, dtype=jnp.int32)
    phases = (lon_index[:, None] * order_index[None, :]) % period
    angles = phases.astype(jnp.float32) * jnp.float32(2.0 * 3.141592653589793 / period)
    stacked = jnp.stack([jnp.cos(angles), -jnp.sin(angles)], axis=2)
    return stacked.reshape(length, 2 * orders).astype(jnp.bfloat16)


def reference(elevation, legendre, cycle_weight, love_factor, assignment):
    table = fourier_block(0, LONS, LONS, ORDERS)

    def forward(field):
        summed = jnp.dot(field, table, preferred_element_type=jnp.float32)
        return (summed * cycle_weight[:, None]).astype(jnp.bfloat16)

    spectra = lax.map(forward, elevation)
    ordered = spectra[assignment].reshape(FIELDS, CYCLES, ORDERS, 2)

    def add_block(running, block_index):
        start = (block_index * CYCLE_DEV).astype(jnp.int32)
        values = lax.dynamic_slice_in_dim(legendre, start, CYCLE_DEV, 0).astype(jnp.float32)
        spec_block = lax.dynamic_slice_in_dim(ordered, start, CYCLE_DEV, 1).astype(jnp.float32)
        partial_value = jnp.einsum('jml,gjmp->lpgm', values, spec_block)
        rounded = lax.optimization_barrier(partial_value.astype(jnp.bfloat16))
        return running + rounded.astype(jnp.float32), None

    zeros = jnp.zeros((DEGREES, 2, FIELDS, ORDERS), jnp.float32)
    analysis, _ = lax.scan(add_block, zeros, jnp.arange(N_BLK, dtype=jnp.int32))
    coefficients = (analysis * love_factor[:, None, None, None]).astype(jnp.bfloat16)
    order_factor = jnp.where(jnp.arange(ORDERS) == 0, 1.0, 2.0).astype(jnp.float32)

    def synth_block(block_index):
        start = (block_index * CYCLE_DEV).astype(jnp.int32)
        values = lax.dynamic_slice_in_dim(legendre, start, CYCLE_DEV, 0).astype(jnp.float32)
        summed = jnp.einsum('jml,lpgm->gjmp', values, coefficients.astype(jnp.float32))
        return (summed * order_factor[None, None, :, None]).astype(jnp.bfloat16)

    blocks = lax.map(synth_block, jnp.arange(N_BLK, dtype=jnp.int32))
    synthesis = jnp.moveaxis(blocks, 0, 1).reshape(FIELDS, CYCLES, 2 * ORDERS)

    def inverse(field):
        return jnp.dot(field, table.T, preferred_element_type=jnp.float32)

    return lax.map(inverse, synthesis)
```

```python
import functools

import jax
import jax.numpy as jnp
from jax import lax
from jax.experimental import pallas as pl
from jax.experimental.pallas import tpu as pltpu
from jax.sharding import PartitionSpec as P

GROUP = 16
LANES = 128
LEAD = 6
GAP = 3
MESH = pl.DeviceIdType.MESH


class Plan:
    def __init__(self, n_cons, n_blk, orders_dev, degrees):
        self.n_cons, self.chips = n_cons, n_blk // 2
        self.groups, self.columns = orders_dev // GROUP, degrees // LANES
        counts = [sum(self.width(c, g) for g in range(self.groups)) for c in range(n_cons)]
        self.counts = counts
        moved = [max(0, (counts[c] - counts[n_cons - 1 - c]) // 2) for c in range(n_cons)]
        self.moved = moved
        self.max_tiles = max(counts)
        self.max_moved = max(1, max(moved))
        self.queues = [counts[c] - moved[c] + moved[n_cons - 1 - c] for c in range(n_cons)]
        self.max_queue = max(self.queues)

    def first(self, c, g):
        return (c * self.groups + g) * GROUP // LANES

    def width(self, c, g):
        return self.columns - self.first(c, g)

    def starts(self, c):
        begin, out = 0, []
        for g in range(self.groups):
            out.append(begin)
            begin = begin + self.width(c, g)
        return out, begin

    def place(self, c, starts, t):
        g = 0
        for start in starts[1:]:
            g = g + jnp.where(t >= start, 1, 0)
        begin = 0
        for k in range(1, self.groups):
            begin = jnp.where(t >= starts[k], starts[k], begin)
        return g, (c * self.groups + g) * GROUP // LANES + t - begin


def pick(c, values):
    out = values[-1]
    for k in range(len(values) - 1):
        out = jnp.where(c == k, values[k], out)
    return out


def sum_kernel(plan, part, love, out, pair_in, acc, given, inward_in, cross_in, coef, *sems):
    (pair_s, pair_r, give_s, give_r, in_s, in_r, cross_s, cross_r, mid_s, out_s, coef_r, ret_s, ret_r, fin_s, fin_r) = sems
    me, c = lax.axis_index("blk"), lax.axis_index("cons")
    chips, half = plan.chips, part.shape[1] // 2
    p, core = me // 2, lax.rem(me, 2)
    mid = chips // 2
    left = p < mid
    depth = jnp.where(left, mid - 1 - p, p - mid)
    side = jnp.where(left, 0, 1)
    inner = jnp.where(left, me + 2, me - 2)
    outer = jnp.where(left, me - 2, me + 2)
    partner = me + 1 - 2 * core
    other_c = plan.n_cons - 1 - c
    last = mid - 1

    starts, tiles = plan.starts(c)
    other_starts, _ = plan.starts(other_c)
    exports, imports = pick(c, plan.moved), pick(other_c, plan.moved)
    queue = pick(c, plan.queues)

    barrier = pltpu.get_barrier_semaphore()

    def greet(where):
        pl.semaphore_signal(barrier, inc=1, device_id=where, device_id_type=MESH)

    greet({"blk": partner})

    @pl.when(p > 0)
    def _():
        greet({"blk": me - 2})

    @pl.when(p < chips - 1)
    def _():
        greet({"blk": me + 2})

    @pl.when(c != other_c)
    def _():
        greet({"cons": other_c})

    heard = 1 + jnp.where(p > 0, 1, 0) + jnp.where(p < chips - 1, 1, 0) + jnp.where(c != other_c, 1, 0)
    pl.semaphore_wait(barrier, heard)

    def copy(src, dst, send, recv, where):
        return pltpu.make_async_remote_copy(
            src_ref=src, dst_ref=dst, send_sem=send, recv_sem=recv, device_id=where, device_id_type=MESH
        )

    def rows_of(k):
        return pl.ds(pl.multiple_of(k * half, half), half)

    mine, theirs = rows_of(core), rows_of(1 - core)

    def at(ref, spot, rows):
        g, lt = spot
        return ref.at[g, rows, pl.ds(pl.multiple_of(lt * LANES, LANES), LANES)]

    def pair_copy(t, spot):
        return copy(at(part, spot, theirs), pair_in.at[t], pair_s.at[t], pair_r.at[t], {"blk": partner})

    def give_copy(e):
        return copy(given.at[e], acc.at[LEAD + e], give_s.at[e], give_r.at[e], {"cons": other_c})

    def in_copy(q):
        return copy(acc.at[q], inward_in.at[q], in_s.at[q], in_r.at[q], {"blk": inner})

    def cross_copy(q):
        h = q // 2
        return copy(acc.at[q], cross_in.at[h], cross_s.at[h], cross_r.at[h], {"blk": inner})

    def mid_copy(q):
        return copy(coef.at[q], coef.at[q], mid_s.at[q // 2], coef_r.at[q], {"blk": inner})

    def out_copy(q):
        return copy(coef.at[q], coef.at[q], out_s.at[q], coef_r.at[q], {"blk": outer})

    def ret_copy(q, e, spot):
        return copy(coef.at[q], at(out, spot, mine), ret_s.at[e], ret_r.at[e], {"cons": other_c})

    def fin_copy(t, spot):
        part_of = at(out, spot, mine)
        return copy(part_of, part_of, fin_s.at[t], fin_r.at[t], {"blk": partner})

    def loop(count, body):
        def step(i, carry):
            body(i)
            return carry

        lax.fori_loop(0, count, step, 0)

    def add(x, y):
        return x.astype(jnp.float32) + y.astype(jnp.float32)

    def is_import(q):
        return (q >= LEAD) & (q < LEAD + imports)

    def tile_of(q):
        return exports + q - jnp.where(q >= LEAD, imports, 0)

    loop(tiles, lambda t: pair_copy(t, plan.place(c, starts, t)).start())

    def clear(g):
        def one(lt):
            out[g, :, pl.ds(pl.multiple_of(lt * LANES, LANES), LANES)] = jnp.zeros((2 * half, LANES), out.dtype)

        loop((c * plan.groups + g) * GROUP // LANES, one)

    loop(plan.groups, clear)

    def give(e):
        spot = plan.place(c, starts, e)
        pair_copy(e, spot).wait_recv()
        given[e] = add(at(part, spot, mine)[...], pair_in[e]).astype(given.dtype)
        give_copy(e).start()

    loop(exports, give)

    def gather(q):
        native = jnp.logical_not(is_import(q))

        @pl.when(native)
        def _():
            t = tile_of(q)
            spot = plan.place(c, starts, t)
            pair_copy(t, spot).wait_recv()
            acc[q] = add(at(part, spot, mine)[...], pair_in[t]).astype(acc.dtype)

        @pl.when(is_import(q))
        def _():
            give_copy(q - LEAD).wait_recv()

        @pl.when(depth < last)
        def _():
            in_copy(q).wait_recv()
            acc[q] = add(acc[q], inward_in[q]).astype(acc.dtype)

        @pl.when(depth > 0)
        def _():
            in_copy(q).start()

        @pl.when((depth == 0) & (lax.rem(q, 2) != side))
        def _():
            cross_copy(q).start()

    def spread(q):
        @pl.when(depth < last)
        def _():
            out_copy(q).start()

        @pl.when(is_import(q))
        def _():
            e = q - LEAD
            ret_copy(q, e, plan.place(other_c, other_starts, e)).start()

        @pl.when(jnp.logical_not(is_import(q)))
        def _():
            t = tile_of(q)
            spot = plan.place(c, starts, t)
            at(out, spot, mine)[...] = coef[q]
            fin_copy(t, spot).start()

    def finish(q):
        @pl.when((depth == 0) & (lax.rem(q, 2) == side))
        def _():
            cross_copy(q).wait_recv()
            own = plan.place(c, starts, tile_of(q))[1]
            lent = plan.place(other_c, other_starts, q - LEAD)[1]
            lt = jnp.where(is_import(q), lent, own)
            total = add(acc[q], cross_in[q // 2]) * love[pl.ds(lt, 1), :]
            coef[q] = total.astype(coef.dtype)
            mid_copy(q).start()
            spread(q)

    def relay(q):
        @pl.when((depth > 0) | (lax.rem(q, 2) != side))
        def _():
            out_copy(q).wait_recv()
            spread(q)

    def take_back(e):
        spot = plan.place(c, starts, e)
        ret_copy(0, e, spot).wait_recv()
        fin_copy(e, spot).start()

    relay_gap = jnp.where(depth == 0, 2 * GAP, 3 * GAP + (depth - 1) * GAP)
    back_gap = LEAD + relay_gap + GAP

    def step(i):
        @pl.when(i < queue)
        def _():
            gather(i)

        q = i - GAP

        @pl.when((q >= 0) & (q < queue))
        def _():
            finish(q)

        r = i - relay_gap

        @pl.when((r >= 0) & (r < queue))
        def _():
            relay(r)

        e = i - back_gap

        @pl.when((e >= 0) & (e < exports))
        def _():
            take_back(e)

    loop(plan.max_queue + LEAD + 4 * GAP + mid * GAP, step)

    def drain_tile(t):
        spot = plan.place(c, starts, t)
        pair_copy(t, spot).wait_send()
        fin_copy(t, spot).wait_send()
        fin_copy(t, spot).wait_recv()

    loop(tiles, drain_tile)
    loop(exports, lambda e: give_copy(e).wait_send())

    def drain_queue(q):
        @pl.when(depth > 0)
        def _():
            in_copy(q).wait_send()

        @pl.when((depth == 0) & (lax.rem(q, 2) != side))
        def _():
            cross_copy(q).wait_send()

        @pl.when((depth == 0) & (lax.rem(q, 2) == side))
        def _():
            mid_copy(q).wait_send()

        @pl.when(depth < last)
        def _():
            out_copy(q).wait_send()

        @pl.when(is_import(q))
        def _():
            e = q - LEAD
            ret_copy(q, e, plan.place(other_c, other_starts, e)).wait_send()

    loop(queue, drain_queue)


def tree_sum(partial, love, n_cons, n_blk):
    orders_dev, rows, degrees = partial.shape
    plan = Plan(n_cons, n_blk, orders_dev, degrees)
    shape = (plan.groups, GROUP * rows, degrees)
    half = (GROUP * rows // 2, LANES)
    kind = partial.dtype
    tiles, queue, moved = plan.max_tiles, plan.max_queue, plan.max_moved
    halves = (queue + 1) // 2
    sems = [tiles] * 2 + [moved] * 2 + [queue] * 2 + [halves] * 2 + [halves, queue, queue] + [moved] * 2 + [tiles] * 2
    out = pl.pallas_call(
        functools.partial(sum_kernel, plan),
        out_shape=jax.ShapeDtypeStruct(shape, kind),
        in_specs=[pl.BlockSpec(memory_space=pltpu.VMEM)] * 2,
        out_specs=pl.BlockSpec(memory_space=pltpu.VMEM),
        scratch_shapes=[
            pltpu.VMEM((tiles,) + half, kind),
            pltpu.VMEM((queue,) + half, kind),
            pltpu.VMEM((moved,) + half, kind),
            pltpu.VMEM((queue,) + half, kind),
            pltpu.VMEM((halves,) + half, kind),
            pltpu.VMEM((queue,) + half, kind),
        ]
        + [pltpu.SemaphoreType.DMA((n,)) for n in sems],
        compiler_params=pltpu.CompilerParams(
            collective_id=0, has_side_effects=True, vmem_limit_bytes=56 * 2**20
        ),
    )(partial.reshape(shape), love.reshape(degrees // LANES, LANES))
    return out.reshape(partial.shape)


def angles_of(lon_index, period, orders):
    order_index = jnp.arange(orders, dtype=jnp.int32)
    phases = lon_index[:, None] * order_index[None, :] % period
    angles = phases.astype(jnp.float32) * jnp.float32(2.0 * 3.141592653589793 / period)
    return jnp.cos(angles), jnp.sin(angles)


def quarter_table(length, period, orders):
    fine = 32
    coarse = length // fine
    parts = angles_of(jnp.arange(coarse, dtype=jnp.int32) * fine, period, orders)
    parts += angles_of(jnp.arange(fine, dtype=jnp.int32), period, orders)
    cos_a, sin_a, cos_b, sin_b = lax.optimization_barrier(parts)
    cos_a, sin_a = cos_a[:, None, :], sin_a[:, None, :]
    cosine = cos_a * cos_b[None] - sin_a * sin_b[None]
    minus_sine = -(sin_a * cos_b[None] + cos_a * sin_b[None])
    both = jnp.concatenate([cosine.astype(jnp.bfloat16), minus_sine.astype(jnp.bfloat16)], axis=2)
    return both.reshape(length, 2 * orders)


def local(elevation, legendre, cycle_weight, love_factor, assignment):
    fld_dev, cycle_dev, longitudes = elevation.shape
    orders_dev, degrees = legendre.shape[1:]
    orders = orders_dev * lax.axis_size("cons")
    quarter = longitudes // 4
    table = lax.optimization_barrier(quarter_table(quarter, longitudes, orders))
    residue = jnp.arange(orders, dtype=jnp.int32) % 4
    turn_re = (residue == 0).astype(jnp.float32) - (residue == 2).astype(jnp.float32)
    turn_im = (residue == 1).astype(jnp.float32) - (residue == 3).astype(jnp.float32)
    sign = turn_re * turn_re - turn_im * turn_im

    def halves(q):
        part = lax.slice_in_dim(elevation, q * quarter, (q + 1) * quarter, axis=2)
        both = jnp.einsum("fjk,kn->fjn", part, table, preferred_element_type=jnp.float32)
        return both[..., :orders], both[..., orders:]

    (re0, im0), (re1, im1), (re2, im2), (re3, im3) = (halves(q) for q in range(4))
    even_re, even_im = re0 + sign * re2, im0 + sign * im2
    odd_re, odd_im = re1 + sign * re3, im1 + sign * im3
    running = jnp.stack(
        [
            even_re + turn_re * odd_re + turn_im * odd_im,
            even_im + turn_re * odd_im - turn_im * odd_re,
        ],
        axis=1,
    )
    spectra = (running * cycle_weight[None, None, :, None]).astype(jnp.bfloat16)
    moved = lax.all_to_all(spectra, "cons", split_axis=3, concat_axis=0, tiled=True)
    fields = moved.shape[0]
    one_hot = (assignment[:, None] == jnp.arange(fields, dtype=jnp.int32)[None, :]).astype(
        jnp.bfloat16
    )
    ordered = jnp.einsum(
        "gf,fpjm->gpjm", one_hot, moved, preferred_element_type=jnp.float32
    ).astype(jnp.bfloat16)
    slots = ordered.reshape(2 * fields, cycle_dev, orders_dev)
    partial = jnp.einsum(
        "jml,rjm->mrl", legendre, slots, preferred_element_type=jnp.float32
    ).astype(jnp.bfloat16)
    coefficients = tree_sum(partial, love_factor, lax.axis_size("cons"), lax.axis_size("blk"))
    order_index = lax.axis_index("cons") * orders_dev + jnp.arange(orders_dev, dtype=jnp.int32)
    order_factor = jnp.where(order_index == 0, 1.0, 2.0).astype(jnp.float32)
    summed = jnp.einsum(
        "jml,mrl->rjm", legendre, coefficients, preferred_element_type=jnp.float32
    )
    synthesis = (summed * order_factor).astype(jnp.bfloat16)
    synthesis = synthesis.reshape(fields, 2, cycle_dev, orders_dev)
    returned = lax.all_to_all(synthesis, "cons", split_axis=0, concat_axis=3, tiled=True)
    re, im = returned[:, 0].astype(jnp.float32), returned[:, 1].astype(jnp.float32)
    turned = [
        (re, im),
        (turn_re * re - turn_im * im, turn_re * im + turn_im * re),
        (sign * re, sign * im),
        (turn_re * re + turn_im * im, turn_re * im - turn_im * re),
    ]
    return jnp.concatenate(
        [
            jnp.einsum(
                "fjn,kn->fjk",
                jnp.concatenate(pair, axis=2).astype(jnp.bfloat16),
                table,
                preferred_element_type=jnp.float32,
            )
            for pair in turned
        ],
        axis=2,
    )


def solution(mesh):
    placed = (P("cons", "blk", None), P("blk", "cons", None), P("blk"), P(), P())
    return jax.shard_map(
        local, mesh=mesh, in_specs=placed, out_specs=P("cons", "blk", None), check_vma=False
    )
```

```python
import functools

import jax
import jax.numpy as jnp
from jax import lax
from jax.experimental import pallas as pl
from jax.experimental.pallas import tpu as pltpu
from jax.sharding import PartitionSpec as P

GROUP = 16
LANES = 128
LEAD = 6
FIN = 4
REL0 = 8
REL1 = 14
RELN = 5
BACK = 4
SLACK = 2
AHEAD = 2
PACE = 3
CHUNKS = 3
MESH = pl.DeviceIdType.MESH


class Plan:
    def __init__(self, n_cons, n_blk, orders_dev, degrees):
        self.n_cons, self.chips = n_cons, n_blk // 2
        self.groups, self.columns = orders_dev // GROUP, degrees // LANES
        counts = [sum(self.width(c, g) for g in range(self.groups)) for c in range(n_cons)]
        self.counts = counts
        moved = [max(0, (counts[c] - counts[n_cons - 1 - c]) // 2) for c in range(n_cons)]
        self.moved = moved
        self.max_tiles = max(counts)
        self.max_moved = max(1, max(moved))
        self.queues = [counts[c] - moved[c] + moved[n_cons - 1 - c] for c in range(n_cons)]
        self.max_queue = max(self.queues)

    def first(self, c, g):
        return (c * self.groups + g) * GROUP // LANES

    def width(self, c, g):
        return self.columns - self.first(c, g)

    def starts(self, c):
        begin, out = 0, []
        for g in range(self.groups):
            out.append(begin)
            begin = begin + self.width(c, g)
        return out, begin

    def place(self, c, starts, t):
        g = 0
        for start in starts[1:]:
            g = g + jnp.where(t >= start, 1, 0)
        begin = 0
        for k in range(1, self.groups):
            begin = jnp.where(t >= starts[k], starts[k], begin)
        return g, (c * self.groups + g) * GROUP // LANES + t - begin


def pick(c, values):
    out = values[-1]
    for k in range(len(values) - 1):
        out = jnp.where(c == k, values[k], out)
    return out


def swap_blocks(tiles):
    count = LANES // GROUP
    block = lax.broadcasted_iota(jnp.int32, tiles[0].shape, len(tiles[0].shape) - 1) // GROUP
    step = count // 2
    while step:
        high = (block // step) % 2 == 1
        new = list(tiles)
        for a in range(count):
            if (a // step) % 2 == 0:
                low_t, high_t = tiles[a], tiles[a + step]
                up = pltpu.roll(high_t, GROUP * step, high_t.ndim - 1)
                down = pltpu.roll(low_t, LANES - GROUP * step, low_t.ndim - 1)
                new[a] = jnp.where(high, up, low_t)
                new[a + step] = jnp.where(high, high_t, down)
        tiles = new
        step //= 2
    return tiles


def sum_kernel(
    plan, x, love, order, legendre, out, table, table_sem, part, spread_s, whole, sent, taken, back, returned,
    pair_in, acc, given, inward_in, cross_in, coef, *sems
):
    (pair_s, pair_r, give_s, give_r, in_s, in_r, cross_s, cross_r, mid_s, out_s, coef_r, ret_s, ret_r, fin_s, fin_r) = sems[:15]
    there_s, there_r, home_s, home_r = sems[15:]
    me, c = lax.axis_index("blk"), lax.axis_index("cons")
    chips, half = plan.chips, part.shape[1] // 2
    n_cons, groups = plan.n_cons, plan.groups
    cycles = x.shape[1]
    blocks = LANES // GROUP
    folds = cycles // blocks
    rows = x.shape[2]
    all_rows = n_cons * rows
    pairs = plan.columns // 2
    p, core = me // 2, lax.rem(me, 2)
    mid = chips // 2
    left = p < mid
    depth = jnp.where(left, mid - 1 - p, p - mid)
    side = jnp.where(left, 0, 1)
    inner = jnp.where(left, me + 2, me - 2)
    outer = jnp.where(left, me - 2, me + 2)
    partner = me + 1 - 2 * core
    other_c = n_cons - 1 - c
    last = mid - 1

    starts, tiles = plan.starts(c)
    other_starts, _ = plan.starts(other_c)
    exports, imports = pick(c, plan.moved), pick(other_c, plan.moved)
    queue = pick(c, plan.queues)

    barrier = pltpu.get_barrier_semaphore()

    def greet(where):
        pl.semaphore_signal(barrier, inc=1, device_id=where, device_id_type=MESH)

    greet({"blk": partner})

    @pl.when(p > 0)
    def _():
        greet({"blk": me - 2})

    @pl.when(p < chips - 1)
    def _():
        greet({"blk": me + 2})

    peers = [lax.rem(c + k, n_cons) for k in range(1, n_cons)]
    for peer in peers:
        greet({"cons": peer})

    def loop(count, body):
        def step(i, carry):
            body(i)
            return carry

        lax.fori_loop(0, count, step, 0)

    def table_copy(g):
        return pltpu.make_async_copy(
            legendre.at[:, pl.ds(pl.multiple_of(g * GROUP, GROUP), GROUP), :], table.at[g], table_sem.at[g]
        )

    loop(groups, lambda g: table_copy(g).start())

    def pack(i):
        tile, fold = i // folds, lax.rem(i, folds)
        swapped = swap_blocks([x[tile, fold * blocks + k].astype(jnp.float32) for k in range(blocks)])
        for k in range(blocks):
            sent[tile * blocks + k, fold] = swapped[k].astype(sent.dtype)

    loop(x.shape[0] * folds, pack)

    heard = n_cons + jnp.where(p > 0, 1, 0) + jnp.where(p < chips - 1, 1, 0)
    pl.semaphore_wait(barrier, heard)

    def copy(src, dst, send, recv, where):
        return pltpu.make_async_remote_copy(
            src_ref=src, dst_ref=dst, send_sem=send, recv_sem=recv, device_id=where, device_id_type=MESH
        )

    chunk = groups // CHUNKS

    def there_copy(k, h, source):
        peer = peers[k]
        return copy(
            sent.at[pl.ds(peer * groups + h * chunk, chunk)],
            taken.at[source, pl.ds(h * chunk, chunk)],
            there_s.at[k, h],
            there_r.at[source, h],
            {"cons": peer},
        )

    for h in range(CHUNKS):
        for k in range(n_cons - 1):
            there_copy(k, h, c).start()

    def keep(g):
        taken[c, g] = sent[c * groups + g]

    loop(groups, keep)

    def home_copy(k, g, source):
        return copy(
            back.at[g, peers[k]],
            returned.at[source * groups + g],
            home_s.at[k, g],
            home_r.at[source * groups + g],
            {"cons": peers[k]},
        )

    def rows_of(k):
        return pl.ds(pl.multiple_of(k * half, half), half)

    mine, theirs = rows_of(core), rows_of(1 - core)

    def at(ref, spot, rows):
        g, lt = spot
        return ref.at[g, rows, pl.ds(pl.multiple_of(lt * LANES, LANES), LANES)]

    def pair_copy(t, spot):
        return copy(at(part, spot, theirs), pair_in.at[t], pair_s.at[t], pair_r.at[t], {"blk": partner})

    def give_copy(e):
        return copy(given.at[e], acc.at[LEAD + e], give_s.at[e], give_r.at[e], {"cons": other_c})

    def in_copy(q):
        return copy(acc.at[q], inward_in.at[q], in_s.at[q], in_r.at[q], {"blk": inner})

    def cross_copy(q):
        h = q // 2
        return copy(acc.at[q], cross_in.at[h], cross_s.at[h], cross_r.at[h], {"blk": inner})

    def mid_copy(q):
        return copy(coef.at[q], coef.at[q], mid_s.at[q // 2], coef_r.at[q], {"blk": inner})

    def out_copy(q):
        return copy(coef.at[q], coef.at[q], out_s.at[q], coef_r.at[q], {"blk": outer})

    def ret_copy(q, e, spot):
        return copy(coef.at[q], at(whole, spot, mine), ret_s.at[e], ret_r.at[e], {"cons": other_c})

    def fin_copy(t, spot):
        part_of = at(whole, spot, mine)
        return copy(part_of, part_of, fin_s.at[t], fin_r.at[t], {"blk": partner})

    def add(x, y):
        return x.astype(jnp.float32) + y.astype(jnp.float32)

    def is_import(q):
        return (q >= LEAD) & (q < LEAD + imports)

    def tile_of(q):
        return q + jnp.minimum(q + 1, exports) - jnp.where(q >= LEAD, imports, 0)

    def first_of(g):
        return (c * groups + g) * GROUP // LANES

    def start_of(g):
        out = tiles
        for k in range(groups - 1, -1, -1):
            out = jnp.where(g == k, starts[k], out)
        return out

    def lane_pair(lp):
        return pl.ds(pl.multiple_of(lp * 2 * LANES, 2 * LANES), 2 * LANES)

    def span(begin, end, body):
        def step(i, carry):
            body(i)
            return carry

        lax.fori_loop(begin, end, step, 0)

    lane = lax.broadcasted_iota(jnp.int32, (all_rows, LANES), 1) % GROUP

    def clear(g):
        first = first_of(g)

        def one(lt):
            whole[g, :, pl.ds(pl.multiple_of(lt * LANES, LANES), LANES)] = jnp.zeros((2 * half, LANES), whole.dtype)

        span(first // 2 * 2, first, one)

    loop(groups, clear)

    def produce(g):
        @pl.when(lax.rem(g, chunk) == 0)
        def _():
            for source in range(n_cons):

                @pl.when(c != source)
                def _():
                    there_copy(0, g // chunk, source).wait_recv()

        table_copy(g).wait()
        for fold in range(folds):
            parts = [taken[source, g, fold].astype(jnp.float32) for source in range(n_cons)]
            gathered = jnp.concatenate(parts, axis=0).astype(jnp.bfloat16)
            ordered = jnp.dot(order[...], gathered, preferred_element_type=jnp.float32)
            for m in range(GROUP):
                spread_s[pl.ds(m * all_rows, all_rows), pl.ds(fold * LANES, LANES)] = jnp.where(
                    lane == m, ordered, 0.0
                ).astype(spread_s.dtype)

        def one(lp):
            values = table[g, :, :, lane_pair(lp)].reshape(cycles * GROUP, 2 * LANES)
            part[g, :, lane_pair(lp)] = jnp.dot(
                spread_s[...], values, preferred_element_type=jnp.float32
            ).astype(part.dtype)

        span(first_of(g) // 2, pairs, one)
        span(start_of(g), start_of(g + 1), lambda t: pair_copy(t, plan.place(c, starts, t)).start())

    width = folds * LANES
    order_lane = lax.broadcasted_iota(jnp.int32, (rows, LANES), 1) % GROUP

    def restore(g):
        def take(t):
            fin_copy(t, plan.place(c, starts, t)).wait_recv()

        span(start_of(g), start_of(g + 1), take)

        def one(lp, total):
            values = table[g, :, :, lane_pair(lp)].reshape(cycles * GROUP, 2 * LANES)
            full = lax.dot_general(
                whole[g, :, lane_pair(lp)], values, (((1,), (1,)), ((), ())), preferred_element_type=jnp.float32
            )
            wide = lax.broadcasted_iota(jnp.int32, (all_rows, width), 1) % GROUP
            for m in range(GROUP):
                total = total + jnp.where(wide == m, full[m * all_rows : (m + 1) * all_rows], 0.0)
            return total

        total = lax.fori_loop(first_of(g) // 2, pairs, one, jnp.zeros((all_rows, width), jnp.float32))
        zero_order = (c * groups + g) * GROUP + order_lane == 0
        factor = jnp.where(zero_order, 1.0, 2.0)
        for peer in range(n_cons):
            for fold in range(folds):
                piece = total[peer * rows : (peer + 1) * rows, fold * LANES : (fold + 1) * LANES]
                back[g, peer, fold] = (piece * factor).astype(back.dtype)
        for k in range(n_cons - 1):
            home_copy(k, g, c).start()
        returned[c * groups + g] = back[g, c]

    def give(e):
        spot = plan.place(c, starts, 2 * e)
        pair_copy(2 * e, spot).wait_recv()
        given[e] = add(at(part, spot, mine)[...], pair_in[2 * e]).astype(given.dtype)
        give_copy(e).start()

    def gather(q):
        native = jnp.logical_not(is_import(q))

        @pl.when(native)
        def _():
            t = tile_of(q)
            spot = plan.place(c, starts, t)
            pair_copy(t, spot).wait_recv()
            acc[q] = add(at(part, spot, mine)[...], pair_in[t]).astype(acc.dtype)

        @pl.when(is_import(q))
        def _():
            give_copy(q - LEAD).wait_recv()

        @pl.when(depth < last)
        def _():
            in_copy(q).wait_recv()
            acc[q] = add(acc[q], inward_in[q]).astype(acc.dtype)

        @pl.when(depth > 0)
        def _():
            in_copy(q).start()

        @pl.when((depth == 0) & (lax.rem(q, 2) != side))
        def _():
            cross_copy(q).start()

    def spread(q):
        @pl.when(depth < last)
        def _():
            out_copy(q).start()

        @pl.when(is_import(q))
        def _():
            e = q - LEAD
            ret_copy(q, e, plan.place(other_c, other_starts, 2 * e)).start()

        @pl.when(jnp.logical_not(is_import(q)))
        def _():
            t = tile_of(q)
            spot = plan.place(c, starts, t)
            at(whole, spot, mine)[...] = coef[q]
            fin_copy(t, spot).start()

    def finish(q):
        @pl.when((depth == 0) & (lax.rem(q, 2) == side))
        def _():
            cross_copy(q).wait_recv()
            own = plan.place(c, starts, tile_of(q))[1]
            lent = plan.place(other_c, other_starts, 2 * (q - LEAD))[1]
            lt = jnp.where(is_import(q), lent, own)
            total = add(acc[q], cross_in[q // 2]) * love[pl.ds(lt, 1), :]
            coef[q] = total.astype(coef.dtype)
            mid_copy(q).start()
            spread(q)

    def relay(q):
        @pl.when((depth > 0) | (lax.rem(q, 2) != side))
        def _():
            out_copy(q).wait_recv()
            spread(q)

    def take_back(e):
        spot = plan.place(c, starts, 2 * e)
        ret_copy(0, e, spot).wait_recv()
        fin_copy(2 * e, spot).start()

    relay_gap = jnp.where(depth == 0, REL0, REL1 + (depth - 1) * RELN)
    back_gap = LEAD + relay_gap + BACK

    def ready(g):
        t = start_of(g + 1) - 1
        q = jnp.where(t >= LEAD, t + imports, t)
        q = jnp.where(exports > 0, t - exports, q)
        return jnp.where(t < 2 * exports, t // 2 + back_gap, q + relay_gap) + SLACK

    for g in range(AHEAD):
        produce(g)

    def step(i, done):
        ahead = AHEAD + i // PACE

        @pl.when((lax.rem(i, PACE) == 0) & (ahead < groups))
        def _():
            produce(ahead)

        @pl.when(i < exports)
        def _():
            give(i)

        @pl.when(i < queue)
        def _():
            gather(i)

        q = i - FIN

        @pl.when((q >= 0) & (q < queue))
        def _():
            finish(q)

        r = i - relay_gap

        @pl.when((r >= 0) & (r < queue))
        def _():
            relay(r)

        e = i - back_gap

        @pl.when((e >= 0) & (e < exports))
        def _():
            take_back(e)

        now = (done < groups) & (i >= ready(done))

        @pl.when(now)
        def _():
            restore(done)

        return done + jnp.where(now, 1, 0)

    count = plan.max_queue + LEAD + REL1 + mid * RELN + BACK
    done = lax.fori_loop(0, count, step, 0)
    span(done, groups, restore)

    def unpack(tile):
        def heard_from(k):
            index = tile * blocks + k

            @pl.when(index // groups != c)
            def _():
                home_copy(0, lax.rem(index, groups), index // groups).wait_recv()

        loop(blocks, heard_from)

        def one(fold):
            swapped = swap_blocks([returned[tile * blocks + k, fold].astype(jnp.float32) for k in range(blocks)])
            for k in range(blocks):
                out[tile, fold * blocks + k] = swapped[k].astype(out.dtype)

        loop(folds, one)

    loop(x.shape[0], unpack)

    def drain_tile(t):
        spot = plan.place(c, starts, t)
        pair_copy(t, spot).wait_send()
        fin_copy(t, spot).wait_send()

    loop(tiles, drain_tile)
    loop(exports, lambda e: give_copy(e).wait_send())

    def drain_queue(q):
        @pl.when(depth > 0)
        def _():
            in_copy(q).wait_send()

        @pl.when((depth == 0) & (lax.rem(q, 2) != side))
        def _():
            cross_copy(q).wait_send()

        @pl.when((depth == 0) & (lax.rem(q, 2) == side))
        def _():
            mid_copy(q).wait_send()

        @pl.when(depth < last)
        def _():
            out_copy(q).wait_send()

        @pl.when(is_import(q))
        def _():
            e = q - LEAD
            ret_copy(q, e, plan.place(other_c, other_starts, 2 * e)).wait_send()

    loop(queue, drain_queue)
    for k in range(n_cons - 1):
        for h in range(CHUNKS):
            there_copy(k, h, c).wait_send()

        loop(groups, lambda g, k=k: home_copy(k, g, c).wait_send())


def exchange(x, love, order, legendre, n_cons, n_blk):
    cycles, orders_dev, degrees = legendre.shape
    rows = x.shape[2]
    all_rows = n_cons * rows
    plan = Plan(n_cons, n_blk, orders_dev, degrees)
    groups, folds = plan.groups, cycles * GROUP // LANES
    half = (GROUP * all_rows // 2, LANES)
    kind = x.dtype
    tiles, queue, moved = plan.max_tiles, plan.max_queue, plan.max_moved
    halves = (queue + 1) // 2
    sems = [(n,) for n in [tiles] * 2 + [moved] * 2 + [queue] * 2 + [halves] * 2 + [halves, queue, queue] + [moved] * 2 + [tiles] * 2]
    sems += [(n_cons - 1, CHUNKS), (n_cons, CHUNKS), (n_cons - 1, groups), (n_cons * groups,)]
    lane_tiles = (folds, rows, LANES)
    vmem = pl.BlockSpec(memory_space=pltpu.VMEM)
    return pl.pallas_call(
        functools.partial(sum_kernel, plan),
        out_shape=jax.ShapeDtypeStruct(x.shape, kind),
        in_specs=[vmem] * 3 + [pl.BlockSpec(memory_space=pl.ANY)],
        out_specs=vmem,
        scratch_shapes=[
            pltpu.VMEM((groups, cycles, GROUP, degrees), kind),
            pltpu.SemaphoreType.DMA((groups,)),
            pltpu.VMEM((groups, GROUP * all_rows, degrees), kind),
            pltpu.VMEM((GROUP * all_rows, folds * LANES), kind),
            pltpu.VMEM((groups, GROUP * all_rows, degrees), kind),
            pltpu.VMEM((n_cons * groups,) + lane_tiles, kind),
            pltpu.VMEM((n_cons, groups) + lane_tiles, kind),
            pltpu.VMEM((groups, n_cons) + lane_tiles, kind),
            pltpu.VMEM((n_cons * groups,) + lane_tiles, kind),
            pltpu.VMEM((tiles,) + half, kind),
            pltpu.VMEM((queue,) + half, kind),
            pltpu.VMEM((moved,) + half, kind),
            pltpu.VMEM((queue,) + half, kind),
            pltpu.VMEM((halves,) + half, kind),
            pltpu.VMEM((queue,) + half, kind),
        ]
        + [pltpu.SemaphoreType.DMA(n) for n in sems],
        compiler_params=pltpu.CompilerParams(
            collective_id=0, has_side_effects=True, vmem_limit_bytes=60 * 2**20
        ),
    )(x, love.reshape(degrees // LANES, LANES), order, legendre)


def angles_of(lon_index, period, orders):
    order_index = jnp.arange(orders, dtype=jnp.int32)
    phases = lon_index[:, None] * order_index[None, :] % period
    angles = phases.astype(jnp.float32) * jnp.float32(2.0 * 3.141592653589793 / period)
    return jnp.cos(angles), jnp.sin(angles)


def quarter_table(length, period, orders):
    fine = 32
    coarse = length // fine
    parts = angles_of(jnp.arange(coarse, dtype=jnp.int32) * fine, period, orders)
    parts += angles_of(jnp.arange(fine, dtype=jnp.int32), period, orders)
    cos_a, sin_a, cos_b, sin_b = lax.optimization_barrier(parts)
    cos_a, sin_a = cos_a[:, None, :], sin_a[:, None, :]
    cosine = cos_a * cos_b[None] - sin_a * sin_b[None]
    minus_sine = -(sin_a * cos_b[None] + cos_a * sin_b[None])
    both = jnp.concatenate([cosine.astype(jnp.bfloat16), minus_sine.astype(jnp.bfloat16)], axis=2)
    return both.reshape(length, 2 * orders)


def local(elevation, legendre, cycle_weight, love_factor, assignment):
    fld_dev, cycle_dev, longitudes = elevation.shape
    orders_dev, degrees = legendre.shape[1:]
    orders = orders_dev * lax.axis_size("cons")
    quarter = longitudes // 4
    table = lax.optimization_barrier(quarter_table(quarter, longitudes, orders))
    residue = jnp.arange(orders, dtype=jnp.int32) % 4
    turn_re = (residue == 0).astype(jnp.float32) - (residue == 2).astype(jnp.float32)
    turn_im = (residue == 1).astype(jnp.float32) - (residue == 3).astype(jnp.float32)
    sign = turn_re * turn_re - turn_im * turn_im

    def halves(q):
        part = lax.slice_in_dim(elevation, q * quarter, (q + 1) * quarter, axis=2)
        both = jnp.einsum("fjk,kn->fjn", part, table, preferred_element_type=jnp.float32)
        return both[..., :orders], both[..., orders:]

    (re0, im0), (re1, im1), (re2, im2), (re3, im3) = (halves(q) for q in range(4))
    even_re, even_im = re0 + sign * re2, im0 + sign * im2
    odd_re, odd_im = re1 + sign * re3, im1 + sign * im3
    running = jnp.stack(
        [
            even_re + turn_re * odd_re + turn_im * odd_im,
            even_im + turn_re * odd_im - turn_im * odd_re,
        ],
        axis=1,
    )
    spectra = (running * cycle_weight[None, None, :, None]).astype(jnp.bfloat16)
    x = spectra.reshape(fld_dev, 2, cycle_dev, orders // LANES, LANES)
    x = x.transpose(3, 2, 1, 0, 4).reshape(orders // LANES, cycle_dev, 2 * fld_dev, LANES)
    n_cons = lax.axis_size("cons")
    row = jnp.arange(n_cons * 2 * fld_dev, dtype=jnp.int32)
    field, piece = row // (2 * fld_dev) * fld_dev + row % fld_dev, row // fld_dev % 2
    same = (assignment[field][:, None] == field[None, :]) & (piece[:, None] == piece[None, :])
    y = exchange(x, love_factor, same.astype(jnp.bfloat16), legendre, n_cons, lax.axis_size("blk"))
    y = y.reshape(orders // LANES, cycle_dev, 2, fld_dev, LANES).transpose(2, 3, 1, 0, 4)
    y = y.reshape(2, fld_dev, cycle_dev, orders).astype(jnp.float32)
    re, im = y[0], y[1]
    turned = [
        (re, im),
        (turn_re * re - turn_im * im, turn_re * im + turn_im * re),
        (sign * re, sign * im),
        (turn_re * re + turn_im * im, turn_re * im - turn_im * re),
    ]
    return jnp.concatenate(
        [
            jnp.einsum(
                "fjn,kn->fjk",
                jnp.concatenate(pair, axis=2).astype(jnp.bfloat16),
                table,
                preferred_element_type=jnp.float32,
            )
            for pair in turned
        ],
        axis=2,
    )


def solution(mesh):
    placed = (P("cons", "blk", None), P("blk", "cons", None), P("blk"), P(), P())
    return jax.shard_map(
        local, mesh=mesh, in_specs=placed, out_specs=P("cons", "blk", None), check_vma=False
    )
```

```python
import functools

import jax
import jax.numpy as jnp
from jax import lax
from jax.experimental import pallas as pl
from jax.experimental.pallas import tpu as pltpu
from jax.sharding import PartitionSpec as P

GROUP = 16
LANES = 128
LEAD = 6
FIN = 4
REL0 = 8
REL1 = 14
RELN = 5
BACK = 4
SLACK = 2
AHEAD = 2
PACE = 3
CHUNKS = 3
WAVE_AT = 1
FINE = 32
MESH = pl.DeviceIdType.MESH


class Plan:
    def __init__(self, n_cons, n_blk, orders_dev, degrees):
        self.n_cons, self.chips = n_cons, n_blk // 2
        self.groups, self.columns = orders_dev // GROUP, degrees // LANES
        counts = [sum(self.width(c, g) for g in range(self.groups)) for c in range(n_cons)]
        self.counts = counts
        moved = [max(0, (counts[c] - counts[n_cons - 1 - c]) // 2) for c in range(n_cons)]
        self.moved = moved
        self.max_tiles = max(counts)
        self.max_moved = max(1, max(moved))
        self.queues = [counts[c] - moved[c] + moved[n_cons - 1 - c] for c in range(n_cons)]
        self.max_queue = max(self.queues)

    def first(self, c, g):
        return (c * self.groups + g) * GROUP // LANES

    def width(self, c, g):
        return self.columns - self.first(c, g)

    def starts(self, c):
        begin, out = 0, []
        for g in range(self.groups):
            out.append(begin)
            begin = begin + self.width(c, g)
        return out, begin

    def place(self, c, starts, t):
        g = 0
        for start in starts[1:]:
            g = g + jnp.where(t >= start, 1, 0)
        begin = 0
        for k in range(1, self.groups):
            begin = jnp.where(t >= starts[k], starts[k], begin)
        return g, (c * self.groups + g) * GROUP // LANES + t - begin


def pick(c, values):
    out = values[-1]
    for k in range(len(values) - 1):
        out = jnp.where(c == k, values[k], out)
    return out


def swap_blocks(tiles):
    count = LANES // GROUP
    block = lax.broadcasted_iota(jnp.int32, tiles[0].shape, len(tiles[0].shape) - 1) // GROUP
    step = count // 2
    while step:
        high = (block // step) % 2 == 1
        new = list(tiles)
        for a in range(count):
            if (a // step) % 2 == 0:
                low_t, high_t = tiles[a], tiles[a + step]
                up = pltpu.roll(high_t, GROUP * step, high_t.ndim - 1)
                down = pltpu.roll(low_t, LANES - GROUP * step, low_t.ndim - 1)
                new[a] = jnp.where(high, up, low_t)
                new[a + step] = jnp.where(high, high_t, down)
        tiles = new
        step //= 2
    return tiles


def sum_kernel(
    plan, x, love, order, legendre, out, wave, table, table_sem, part, spread_s, whole, sent, taken, back, returned,
    pair_in, acc, given, inward_in, cross_in, coef, fine, waves, wave_sem, *sems
):
    (pair_s, pair_r, give_s, give_r, in_s, in_r, cross_s, cross_r, mid_s, out_s, coef_r, ret_s, ret_r, fin_s, fin_r) = sems[:15]
    there_s, there_r, home_s, home_r = sems[15:]
    me, c = lax.axis_index("blk"), lax.axis_index("cons")
    chips, half = plan.chips, part.shape[1] // 2
    n_cons, groups = plan.n_cons, plan.groups
    cycles = x.shape[1]
    blocks = LANES // GROUP
    folds = cycles // blocks
    rows = x.shape[2]
    all_rows = n_cons * rows
    pairs = plan.columns // 2
    p, core = me // 2, lax.rem(me, 2)
    mid = chips // 2
    left = p < mid
    depth = jnp.where(left, mid - 1 - p, p - mid)
    side = jnp.where(left, 0, 1)
    inner = jnp.where(left, me + 2, me - 2)
    outer = jnp.where(left, me - 2, me + 2)
    partner = me + 1 - 2 * core
    other_c = n_cons - 1 - c
    last = mid - 1

    starts, tiles = plan.starts(c)
    other_starts, _ = plan.starts(other_c)
    exports, imports = pick(c, plan.moved), pick(other_c, plan.moved)
    queue = pick(c, plan.queues)

    barrier = pltpu.get_barrier_semaphore()

    def greet(where):
        pl.semaphore_signal(barrier, inc=1, device_id=where, device_id_type=MESH)

    greet({"blk": partner})

    @pl.when(p > 0)
    def _():
        greet({"blk": me - 2})

    @pl.when(p < chips - 1)
    def _():
        greet({"blk": me + 2})

    peers = [lax.rem(c + k, n_cons) for k in range(1, n_cons)]
    for peer in peers:
        greet({"cons": peer})

    def loop(count, body):
        def step(i, carry):
            body(i)
            return carry

        lax.fori_loop(0, count, step, 0)

    def table_copy(g):
        return pltpu.make_async_copy(
            legendre.at[:, pl.ds(pl.multiple_of(g * GROUP, GROUP), GROUP), :], table.at[g], table_sem.at[g]
        )

    loop(groups, lambda g: table_copy(g).start())

    def pack(tile):
        split = x[tile].astype(jnp.float32).reshape(folds, blocks, rows, LANES)
        swapped = swap_blocks([split[:, k] for k in range(blocks)])
        for k in range(blocks):
            sent[tile * blocks + k] = swapped[k].astype(sent.dtype)

    loop(x.shape[0], pack)

    heard = n_cons + jnp.where(p > 0, 1, 0) + jnp.where(p < chips - 1, 1, 0)
    pl.semaphore_wait(barrier, heard)

    def copy(src, dst, send, recv, where):
        return pltpu.make_async_remote_copy(
            src_ref=src, dst_ref=dst, send_sem=send, recv_sem=recv, device_id=where, device_id_type=MESH
        )

    chunk = groups // CHUNKS

    def there_copy(k, h, source):
        peer = peers[k]
        return copy(
            sent.at[pl.ds(peer * groups + h * chunk, chunk)],
            taken.at[source, pl.ds(h * chunk, chunk)],
            there_s.at[k, h],
            there_r.at[source, h],
            {"cons": peer},
        )

    for h in range(CHUNKS):
        for k in range(n_cons - 1):
            there_copy(k, h, c).start()

    def keep(g):
        taken[c, g] = sent[c * groups + g]

    loop(groups, keep)

    def home_copy(k, g, source):
        return copy(
            back.at[g, peers[k]],
            returned.at[source * groups + g],
            home_s.at[k, g],
            home_r.at[source * groups + g],
            {"cons": peers[k]},
        )

    corner = (0, plan.columns - 1)

    def rows_of(k):
        return pl.ds(pl.multiple_of(k * half, half), half)

    mine, theirs = rows_of(core), rows_of(1 - core)

    def at(ref, spot, rows):
        g, lt = spot
        return ref.at[g, rows, pl.ds(pl.multiple_of(lt * LANES, LANES), LANES)]

    def pair_copy(t, spot):
        return copy(at(part, spot, theirs), pair_in.at[t], pair_s.at[t], pair_r.at[t], {"blk": partner})

    def give_copy(e):
        return copy(given.at[e], acc.at[LEAD + e], give_s.at[e], give_r.at[e], {"cons": other_c})

    def in_copy(q):
        return copy(acc.at[q], inward_in.at[q], in_s.at[q], in_r.at[q], {"blk": inner})

    def cross_copy(q):
        h = q // 2
        return copy(acc.at[q], cross_in.at[h], cross_s.at[h], cross_r.at[h], {"blk": inner})

    def mid_copy(q):
        return copy(coef.at[q], coef.at[q], mid_s.at[q // 2], coef_r.at[q], {"blk": inner})

    def out_copy(q):
        return copy(coef.at[q], coef.at[q], out_s.at[q], coef_r.at[q], {"blk": outer})

    def ret_copy(q, e, spot):
        return copy(coef.at[q], at(whole, spot, mine), ret_s.at[e], ret_r.at[e], {"cons": other_c})

    def fin_copy(t, spot):
        part_of = at(whole, spot, mine)
        return copy(part_of, part_of, fin_s.at[t], fin_r.at[t], {"blk": partner})

    def add(x, y):
        return x.astype(jnp.float32) + y.astype(jnp.float32)

    def is_import(q):
        return (q >= LEAD) & (q < LEAD + imports)

    def tile_of(q):
        return q + jnp.minimum(q + 1, exports) - jnp.where(q >= LEAD, imports, 0)

    def first_of(g):
        return (c * groups + g) * GROUP // LANES

    def start_of(g):
        out = tiles
        for k in range(groups - 1, -1, -1):
            out = jnp.where(g == k, starts[k], out)
        return out

    def lane_pair(lp):
        return pl.ds(pl.multiple_of(lp * 2 * LANES, 2 * LANES), 2 * LANES)

    def span(begin, end, body):
        def step(i, carry):
            body(i)
            return carry

        lax.fori_loop(begin, end, step, 0)

    lane = lax.broadcasted_iota(jnp.int32, (all_rows, LANES), 1) % GROUP

    def clear(g):
        first = first_of(g)

        def one(lt):
            whole[g, :, pl.ds(pl.multiple_of(lt * LANES, LANES), LANES)] = jnp.zeros((2 * half, LANES), whole.dtype)

        span(first // 2 * 2, first, one)

    loop(groups, clear)

    def produce(g):
        @pl.when(lax.rem(g, chunk) == 0)
        def _():
            for source in range(n_cons):

                @pl.when(c != source)
                def _():
                    there_copy(0, g // chunk, source).wait_recv()

        table_copy(g).wait()
        for fold in range(folds):
            parts = [taken[source, g, fold].astype(jnp.float32) for source in range(n_cons)]
            gathered = jnp.concatenate(parts, axis=0).astype(jnp.bfloat16)
            ordered = jnp.dot(order[...], gathered, preferred_element_type=jnp.float32)
            for m in range(GROUP):
                spread_s[pl.ds(m * all_rows, all_rows), pl.ds(fold * LANES, LANES)] = jnp.where(
                    lane == m, ordered, 0.0
                ).astype(spread_s.dtype)

        def one(lp):
            values = table[g, :, :, lane_pair(lp)].reshape(cycles * GROUP, 2 * LANES)
            part[g, :, lane_pair(lp)] = jnp.dot(
                spread_s[...], values, preferred_element_type=jnp.float32
            ).astype(part.dtype)

        span(first_of(g) // 2, pairs, one)
        span(start_of(g), start_of(g + 1), lambda t: pair_copy(t, plan.place(c, starts, t)).start())

    width = folds * LANES
    order_lane = lax.broadcasted_iota(jnp.int32, (rows, LANES), 1) % GROUP

    def restore(g):
        def take(t):
            fin_copy(t, corner).wait_recv()

        span(start_of(g), start_of(g + 1), take)

        def one(lp, total):
            values = table[g, :, :, lane_pair(lp)].reshape(cycles * GROUP, 2 * LANES)
            full = lax.dot_general(
                whole[g, :, lane_pair(lp)], values, (((1,), (1,)), ((), ())), preferred_element_type=jnp.float32
            )
            wide = lax.broadcasted_iota(jnp.int32, (all_rows, width), 1) % GROUP
            for m in range(GROUP):
                total = total + jnp.where(wide == m, full[m * all_rows : (m + 1) * all_rows], 0.0)
            return total

        total = lax.fori_loop(first_of(g) // 2, pairs, one, jnp.zeros((all_rows, width), jnp.float32))
        zero_order = (c * groups + g) * GROUP + order_lane == 0
        factor = jnp.where(zero_order, 1.0, 2.0)
        for peer in range(n_cons):
            for fold in range(folds):
                piece = total[peer * rows : (peer + 1) * rows, fold * LANES : (fold + 1) * LANES]
                back[g, peer, fold] = (piece * factor).astype(back.dtype)
        for k in range(n_cons - 1):
            home_copy(k, g, c).start()
        returned[c * groups + g] = back[g, c]

    def give(e):
        spot = plan.place(c, starts, 2 * e)
        pair_copy(2 * e, spot).wait_recv()
        given[e] = add(at(part, spot, mine)[...], pair_in[2 * e]).astype(given.dtype)
        give_copy(e).start()

    def gather(q):
        native = jnp.logical_not(is_import(q))

        @pl.when(native)
        def _():
            t = tile_of(q)
            spot = plan.place(c, starts, t)
            pair_copy(t, spot).wait_recv()
            acc[q] = add(at(part, spot, mine)[...], pair_in[t]).astype(acc.dtype)

        @pl.when(is_import(q))
        def _():
            give_copy(q - LEAD).wait_recv()

        @pl.when(depth < last)
        def _():
            in_copy(q).wait_recv()
            acc[q] = add(acc[q], inward_in[q]).astype(acc.dtype)

        @pl.when(depth > 0)
        def _():
            in_copy(q).start()

        @pl.when((depth == 0) & (lax.rem(q, 2) != side))
        def _():
            cross_copy(q).start()

    def spread(q):
        @pl.when(depth < last)
        def _():
            out_copy(q).start()

        @pl.when(is_import(q))
        def _():
            e = q - LEAD
            ret_copy(q, e, plan.place(other_c, other_starts, 2 * e)).start()

        @pl.when(jnp.logical_not(is_import(q)))
        def _():
            t = tile_of(q)
            spot = plan.place(c, starts, t)
            at(whole, spot, mine)[...] = coef[q]
            fin_copy(t, spot).start()

    def finish(q):
        @pl.when((depth == 0) & (lax.rem(q, 2) == side))
        def _():
            cross_copy(q).wait_recv()
            own = plan.place(c, starts, tile_of(q))[1]
            lent = plan.place(other_c, other_starts, 2 * (q - LEAD))[1]
            lt = jnp.where(is_import(q), lent, own)
            total = add(acc[q], cross_in[q // 2]) * love[pl.ds(lt, 1), :]
            coef[q] = total.astype(coef.dtype)
            mid_copy(q).start()
            spread(q)

    def relay(q):
        @pl.when((depth > 0) | (lax.rem(q, 2) != side))
        def _():
            out_copy(q).wait_recv()
            spread(q)

    def take_back(e):
        spot = plan.place(c, starts, 2 * e)
        ret_copy(0, e, spot).wait_recv()
        fin_copy(2 * e, spot).start()

    relay_gap = jnp.where(depth == 0, REL0, REL1 + (depth - 1) * RELN)
    back_gap = LEAD + relay_gap + BACK

    def ready(g):
        t = start_of(g + 1) - 1
        q = jnp.where(t >= LEAD, t + imports, t)
        q = jnp.where(exports > 0, t - exports, q)
        return jnp.where(t < 2 * exports, t // 2 + back_gap, q + relay_gap) + SLACK

    quarter = waves.shape[2]
    fine_rows = fine.shape[1]
    wave_blocks = waves.shape[1] // fine_rows

    def wave_copy(b):
        rows_here = pl.ds(pl.multiple_of(b * fine_rows, fine_rows), fine_rows)
        return pltpu.make_async_copy(waves.at[:, rows_here, :], wave.at[:, rows_here, :], wave_sem.at[b])

    def turn(row):
        lon = lax.broadcasted_iota(jnp.int32, row.shape, 1).astype(jnp.float32)
        phase = row.astype(jnp.float32) * lon
        period = 4.0 * quarter
        phase = phase - jnp.floor(phase * (1.0 / period)) * period
        angle = phase * (2.0 * 3.141592653589793 / period)
        return jnp.cos(angle), jnp.sin(angle)

    def make_fine():
        fine[0], fine[1] = turn(lax.broadcasted_iota(jnp.int32, (fine_rows, quarter), 0))

    def make_wave(b):
        cos_a, sin_a = turn(jnp.full((8, quarter), b * fine_rows, jnp.int32))
        cos_a, sin_a = cos_a[:1], sin_a[:1]
        here = pl.ds(pl.multiple_of(b * fine_rows, fine_rows), fine_rows)
        waves[0, here, :] = (cos_a * fine[0] - sin_a * fine[1]).astype(waves.dtype)
        waves[1, here, :] = (-sin_a * fine[0] - cos_a * fine[1]).astype(waves.dtype)
        wave_copy(b).start()

    for g in range(AHEAD):
        produce(g)

    def step(i, done):
        @pl.when(i == WAVE_AT)
        def _():
            make_fine()

        b = i - WAVE_AT - 1

        @pl.when((b >= 0) & (b < wave_blocks))
        def _():
            make_wave(b)

        ahead = AHEAD + i // PACE

        @pl.when((lax.rem(i, PACE) == 0) & (ahead < groups))
        def _():
            produce(ahead)

        @pl.when(i < exports)
        def _():
            give(i)

        @pl.when(i < queue)
        def _():
            gather(i)

        q = i - FIN

        @pl.when((q >= 0) & (q < queue))
        def _():
            finish(q)

        r = i - relay_gap

        @pl.when((r >= 0) & (r < queue))
        def _():
            relay(r)

        e = i - back_gap

        @pl.when((e >= 0) & (e < exports))
        def _():
            take_back(e)

        now = (done < groups) & (i >= ready(done))

        @pl.when(now)
        def _():
            restore(done)

        return done + jnp.where(now, 1, 0)

    count = plan.max_queue + LEAD + REL1 + mid * RELN + BACK
    done = lax.fori_loop(0, count, step, 0)
    span(done, groups, restore)

    def unpack(tile):
        def heard_from(k):
            index = tile * blocks + k

            @pl.when(index // groups != c)
            def _():
                home_copy(0, lax.rem(index, groups), index // groups).wait_recv()

        loop(blocks, heard_from)

        swapped = swap_blocks([returned[tile * blocks + k].astype(jnp.float32) for k in range(blocks)])
        merged = jnp.stack(swapped, axis=1).reshape(cycles * rows, LANES)
        out[pl.ds(pl.multiple_of(tile * cycles * rows, 8), cycles * rows), :] = merged

    loop(x.shape[0], unpack)

    def drain_tile(t):
        pair_copy(t, corner).wait_send()
        fin_copy(t, corner).wait_send()

    loop(tiles, drain_tile)
    loop(exports, lambda e: give_copy(e).wait_send())

    def drain_queue(q):
        @pl.when(depth > 0)
        def _():
            in_copy(q).wait_send()

        @pl.when((depth == 0) & (lax.rem(q, 2) != side))
        def _():
            cross_copy(q).wait_send()

        @pl.when((depth == 0) & (lax.rem(q, 2) == side))
        def _():
            mid_copy(q).wait_send()

        @pl.when(depth < last)
        def _():
            out_copy(q).wait_send()

        @pl.when(is_import(q))
        def _():
            e = q - LEAD
            ret_copy(q, e, corner).wait_send()

    loop(queue, drain_queue)
    loop(wave_blocks, lambda b: wave_copy(b).wait())
    for k in range(n_cons - 1):
        for h in range(CHUNKS):
            there_copy(k, h, c).wait_send()

        loop(groups, lambda g, k=k: home_copy(k, g, c).wait_send())


def exchange(x, love, order, legendre, quarter, n_cons, n_blk):
    cycles, orders_dev, degrees = legendre.shape
    rows = x.shape[2]
    all_rows = n_cons * rows
    plan = Plan(n_cons, n_blk, orders_dev, degrees)
    groups, folds = plan.groups, cycles * GROUP // LANES
    half = (GROUP * all_rows // 2, LANES)
    kind = x.dtype
    tiles, queue, moved = plan.max_tiles, plan.max_queue, plan.max_moved
    halves = (queue + 1) // 2
    sems = [(n,) for n in [tiles] * 2 + [moved] * 2 + [queue] * 2 + [halves] * 2 + [halves, queue, queue] + [moved] * 2 + [tiles] * 2]
    sems += [(n_cons - 1, CHUNKS), (n_cons, CHUNKS), (n_cons - 1, groups), (n_cons * groups,)]
    lane_tiles = (folds, rows, LANES)
    waves = (2, x.shape[0] * LANES, quarter)
    vmem = pl.BlockSpec(memory_space=pltpu.VMEM)
    return pl.pallas_call(
        functools.partial(sum_kernel, plan),
        out_shape=[
            jax.ShapeDtypeStruct((x.shape[0] * x.shape[1] * rows, LANES), jnp.float32),
            jax.ShapeDtypeStruct(waves, kind),
        ],
        in_specs=[vmem] * 3 + [pl.BlockSpec(memory_space=pl.ANY)],
        out_specs=[vmem, pl.BlockSpec(memory_space=pl.ANY)],
        scratch_shapes=[
            pltpu.VMEM((groups, cycles, GROUP, degrees), kind),
            pltpu.SemaphoreType.DMA((groups,)),
            pltpu.VMEM((groups, GROUP * all_rows, degrees), kind),
            pltpu.VMEM((GROUP * all_rows, folds * LANES), kind),
            pltpu.VMEM((groups, GROUP * all_rows, degrees), kind),
            pltpu.VMEM((n_cons * groups,) + lane_tiles, kind),
            pltpu.VMEM((n_cons, groups) + lane_tiles, kind),
            pltpu.VMEM((groups, n_cons) + lane_tiles, kind),
            pltpu.VMEM((n_cons * groups,) + lane_tiles, kind),
            pltpu.VMEM((tiles,) + half, kind),
            pltpu.VMEM((queue,) + half, kind),
            pltpu.VMEM((moved,) + half, kind),
            pltpu.VMEM((queue,) + half, kind),
            pltpu.VMEM((halves,) + half, kind),
            pltpu.VMEM((queue,) + half, kind),
            pltpu.VMEM((2, FINE, quarter), jnp.float32),
            pltpu.VMEM(waves, kind),
            pltpu.SemaphoreType.DMA((waves[1] // FINE,)),
        ]
        + [pltpu.SemaphoreType.DMA(n) for n in sems],
        compiler_params=pltpu.CompilerParams(
            collective_id=0, has_side_effects=True, vmem_limit_bytes=60 * 2**20
        ),
    )(x, love.reshape(degrees // LANES, LANES), order, legendre)


def inverse_kernel(y, wave, loading, lhs, held, result, wave_sem, out_sem):
    fields, cycles, longitudes = loading.shape
    quarter, tiles = longitudes // 4, lhs.shape[1] // LANES
    width, parts = held.shape[3], held.shape[0]
    rows = 2 * fields

    def columns(n):
        return pl.ds(pl.multiple_of(n * width, width), width)

    def wave_copy(n):
        return pltpu.make_async_copy(wave.at[:, :, columns(n)], held.at[n], wave_sem.at[n])

    def out_copy(n, q):
        place = pl.ds(pl.multiple_of(q * quarter + n * width, width), width)
        return pltpu.make_async_copy(
            result.at[n, pl.ds(q * fields, fields)], loading.at[:, :, place], out_sem.at[n, q]
        )

    for n in range(parts):
        wave_copy(n).start()
    residue = lax.broadcasted_iota(jnp.int32, (2 * cycles, LANES), 1) % 4
    turn_re = jnp.where(residue == 0, 1.0, jnp.where(residue == 2, -1.0, 0.0))
    turn_im = jnp.where(residue == 1, 1.0, jnp.where(residue == 3, -1.0, 0.0))
    sign = turn_re * turn_re - turn_im * turn_im
    orders = tiles * LANES // 2
    for tile in range(tiles // 2):

        def load(piece, pair):
            at = [tile * cycles * rows + piece * fields + 2 * pair + k for k in range(2)]
            return jnp.concatenate([y[pl.ds(a, cycles, stride=rows), :] for a in at], axis=0)

        for pair in range(fields // 2):
            re, im = load(0, pair), load(1, pair)
            turned = (
                (re, im),
                (turn_re * re - turn_im * im, turn_re * im + turn_im * re),
                (sign * re, sign * im),
                (turn_re * re + turn_im * im, turn_re * im - turn_im * re),
            )
            for q in range(4):
                here = pl.ds((q * (fields // 2) + pair) * 2 * cycles, 2 * cycles)
                for piece in range(2):
                    lanes = pl.ds(piece * orders + tile * LANES, LANES)
                    lhs[here, lanes] = turned[q][piece].astype(lhs.dtype)

    def one(n, carry):
        wave_copy(n).wait()
        table = held[n].reshape(2 * orders, width)
        product = jnp.dot(lhs[...], table, preferred_element_type=jnp.float32)
        result[n] = product.reshape(4 * fields, cycles, width)
        for q in range(4):
            out_copy(n, q).start()
        return carry

    lax.fori_loop(0, parts, one, 0)
    for n in range(parts):
        for q in range(4):
            out_copy(n, q).wait()


def inverse(y, wave, fields, cycles):
    orders, quarter = wave.shape[1:]
    parts = quarter // (2 * LANES)
    anywhere = pl.BlockSpec(memory_space=pl.ANY)
    return pl.pallas_call(
        inverse_kernel,
        out_shape=jax.ShapeDtypeStruct((fields, cycles, 4 * quarter), jnp.float32),
        in_specs=[pl.BlockSpec(memory_space=pltpu.VMEM), anywhere],
        out_specs=anywhere,
        scratch_shapes=[
            pltpu.VMEM((4 * fields * cycles, 2 * orders), jnp.bfloat16),
            pltpu.VMEM((parts, 2, orders, 2 * LANES), jnp.bfloat16),
            pltpu.VMEM((parts, 4 * fields, cycles, 2 * LANES), jnp.float32),
            pltpu.SemaphoreType.DMA((parts,)),
            pltpu.SemaphoreType.DMA((parts, 4)),
        ],
        compiler_params=pltpu.CompilerParams(vmem_limit_bytes=40 * 2**20),
    )(y, wave)


def angles_of(lon_index, period, orders):
    order_index = jnp.arange(orders, dtype=jnp.int32)
    phases = lon_index[:, None] * order_index[None, :] % period
    angles = phases.astype(jnp.float32) * jnp.float32(2.0 * 3.141592653589793 / period)
    return jnp.cos(angles), jnp.sin(angles)


def quarter_table(length, period, orders):
    fine = 32
    coarse = length // fine
    parts = angles_of(jnp.arange(coarse, dtype=jnp.int32) * fine, period, orders)
    parts += angles_of(jnp.arange(fine, dtype=jnp.int32), period, orders)
    cos_a, sin_a, cos_b, sin_b = lax.optimization_barrier(parts)
    cos_a, sin_a = cos_a[:, None, :], sin_a[:, None, :]
    cosine = cos_a * cos_b[None] - sin_a * sin_b[None]
    minus_sine = -(sin_a * cos_b[None] + cos_a * sin_b[None])
    both = jnp.concatenate([cosine.astype(jnp.bfloat16), minus_sine.astype(jnp.bfloat16)], axis=2)
    return both.reshape(length, 2 * orders)


def local(elevation, legendre, cycle_weight, love_factor, assignment):
    fld_dev, cycle_dev, longitudes = elevation.shape
    orders_dev, degrees = legendre.shape[1:]
    orders = orders_dev * lax.axis_size("cons")
    quarter = longitudes // 4
    table = lax.optimization_barrier(quarter_table(quarter, longitudes, orders))
    residue = jnp.arange(orders, dtype=jnp.int32) % 4
    turn_re = (residue == 0).astype(jnp.float32) - (residue == 2).astype(jnp.float32)
    turn_im = (residue == 1).astype(jnp.float32) - (residue == 3).astype(jnp.float32)
    sign = turn_re * turn_re - turn_im * turn_im

    def halves(q):
        part = lax.slice_in_dim(elevation, q * quarter, (q + 1) * quarter, axis=2)
        both = jnp.einsum("fjk,kn->fjn", part, table, preferred_element_type=jnp.float32)
        return both[..., :orders], both[..., orders:]

    (re0, im0), (re1, im1), (re2, im2), (re3, im3) = (halves(q) for q in range(4))
    even_re, even_im = re0 + sign * re2, im0 + sign * im2
    odd_re, odd_im = re1 + sign * re3, im1 + sign * im3
    running = jnp.stack(
        [
            even_re + turn_re * odd_re + turn_im * odd_im,
            even_im + turn_re * odd_im - turn_im * odd_re,
        ],
        axis=1,
    )
    spectra = (running * cycle_weight[None, None, :, None]).astype(jnp.bfloat16)
    x = spectra.reshape(fld_dev, 2, cycle_dev, orders // LANES, LANES)
    x = x.transpose(3, 2, 1, 0, 4).reshape(orders // LANES, cycle_dev, 2 * fld_dev, LANES)
    n_cons = lax.axis_size("cons")
    slots = (n_cons, 2, fld_dev)
    field = jnp.arange(n_cons * fld_dev, dtype=jnp.int32).reshape(n_cons, 1, fld_dev)
    chosen = assignment.reshape(n_cons, 1, fld_dev)
    piece = jnp.arange(2, dtype=jnp.int32).reshape(1, 2, 1)
    give, have = jnp.broadcast_to(2 * field + piece, slots), jnp.broadcast_to(2 * chosen + piece, slots)
    order = (have.reshape(-1, 1) == give.reshape(1, -1)).astype(jnp.bfloat16)
    y, wave = exchange(x, love_factor, order, legendre, quarter, n_cons, lax.axis_size("blk"))
    return inverse(y, wave, fld_dev, cycle_dev)


def solution(mesh):
    placed = (P("cons", "blk", None), P("blk", "cons", None), P("blk"), P(), P())
    return jax.shard_map(
        local, mesh=mesh, in_specs=placed, out_specs=P("cons", "blk", None), check_vma=False
    )
```

```python
import functools

import jax
import jax.numpy as jnp
from jax import lax
from jax.experimental import pallas as pl
from jax.experimental.pallas import tpu as pltpu
from jax.sharding import PartitionSpec as P

GROUP = 16
LANES = 128
LEAD = 6
FIN = 4
REL0 = 8
REL1 = 14
RELN = 5
BACK = 4
SLACK = 2
AHEAD = 2
PACE = 3
CHUNKS = 3
WAVE_AT = 1
FINE = 32
MESH = pl.DeviceIdType.MESH


class Plan:
    def __init__(self, n_cons, n_blk, orders_dev, degrees):
        self.n_cons, self.chips = n_cons, n_blk // 2
        self.groups, self.columns = orders_dev // GROUP, degrees // LANES
        counts = [sum(self.width(c, g) for g in range(self.groups)) for c in range(n_cons)]
        self.counts = counts
        moved = [max(0, (counts[c] - counts[n_cons - 1 - c]) // 2) for c in range(n_cons)]
        self.moved = moved
        self.max_tiles = max(counts)
        self.max_moved = max(1, max(moved))
        self.queues = [counts[c] - moved[c] + moved[n_cons - 1 - c] for c in range(n_cons)]
        self.max_queue = max(self.queues)

    def first(self, c, g):
        return (c * self.groups + g) * GROUP // LANES

    def width(self, c, g):
        return self.columns - self.first(c, g)

    def starts(self, c):
        begin, out = 0, []
        for g in range(self.groups):
            out.append(begin)
            begin = begin + self.width(c, g)
        return out, begin

    def place(self, c, starts, t):
        g = 0
        for start in starts[1:]:
            g = g + jnp.where(t >= start, 1, 0)
        begin = 0
        for k in range(1, self.groups):
            begin = jnp.where(t >= starts[k], starts[k], begin)
        return g, (c * self.groups + g) * GROUP // LANES + t - begin


def pick(c, values):
    out = values[-1]
    for k in range(len(values) - 1):
        out = jnp.where(c == k, values[k], out)
    return out


def swap_blocks(tiles):
    count = LANES // GROUP
    block = lax.broadcasted_iota(jnp.int32, tiles[0].shape, len(tiles[0].shape) - 1) // GROUP
    step = count // 2
    while step:
        high = (block // step) % 2 == 1
        new = list(tiles)
        for a in range(count):
            if (a // step) % 2 == 0:
                low_t, high_t = tiles[a], tiles[a + step]
                up = pltpu.roll(high_t, GROUP * step, high_t.ndim - 1)
                down = pltpu.roll(low_t, LANES - GROUP * step, low_t.ndim - 1)
                new[a] = jnp.where(high, up, low_t)
                new[a + step] = jnp.where(high, high_t, down)
        tiles = new
        step //= 2
    return tiles


def sum_kernel(
    plan, elevation, weight, assignment, love, legendre, out, wave, table, table_sem, part, spread_s, whole, sent, taken, back, returned,
    pair_in, acc, given, inward_in, cross_in, coef, fine, waves, wave_sem,
    field_sem, coarse, near, forward, weights, order, split_s, *sems
):
    (pair_s, pair_r, give_s, give_r, in_s, in_r, cross_s, cross_r, mid_s, out_s, coef_r, ret_s, ret_r, fin_s, fin_r) = sems[:15]
    there_s, there_r, home_s, home_r = sems[15:]
    me, c = lax.axis_index("blk"), lax.axis_index("cons")
    chips, half = plan.chips, part.shape[1] // 2
    n_cons, groups = plan.n_cons, plan.groups
    cycles = weight.shape[0]
    blocks = LANES // GROUP
    folds = cycles // blocks
    fields = elevation.shape[0] // cycles
    rows = 2 * fields
    order_tiles = n_cons * groups // blocks
    all_rows = n_cons * rows
    pairs = plan.columns // 2
    p, core = me // 2, lax.rem(me, 2)
    mid = chips // 2
    left = p < mid
    depth = jnp.where(left, mid - 1 - p, p - mid)
    side = jnp.where(left, 0, 1)
    inner = jnp.where(left, me + 2, me - 2)
    outer = jnp.where(left, me - 2, me + 2)
    partner = me + 1 - 2 * core
    other_c = n_cons - 1 - c
    last = mid - 1

    starts, tiles = plan.starts(c)
    other_starts, _ = plan.starts(other_c)
    exports, imports = pick(c, plan.moved), pick(other_c, plan.moved)
    queue = pick(c, plan.queues)

    barrier = pltpu.get_barrier_semaphore()

    def greet(where):
        pl.semaphore_signal(barrier, inc=1, device_id=where, device_id_type=MESH)

    greet({"blk": partner})

    @pl.when(p > 0)
    def _():
        greet({"blk": me - 2})

    @pl.when(p < chips - 1)
    def _():
        greet({"blk": me + 2})

    peers = [lax.rem(c + k, n_cons) for k in range(1, n_cons)]
    for peer in peers:
        greet({"cons": peer})

    def loop(count, body):
        def step(i, carry):
            body(i)
            return carry

        lax.fori_loop(0, count, step, 0)

    def table_copy(g):
        return pltpu.make_async_copy(
            legendre.at[:, pl.ds(pl.multiple_of(g * GROUP, GROUP), GROUP), :], table.at[g], table_sem.at[g]
        )

    def copy(src, dst, send, recv, where):
        return pltpu.make_async_remote_copy(
            src_ref=src, dst_ref=dst, send_sem=send, recv_sem=recv, device_id=where, device_id_type=MESH
        )

    chunk = groups // CHUNKS

    def there_copy(k, h, source):
        peer = peers[k]
        return copy(
            sent.at[pl.ds(peer * groups + h * chunk, chunk)],
            taken.at[source, pl.ds(h * chunk, chunk)],
            there_s.at[k, h],
            there_r.at[source, h],
            {"cons": peer},
        )

    quarter = waves.shape[2]
    period = 4.0 * quarter
    slot_lanes = whole.shape[2]
    per_quarter = quarter // slot_lanes
    chunk_orders = chunk * GROUP
    half_lanes = n_cons * chunk_orders
    lens = coarse.shape[1]

    def circle(phase):
        phase = phase - jnp.floor(phase * (1.0 / period)) * period
        angle = phase * (2.0 * 3.141592653589793 / period)
        return jnp.cos(angle), jnp.sin(angle)

    def field_copy(i):
        lanes = pl.ds(i * slot_lanes, slot_lanes)
        return pltpu.make_async_copy(
            elevation.at[:, lanes], whole.at[i, pl.ds(0, elevation.shape[0]), :], field_sem.at[i]
        )

    for i in range(4 * per_quarter):
        field_copy(i).start()
    loop(groups, lambda g: table_copy(g).start())

    def set_weight(j):
        weights[pl.ds(j, 1), :] = jnp.full((1, LANES), weight[j], jnp.float32)

    loop(cycles, set_weight)
    out_row = lax.broadcasted_iota(jnp.int32, order.shape, 0)
    in_row = lax.broadcasted_iota(jnp.int32, order.shape, 1)
    out_slot = out_row // rows * fields + out_row % fields
    wanted = jnp.zeros(order.shape, jnp.int32)
    for k in range(n_cons * fields):
        wanted = jnp.where(out_slot == k, assignment[k], wanted)
    in_field = in_row // rows * fields + in_row % fields
    same = (wanted == in_field) & (out_row // fields % 2 == in_row // fields % 2)
    order[...] = jnp.where(same, 1.0, 0.0).astype(order.dtype)

    def analyse(h):
        def orders_of(shape):
            at_lane = lax.broadcasted_iota(jnp.int32, shape, 1)
            return at_lane // chunk_orders * (groups * GROUP) + h * chunk_orders + at_lane % chunk_orders

        for ref, stride in ((coarse, near.shape[1]), (near, 1)):
            shape = ref.shape[1:]
            lon = lax.broadcasted_iota(jnp.int32, shape, 0) * stride
            ref[0], ref[1] = circle((lon * orders_of(shape)).astype(jnp.float32))

        def make_rows(a, carry):
            cos_a, sin_a = coarse[0, pl.ds(a, 1), :], coarse[1, pl.ds(a, 1), :]
            here = pl.ds(pl.multiple_of(a * near.shape[1], near.shape[1]), near.shape[1])
            forward[here, :half_lanes] = (cos_a * near[0] - sin_a * near[1]).astype(forward.dtype)
            forward[here, half_lanes:] = (-sin_a * near[0] - cos_a * near[1]).astype(forward.dtype)
            return carry

        lax.fori_loop(0, lens, make_rows, 0, unroll=2)
        if h == 0:
            for i in range(4 * per_quarter):
                field_copy(i).wait()
        parts = []
        for q in range(4):
            total = 0.0
            for i in range(per_quarter):
                total = total + jnp.dot(
                    whole[q * per_quarter + i, : elevation.shape[0], :],
                    forward[i * slot_lanes : (i + 1) * slot_lanes, :],
                    preferred_element_type=jnp.float32,
                )
            parts.append((total[:, :half_lanes], total[:, half_lanes:]))
        (re0, im0), (re1, im1), (re2, im2), (re3, im3) = parts
        residue = lax.broadcasted_iota(jnp.int32, re0.shape, 1) % 4
        turn_re = jnp.where(residue == 0, 1.0, jnp.where(residue == 2, -1.0, 0.0))
        turn_im = jnp.where(residue == 1, 1.0, jnp.where(residue == 3, -1.0, 0.0))
        sign = turn_re * turn_re - turn_im * turn_im
        even_re, even_im = re0 + sign * re2, im0 + sign * im2
        odd_re, odd_im = re1 + sign * re3, im1 + sign * im3
        sums = (even_re + turn_re * odd_re + turn_im * odd_im, even_im + turn_re * odd_im - turn_im * odd_re)
        per_tile = LANES // chunk_orders
        for u in range(half_lanes // LANES):
            for piece in range(2):
                for f in range(fields):
                    value = sums[piece][f * cycles : (f + 1) * cycles, u * LANES : (u + 1) * LANES]
                    split_s[u, pl.ds(piece * fields + f, cycles, stride=rows), :] = value * weights[...]
            split = split_s[u].reshape(folds, blocks, rows, LANES)
            swapped = swap_blocks([split[:, k] for k in range(blocks)])
            for k in range(blocks):
                owner = u * per_tile + k // chunk
                sent[owner * groups + h * chunk + k % chunk] = swapped[k].astype(sent.dtype)

    heard = n_cons + jnp.where(p > 0, 1, 0) + jnp.where(p < chips - 1, 1, 0)
    for h in range(CHUNKS):
        analyse(h)
        if h == 0:
            pl.semaphore_wait(barrier, heard)
        for k in range(n_cons - 1):
            there_copy(k, h, c).start()

    def keep(g):
        taken[c, g] = sent[c * groups + g]

    loop(groups, keep)

    def home_copy(k, g, source):
        return copy(
            back.at[g, peers[k]],
            returned.at[source * groups + g],
            home_s.at[k, g],
            home_r.at[source * groups + g],
            {"cons": peers[k]},
        )

    corner = (0, plan.columns - 1)

    def rows_of(k):
        return pl.ds(pl.multiple_of(k * half, half), half)

    mine, theirs = rows_of(core), rows_of(1 - core)

    def at(ref, spot, rows):
        g, lt = spot
        return ref.at[g, rows, pl.ds(pl.multiple_of(lt * LANES, LANES), LANES)]

    def pair_copy(t, spot):
        return copy(at(part, spot, theirs), pair_in.at[t], pair_s.at[t], pair_r.at[t], {"blk": partner})

    def give_copy(e):
        return copy(given.at[e], acc.at[LEAD + e], give_s.at[e], give_r.at[e], {"cons": other_c})

    def in_copy(q):
        return copy(acc.at[q], inward_in.at[q], in_s.at[q], in_r.at[q], {"blk": inner})

    def cross_copy(q):
        h = q // 2
        return copy(acc.at[q], cross_in.at[h], cross_s.at[h], cross_r.at[h], {"blk": inner})

    def mid_copy(q):
        return copy(coef.at[q], coef.at[q], mid_s.at[q // 2], coef_r.at[q], {"blk": inner})

    def out_copy(q):
        return copy(coef.at[q], coef.at[q], out_s.at[q], coef_r.at[q], {"blk": outer})

    def ret_copy(q, e, spot):
        return copy(coef.at[q], at(whole, spot, mine), ret_s.at[e], ret_r.at[e], {"cons": other_c})

    def fin_copy(t, spot):
        part_of = at(whole, spot, mine)
        return copy(part_of, part_of, fin_s.at[t], fin_r.at[t], {"blk": partner})

    def add(x, y):
        return x.astype(jnp.float32) + y.astype(jnp.float32)

    def is_import(q):
        return (q >= LEAD) & (q < LEAD + imports)

    def tile_of(q):
        return q + jnp.minimum(q + 1, exports) - jnp.where(q >= LEAD, imports, 0)

    def first_of(g):
        return (c * groups + g) * GROUP // LANES

    def start_of(g):
        out = tiles
        for k in range(groups - 1, -1, -1):
            out = jnp.where(g == k, starts[k], out)
        return out

    def lane_pair(lp):
        return pl.ds(pl.multiple_of(lp * 2 * LANES, 2 * LANES), 2 * LANES)

    def span(begin, end, body):
        def step(i, carry):
            body(i)
            return carry

        lax.fori_loop(begin, end, step, 0)

    lane = lax.broadcasted_iota(jnp.int32, (all_rows, LANES), 1) % GROUP

    def clear(g):
        first = first_of(g)

        def one(lt):
            whole[g, :, pl.ds(pl.multiple_of(lt * LANES, LANES), LANES)] = jnp.zeros((2 * half, LANES), whole.dtype)

        span(first // 2 * 2, first, one)

    loop(groups, clear)

    def produce(g):
        @pl.when(lax.rem(g, chunk) == 0)
        def _():
            for source in range(n_cons):

                @pl.when(c != source)
                def _():
                    there_copy(0, g // chunk, source).wait_recv()

        table_copy(g).wait()
        for fold in range(folds):
            parts = [taken[source, g, fold].astype(jnp.float32) for source in range(n_cons)]
            gathered = jnp.concatenate(parts, axis=0).astype(jnp.bfloat16)
            ordered = jnp.dot(order[...], gathered, preferred_element_type=jnp.float32)
            for m in range(GROUP):
                spread_s[pl.ds(m * all_rows, all_rows), pl.ds(fold * LANES, LANES)] = jnp.where(
                    lane == m, ordered, 0.0
                ).astype(spread_s.dtype)

        def one(lp):
            values = table[g, :, :, lane_pair(lp)].reshape(cycles * GROUP, 2 * LANES)
            part[g, :, lane_pair(lp)] = jnp.dot(
                spread_s[...], values, preferred_element_type=jnp.float32
            ).astype(part.dtype)

        span(first_of(g) // 2, pairs, one)
        span(start_of(g), start_of(g + 1), lambda t: pair_copy(t, plan.place(c, starts, t)).start())

    width = folds * LANES
    order_lane = lax.broadcasted_iota(jnp.int32, (rows, LANES), 1) % GROUP

    def restore(g):
        def take(t):
            fin_copy(t, corner).wait_recv()

        span(start_of(g), start_of(g + 1), take)

        def one(lp, total):
            values = table[g, :, :, lane_pair(lp)].reshape(cycles * GROUP, 2 * LANES)
            full = lax.dot_general(
                whole[g, :, lane_pair(lp)], values, (((1,), (1,)), ((), ())), preferred_element_type=jnp.float32
            )
            wide = lax.broadcasted_iota(jnp.int32, (all_rows, width), 1) % GROUP
            for m in range(GROUP):
                total = total + jnp.where(wide == m, full[m * all_rows : (m + 1) * all_rows], 0.0)
            return total

        total = lax.fori_loop(first_of(g) // 2, pairs, one, jnp.zeros((all_rows, width), jnp.float32))
        zero_order = (c * groups + g) * GROUP + order_lane == 0
        factor = jnp.where(zero_order, 1.0, 2.0)
        for peer in range(n_cons):
            for fold in range(folds):
                piece = total[peer * rows : (peer + 1) * rows, fold * LANES : (fold + 1) * LANES]
                back[g, peer, fold] = (piece * factor).astype(back.dtype)
        for k in range(n_cons - 1):
            home_copy(k, g, c).start()
        returned[c * groups + g] = back[g, c]

    def give(e):
        spot = plan.place(c, starts, 2 * e)
        pair_copy(2 * e, spot).wait_recv()
        given[e] = add(at(part, spot, mine)[...], pair_in[2 * e]).astype(given.dtype)
        give_copy(e).start()

    def gather(q):
        native = jnp.logical_not(is_import(q))

        @pl.when(native)
        def _():
            t = tile_of(q)
            spot = plan.place(c, starts, t)
            pair_copy(t, spot).wait_recv()
            acc[q] = add(at(part, spot, mine)[...], pair_in[t]).astype(acc.dtype)

        @pl.when(is_import(q))
        def _():
            give_copy(q - LEAD).wait_recv()

        @pl.when(depth < last)
        def _():
            in_copy(q).wait_recv()
            acc[q] = add(acc[q], inward_in[q]).astype(acc.dtype)

        @pl.when(depth > 0)
        def _():
            in_copy(q).start()

        @pl.when((depth == 0) & (lax.rem(q, 2) != side))
        def _():
            cross_copy(q).start()

    def spread(q):
        @pl.when(depth < last)
        def _():
            out_copy(q).start()

        @pl.when(is_import(q))
        def _():
            e = q - LEAD
            ret_copy(q, e, plan.place(other_c, other_starts, 2 * e)).start()

        @pl.when(jnp.logical_not(is_import(q)))
        def _():
            t = tile_of(q)
            spot = plan.place(c, starts, t)
            at(whole, spot, mine)[...] = coef[q]
            fin_copy(t, spot).start()

    def finish(q):
        @pl.when((depth == 0) & (lax.rem(q, 2) == side))
        def _():
            cross_copy(q).wait_recv()
            own = plan.place(c, starts, tile_of(q))[1]
            lent = plan.place(other_c, other_starts, 2 * (q - LEAD))[1]
            lt = jnp.where(is_import(q), lent, own)
            total = add(acc[q], cross_in[q // 2]) * love[pl.ds(lt, 1), :]
            coef[q] = total.astype(coef.dtype)
            mid_copy(q).start()
            spread(q)

    def relay(q):
        @pl.when((depth > 0) | (lax.rem(q, 2) != side))
        def _():
            out_copy(q).wait_recv()
            spread(q)

    def take_back(e):
        spot = plan.place(c, starts, 2 * e)
        ret_copy(0, e, spot).wait_recv()
        fin_copy(2 * e, spot).start()

    relay_gap = jnp.where(depth == 0, REL0, REL1 + (depth - 1) * RELN)
    back_gap = LEAD + relay_gap + BACK

    def ready(g):
        t = start_of(g + 1) - 1
        q = jnp.where(t >= LEAD, t + imports, t)
        q = jnp.where(exports > 0, t - exports, q)
        return jnp.where(t < 2 * exports, t // 2 + back_gap, q + relay_gap) + SLACK

    fine_rows = fine.shape[1]
    wave_blocks = waves.shape[1] // fine_rows

    def wave_copy(b):
        rows_here = pl.ds(pl.multiple_of(b * fine_rows, fine_rows), fine_rows)
        return pltpu.make_async_copy(waves.at[:, rows_here, :], wave.at[:, rows_here, :], wave_sem.at[b])

    def turn(row):
        lon = lax.broadcasted_iota(jnp.int32, row.shape, 1).astype(jnp.float32)
        return circle(row.astype(jnp.float32) * lon)

    def make_fine():
        fine[0], fine[1] = turn(lax.broadcasted_iota(jnp.int32, (fine_rows, quarter), 0))

    def make_wave(b):
        cos_a, sin_a = turn(jnp.full((8, quarter), b * fine_rows, jnp.int32))
        cos_a, sin_a = cos_a[:1], sin_a[:1]
        here = pl.ds(pl.multiple_of(b * fine_rows, fine_rows), fine_rows)
        waves[0, here, :] = (cos_a * fine[0] - sin_a * fine[1]).astype(waves.dtype)
        waves[1, here, :] = (-sin_a * fine[0] - cos_a * fine[1]).astype(waves.dtype)
        wave_copy(b).start()

    for g in range(AHEAD):
        produce(g)

    def step(i, done):
        @pl.when(i == WAVE_AT)
        def _():
            make_fine()

        b = i - WAVE_AT - 1

        @pl.when((b >= 0) & (b < wave_blocks))
        def _():
            make_wave(b)

        ahead = AHEAD + i // PACE

        @pl.when((lax.rem(i, PACE) == 0) & (ahead < groups))
        def _():
            produce(ahead)

        @pl.when(i < exports)
        def _():
            give(i)

        @pl.when(i < queue)
        def _():
            gather(i)

        q = i - FIN

        @pl.when((q >= 0) & (q < queue))
        def _():
            finish(q)

        r = i - relay_gap

        @pl.when((r >= 0) & (r < queue))
        def _():
            relay(r)

        e = i - back_gap

        @pl.when((e >= 0) & (e < exports))
        def _():
            take_back(e)

        now = (done < groups) & (i >= ready(done))

        @pl.when(now)
        def _():
            restore(done)

        return done + jnp.where(now, 1, 0)

    count = plan.max_queue + LEAD + REL1 + mid * RELN + BACK
    done = lax.fori_loop(0, count, step, 0)
    span(done, groups, restore)

    def unpack(tile):
        def heard_from(k):
            index = tile * blocks + k

            @pl.when(index // groups != c)
            def _():
                home_copy(0, lax.rem(index, groups), index // groups).wait_recv()

        loop(blocks, heard_from)

        swapped = swap_blocks([returned[tile * blocks + k].astype(jnp.float32) for k in range(blocks)])
        merged = jnp.stack(swapped, axis=1).reshape(cycles * rows, LANES)
        out[pl.ds(pl.multiple_of(tile * cycles * rows, 8), cycles * rows), :] = merged

    loop(order_tiles, unpack)

    def drain_tile(t):
        pair_copy(t, corner).wait_send()
        fin_copy(t, corner).wait_send()

    loop(tiles, drain_tile)
    loop(exports, lambda e: give_copy(e).wait_send())

    def drain_queue(q):
        @pl.when(depth > 0)
        def _():
            in_copy(q).wait_send()

        @pl.when((depth == 0) & (lax.rem(q, 2) != side))
        def _():
            cross_copy(q).wait_send()

        @pl.when((depth == 0) & (lax.rem(q, 2) == side))
        def _():
            mid_copy(q).wait_send()

        @pl.when(depth < last)
        def _():
            out_copy(q).wait_send()

        @pl.when(is_import(q))
        def _():
            e = q - LEAD
            ret_copy(q, e, corner).wait_send()

    loop(queue, drain_queue)
    loop(wave_blocks, lambda b: wave_copy(b).wait())
    for k in range(n_cons - 1):
        for h in range(CHUNKS):
            there_copy(k, h, c).wait_send()

        loop(groups, lambda g, k=k: home_copy(k, g, c).wait_send())


def exchange(elevation, weight, assignment, love, legendre, n_cons, n_blk):
    cycles, orders_dev, degrees = legendre.shape
    fields, _, longitudes = elevation.shape
    quarter, rows = longitudes // 4, 2 * fields
    all_rows, orders = n_cons * rows, n_cons * orders_dev
    plan = Plan(n_cons, n_blk, orders_dev, degrees)
    groups, folds = plan.groups, cycles * GROUP // LANES
    half = (GROUP * all_rows // 2, LANES)
    kind = elevation.dtype
    tiles, queue, moved = plan.max_tiles, plan.max_queue, plan.max_moved
    halves = (queue + 1) // 2
    sems = [(n,) for n in [tiles] * 2 + [moved] * 2 + [queue] * 2 + [halves] * 2 + [halves, queue, queue] + [moved] * 2 + [tiles] * 2]
    sems += [(n_cons - 1, CHUNKS), (n_cons, CHUNKS), (n_cons - 1, groups), (n_cons * groups,)]
    lane_tiles = (folds, rows, LANES)
    waves = (2, orders, quarter)
    chunk_lanes = orders // CHUNKS
    vmem = pl.BlockSpec(memory_space=pltpu.VMEM)
    scalars = pl.BlockSpec(memory_space=pltpu.SMEM)
    anywhere = pl.BlockSpec(memory_space=pl.ANY)
    return pl.pallas_call(
        functools.partial(sum_kernel, plan),
        out_shape=[
            jax.ShapeDtypeStruct((orders // LANES * cycles * rows, LANES), jnp.float32),
            jax.ShapeDtypeStruct(waves, kind),
        ],
        in_specs=[anywhere, scalars, scalars, vmem, anywhere],
        out_specs=[vmem, anywhere],
        scratch_shapes=[
            pltpu.VMEM((groups, cycles, GROUP, degrees), kind),
            pltpu.SemaphoreType.DMA((groups,)),
            pltpu.VMEM((groups, GROUP * all_rows, degrees), kind),
            pltpu.VMEM((GROUP * all_rows, folds * LANES), kind),
            pltpu.VMEM((groups, GROUP * all_rows, degrees), kind),
            pltpu.VMEM((n_cons * groups,) + lane_tiles, kind),
            pltpu.VMEM((n_cons, groups) + lane_tiles, kind),
            pltpu.VMEM((groups, n_cons) + lane_tiles, kind),
            pltpu.VMEM((n_cons * groups,) + lane_tiles, kind),
            pltpu.VMEM((tiles,) + half, kind),
            pltpu.VMEM((queue,) + half, kind),
            pltpu.VMEM((moved,) + half, kind),
            pltpu.VMEM((queue,) + half, kind),
            pltpu.VMEM((halves,) + half, kind),
            pltpu.VMEM((queue,) + half, kind),
            pltpu.VMEM((2, FINE, quarter), jnp.float32),
            pltpu.VMEM(waves, kind),
            pltpu.SemaphoreType.DMA((waves[1] // FINE,)),
            pltpu.SemaphoreType.DMA((longitudes // degrees,)),
            pltpu.VMEM((2, quarter // FINE, chunk_lanes), jnp.float32),
            pltpu.VMEM((2, FINE, chunk_lanes), jnp.float32),
            pltpu.VMEM((quarter, 2 * chunk_lanes), kind),
            pltpu.VMEM((cycles, LANES), jnp.float32),
            pltpu.VMEM((all_rows, all_rows), kind),
            pltpu.VMEM((chunk_lanes // LANES, cycles * rows, LANES), jnp.float32),
        ]
        + [pltpu.SemaphoreType.DMA(n) for n in sems],
        compiler_params=pltpu.CompilerParams(
            collective_id=0, has_side_effects=True, vmem_limit_bytes=60 * 2**20
        ),
    )(
        elevation.reshape(fields * cycles, longitudes),
        weight,
        assignment,
        love.reshape(degrees // LANES, LANES),
        legendre,
    )


def inverse_kernel(y, wave, loading, lhs, held, result, wave_sem, out_sem):
    fields, cycles, longitudes = loading.shape
    quarter, tiles = longitudes // 4, lhs.shape[1] // LANES
    width, parts = held.shape[3], held.shape[0]
    rows = 2 * fields

    def columns(n):
        return pl.ds(pl.multiple_of(n * width, width), width)

    def wave_copy(n):
        return pltpu.make_async_copy(wave.at[:, :, columns(n)], held.at[n], wave_sem.at[n])

    def out_copy(n, q):
        place = pl.ds(pl.multiple_of(q * quarter + n * width, width), width)
        return pltpu.make_async_copy(
            result.at[n, pl.ds(q * fields, fields)], loading.at[:, :, place], out_sem.at[n, q]
        )

    for n in range(parts):
        wave_copy(n).start()
    residue = lax.broadcasted_iota(jnp.int32, (2 * cycles, LANES), 1) % 4
    turn_re = jnp.where(residue == 0, 1.0, jnp.where(residue == 2, -1.0, 0.0))
    turn_im = jnp.where(residue == 1, 1.0, jnp.where(residue == 3, -1.0, 0.0))
    sign = turn_re * turn_re - turn_im * turn_im
    orders = tiles * LANES // 2
    for tile in range(tiles // 2):

        def load(piece, pair):
            at = [tile * cycles * rows + piece * fields + 2 * pair + k for k in range(2)]
            return jnp.concatenate([y[pl.ds(a, cycles, stride=rows), :] for a in at], axis=0)

        for pair in range(fields // 2):
            re, im = load(0, pair), load(1, pair)
            turned = (
                (re, im),
                (turn_re * re - turn_im * im, turn_re * im + turn_im * re),
                (sign * re, sign * im),
                (turn_re * re + turn_im * im, turn_re * im - turn_im * re),
            )
            for q in range(4):
                here = pl.ds((q * (fields // 2) + pair) * 2 * cycles, 2 * cycles)
                for piece in range(2):
                    lanes = pl.ds(piece * orders + tile * LANES, LANES)
                    lhs[here, lanes] = turned[q][piece].astype(lhs.dtype)

    def one(n, carry):
        wave_copy(n).wait()
        table = held[n].reshape(2 * orders, width)
        product = jnp.dot(lhs[...], table, preferred_element_type=jnp.float32)
        result[n] = product.reshape(4 * fields, cycles, width)
        for q in range(4):
            out_copy(n, q).start()
        return carry

    lax.fori_loop(0, parts, one, 0)
    for n in range(parts):
        for q in range(4):
            out_copy(n, q).wait()


def inverse(y, wave, fields, cycles):
    orders, quarter = wave.shape[1:]
    parts = quarter // (2 * LANES)
    anywhere = pl.BlockSpec(memory_space=pl.ANY)
    return pl.pallas_call(
        inverse_kernel,
        out_shape=jax.ShapeDtypeStruct((fields, cycles, 4 * quarter), jnp.float32),
        in_specs=[pl.BlockSpec(memory_space=pltpu.VMEM), anywhere],
        out_specs=anywhere,
        scratch_shapes=[
            pltpu.VMEM((4 * fields * cycles, 2 * orders), jnp.bfloat16),
            pltpu.VMEM((parts, 2, orders, 2 * LANES), jnp.bfloat16),
            pltpu.VMEM((parts, 4 * fields, cycles, 2 * LANES), jnp.float32),
            pltpu.SemaphoreType.DMA((parts,)),
            pltpu.SemaphoreType.DMA((parts, 4)),
        ],
        compiler_params=pltpu.CompilerParams(vmem_limit_bytes=60 * 2**20),
    )(y, wave)


def local(elevation, legendre, cycle_weight, love_factor, assignment):
    n_cons, n_blk = lax.axis_size("cons"), lax.axis_size("blk")
    y, wave = exchange(elevation, cycle_weight, assignment, love_factor, legendre, n_cons, n_blk)
    return inverse(y, wave, *elevation.shape[:2])


def solution(mesh):
    placed = (P("cons", "blk", None), P("blk", "cons", None), P("blk"), P(), P())
    return jax.shard_map(
        local, mesh=mesh, in_specs=placed, out_specs=P("cons", "blk", None), check_vma=False
    )
```

```python
import functools

import jax
import jax.numpy as jnp
from jax import lax
from jax.experimental import pallas as pl
from jax.experimental.pallas import tpu as pltpu
from jax.sharding import PartitionSpec as P

GROUP = 16
LANES = 128
LEAD = 4
FIN = 4
REL0 = 8
REL1 = 14
RELN = 5
BACK = 4
SLACK = 2
AHEAD = 1
PACE = 2
EARLY = 2
CHUNK_AT = 3
CHUNKS = 3
VMEM_MIB = 60
WAVE_AT = 5
FINE = 32
MESH = pl.DeviceIdType.MESH


class Plan:
    def __init__(self, n_cons, n_blk, orders_dev, degrees):
        self.n_cons, self.chips = n_cons, n_blk // 2
        self.groups, self.columns = orders_dev // GROUP, degrees // LANES
        counts = [sum(self.width(c, g) for g in range(self.groups)) for c in range(n_cons)]
        self.counts = counts
        moved = [max(0, (counts[c] - counts[n_cons - 1 - c]) // 2) for c in range(n_cons)]
        self.moved = moved
        self.max_tiles = max(counts)
        self.max_moved = max(1, max(moved))
        self.queues = [counts[c] - moved[c] + moved[n_cons - 1 - c] for c in range(n_cons)]
        self.max_queue = max(self.queues)

    def first(self, c, g):
        return (c * self.groups + g) * GROUP // LANES

    def turn(self, c, g):
        return (c * self.groups + g) % (LANES // GROUP)

    def mate(self, c, g):
        return g + LANES // GROUP - 2 * self.turn(c, g)

    def merged(self, c, g):
        return (self.turn(c, g) > LANES // GROUP // 2) & (self.mate(c, g) >= 0)

    def lost(self, c, g):
        place = self.turn(c, g)
        return (place > 0) & (place < LANES // GROUP // 2) & (self.mate(c, g) < self.groups)

    def width(self, c, g):
        return self.columns - self.first(c, g) - (1 if self.lost(c, g) else 0)

    def starts(self, c):
        sums = []
        for k in range(self.groups + 1):
            sums.append(pick(c, [sum(self.width(b, g) for g in range(k)) for b in range(self.n_cons)]))
        return sums[:-1], sums[-1]

    def place(self, c, starts, t):
        starts, tiles = starts
        g, end = 0, starts[1]
        for k in range(1, self.groups):
            after = starts[k + 1] if k + 1 < self.groups else tiles
            g = g + jnp.where(t >= starts[k], 1, 0)
            end = jnp.where(t >= starts[k], after, end)
        return g, self.columns - end + t

    def shift(self, c, spot):
        g, lt = spot
        joined = self.merged(c, g) & (lt == self.first(c, g))
        return jnp.where(joined, LANES - GROUP * self.turn(c, g), 0)


def pick(c, values):
    out = values[-1]
    for k in range(len(values) - 1):
        out = jnp.where(c == k, values[k], out)
    return out


def swap_blocks(tiles):
    count = LANES // GROUP
    block = lax.broadcasted_iota(jnp.int32, tiles[0].shape, len(tiles[0].shape) - 1) // GROUP
    step = count // 2
    while step:
        high = (block // step) % 2 == 1
        new = list(tiles)
        for a in range(count):
            if (a // step) % 2 == 0:
                low_t, high_t = tiles[a], tiles[a + step]
                up = pltpu.roll(high_t, GROUP * step, high_t.ndim - 1)
                down = pltpu.roll(low_t, LANES - GROUP * step, low_t.ndim - 1)
                new[a] = jnp.where(high, up, low_t)
                new[a + step] = jnp.where(high, high_t, down)
        tiles = new
        step //= 2
    return tiles


def sum_kernel(
    plan, elevation, weight, assignment, love, legendre, out, wave, table, table_sem, part, spread_s, whole, sent, taken, back, returned,
    pair_in, acc, given, inward_in, cross_in, coef, fine, waves, wave_sem,
    field_sem, coarse, near, forward, weights, order, split_s, *sems
):
    (pair_s, pair_r, give_s, give_r, in_s, in_r, cross_s, cross_r, mid_s, out_s, coef_r, ret_s, ret_r, fin_s, fin_r) = sems[:15]
    there_s, there_r, home_s, home_r = sems[15:]
    me, c = lax.axis_index("blk"), lax.axis_index("cons")
    chips, half = plan.chips, part.shape[1] // 2
    n_cons, groups = plan.n_cons, plan.groups
    cycles = weight.shape[0]
    blocks = LANES // GROUP
    folds = cycles // blocks
    fields = elevation.shape[0] // cycles
    rows = 2 * fields
    order_tiles = n_cons * groups // blocks
    all_rows = n_cons * rows
    pairs = plan.columns // 2
    p, core = me // 2, lax.rem(me, 2)
    mid = chips // 2
    left = p < mid
    depth = jnp.where(left, mid - 1 - p, p - mid)
    side = jnp.where(left, 0, 1)
    inner = jnp.where(left, me + 2, me - 2)
    outer = jnp.where(left, me - 2, me + 2)
    partner = me + 1 - 2 * core
    other_c = n_cons - 1 - c
    last = mid - 1

    listed, other_starts = plan.starts(c), plan.starts(other_c)
    starts, tiles = listed
    exports, imports = pick(c, plan.moved), pick(other_c, plan.moved)
    queue = pick(c, plan.queues)

    barrier = pltpu.get_barrier_semaphore()

    def greet(where):
        pl.semaphore_signal(barrier, inc=1, device_id=where, device_id_type=MESH)

    greet({"blk": partner})

    @pl.when(p > 0)
    def _():
        greet({"blk": me - 2})

    @pl.when(p < chips - 1)
    def _():
        greet({"blk": me + 2})

    peers = [lax.rem(c + k, n_cons) for k in range(1, n_cons)]
    for peer in peers:
        greet({"cons": peer})

    def loop(count, body):
        def step(i, carry):
            body(i)
            return carry

        lax.fori_loop(0, count, step, 0)

    def table_copy(g):
        return pltpu.make_async_copy(
            legendre.at[:, pl.ds(pl.multiple_of(g * GROUP, GROUP), GROUP), :], table.at[g], table_sem.at[g]
        )

    def copy(src, dst, send, recv, where):
        return pltpu.make_async_remote_copy(
            src_ref=src, dst_ref=dst, send_sem=send, recv_sem=recv, device_id=where, device_id_type=MESH
        )

    chunk = groups // CHUNKS

    def there_copy(k, h, source):
        peer = peers[k]
        return copy(
            sent.at[pl.ds(peer * groups + h * chunk, chunk)],
            taken.at[source, pl.ds(h * chunk, chunk)],
            there_s.at[k, h],
            there_r.at[source, h],
            {"cons": peer},
        )

    quarter = waves.shape[2]
    period = 4.0 * quarter
    slot_lanes = whole.shape[2]
    per_quarter = quarter // slot_lanes
    base = groups - 4 * per_quarter
    chunk_orders = chunk * GROUP
    half_lanes = n_cons * chunk_orders
    lens = coarse.shape[1]

    def circle(phase):
        phase = phase - jnp.floor(phase * (1.0 / period)) * period
        angle = phase * (2.0 * 3.141592653589793 / period)
        return jnp.cos(angle), jnp.sin(angle)

    def field_copy(i):
        lanes = pl.ds(i * slot_lanes, slot_lanes)
        return pltpu.make_async_copy(
            elevation.at[:, lanes], part.at[base + i, pl.ds(0, elevation.shape[0]), :], field_sem.at[i]
        )

    for i in range(4 * per_quarter):
        field_copy(i).start()
    loop(groups, lambda g: table_copy(g).start())

    def set_weight(j):
        weights[pl.ds(j, 1), :] = jnp.full((1, LANES), weight[j], jnp.float32)

    loop(cycles, set_weight)
    out_row = lax.broadcasted_iota(jnp.int32, order.shape, 0)
    in_row = lax.broadcasted_iota(jnp.int32, order.shape, 1)
    out_slot = out_row // rows * fields + out_row % fields
    wanted = jnp.zeros(order.shape, jnp.int32)
    for k in range(n_cons * fields):
        wanted = jnp.where(out_slot == k, assignment[k], wanted)
    in_field = in_row // rows * fields + in_row % fields
    same = (wanted == in_field) & (out_row // fields % 2 == in_row // fields % 2)
    order[...] = jnp.where(same, 1.0, 0.0).astype(order.dtype)

    def analyse(h):
        def orders_of(shape):
            at_lane = lax.broadcasted_iota(jnp.int32, shape, 1)
            return at_lane // chunk_orders * (groups * GROUP) + h * chunk_orders + at_lane % chunk_orders

        for ref, stride in ((coarse, near.shape[1]), (near, 1)):
            shape = ref.shape[1:]
            lon = lax.broadcasted_iota(jnp.int32, shape, 0) * stride
            ref[0], ref[1] = circle((lon * orders_of(shape)).astype(jnp.float32))

        def make_rows(a, carry):
            cos_a, sin_a = coarse[0, pl.ds(a, 1), :], coarse[1, pl.ds(a, 1), :]
            here = pl.ds(pl.multiple_of(a * near.shape[1], near.shape[1]), near.shape[1])
            forward[here, :half_lanes] = (cos_a * near[0] - sin_a * near[1]).astype(forward.dtype)
            forward[here, half_lanes:] = (-sin_a * near[0] - cos_a * near[1]).astype(forward.dtype)
            return carry

        lax.fori_loop(0, lens, make_rows, 0, unroll=8)
        if h == 0:
            for i in range(4 * per_quarter):
                field_copy(i).wait()
        parts = []
        for q in range(4):
            total = 0.0
            for i in range(per_quarter):
                total = total + jnp.dot(
                    part[base + q * per_quarter + i, : elevation.shape[0], :],
                    forward[i * slot_lanes : (i + 1) * slot_lanes, :],
                    preferred_element_type=jnp.float32,
                )
            parts.append((total[:, :half_lanes], total[:, half_lanes:]))
        (re0, im0), (re1, im1), (re2, im2), (re3, im3) = parts
        residue = lax.broadcasted_iota(jnp.int32, re0.shape, 1) % 4
        turn_re = jnp.where(residue == 0, 1.0, jnp.where(residue == 2, -1.0, 0.0))
        turn_im = jnp.where(residue == 1, 1.0, jnp.where(residue == 3, -1.0, 0.0))
        sign = turn_re * turn_re - turn_im * turn_im
        even_re, even_im = re0 + sign * re2, im0 + sign * im2
        odd_re, odd_im = re1 + sign * re3, im1 + sign * im3
        sums = (even_re + turn_re * odd_re + turn_im * odd_im, even_im + turn_re * odd_im - turn_im * odd_re)
        per_tile = LANES // chunk_orders
        for u in range(half_lanes // LANES):
            for piece in range(2):
                for f in range(fields):
                    value = sums[piece][f * cycles : (f + 1) * cycles, u * LANES : (u + 1) * LANES]
                    split_s[u, pl.ds(piece * fields + f, cycles, stride=rows), :] = value * weights[...]
            split = split_s[u].reshape(folds, blocks, rows, LANES)
            swapped = swap_blocks([split[:, k] for k in range(blocks)])
            for k in range(blocks):
                owner = u * per_tile + k // chunk
                sent[owner * groups + h * chunk + k % chunk] = swapped[k].astype(sent.dtype)

    heard = n_cons + jnp.where(p > 0, 1, 0) + jnp.where(p < chips - 1, 1, 0)

    def send_chunk(h):
        analyse(h)
        if h == 0:
            pl.semaphore_wait(barrier, heard)
        for k in range(n_cons - 1):
            there_copy(k, h, c).start()
        for g in range(h * chunk, (h + 1) * chunk):
            taken[c, g] = sent[c * groups + g]

    for h in range(min(EARLY, CHUNKS)):
        send_chunk(h)

    def home_copy(k, g, source):
        return copy(
            back.at[g, peers[k]],
            returned.at[source * groups + g],
            home_s.at[k, g],
            home_r.at[source * groups + g],
            {"cons": peers[k]},
        )

    corner = (0, plan.columns - 1)

    def rows_of(k):
        return pl.ds(pl.multiple_of(k * half, half), half)

    mine, theirs = rows_of(core), rows_of(1 - core)

    def at(ref, spot, rows):
        g, lt = spot
        return ref.at[g, rows, pl.ds(pl.multiple_of(lt * LANES, LANES), LANES)]

    def pair_copy(t, spot):
        return copy(at(part, spot, theirs), pair_in.at[t], pair_s.at[t], pair_r.at[t], {"blk": partner})

    def give_copy(e):
        return copy(given.at[e], acc.at[LEAD + e], give_s.at[e], give_r.at[e], {"cons": other_c})

    def in_copy(q):
        return copy(acc.at[q], inward_in.at[q], in_s.at[q], in_r.at[q], {"blk": inner})

    def cross_copy(q):
        h = q // 2
        return copy(acc.at[q], cross_in.at[h], cross_s.at[h], cross_r.at[h], {"blk": inner})

    def mid_copy(q):
        return copy(coef.at[q], coef.at[q], mid_s.at[q // 2], coef_r.at[q], {"blk": inner})

    def out_copy(q):
        return copy(coef.at[q], coef.at[q], out_s.at[q], coef_r.at[q], {"blk": outer})

    def ret_copy(q, e, spot):
        return copy(coef.at[q], at(whole, spot, mine), ret_s.at[e], ret_r.at[e], {"cons": other_c})

    def fin_copy(t, spot):
        part_of = at(whole, spot, mine)
        return copy(part_of, part_of, fin_s.at[t], fin_r.at[t], {"blk": partner})

    def add(x, y):
        return x.astype(jnp.float32) + y.astype(jnp.float32)

    def is_import(q):
        return (q >= LEAD) & (q < LEAD + imports)

    def tile_of(q):
        return q + jnp.minimum(q + 1, exports) - jnp.where(q >= LEAD, imports, 0)

    def first_of(g):
        return (c * groups + g) * GROUP // LANES

    def start_of(g):
        out = tiles
        for k in range(groups - 1, -1, -1):
            out = jnp.where(g == k, starts[k], out)
        return out

    def lane_pair(lp):
        return pl.ds(pl.multiple_of(lp * 2 * LANES, 2 * LANES), 2 * LANES)

    def span(begin, end, body):
        def step(i, carry):
            body(i)
            return carry

        lax.fori_loop(begin, end, step, 0)

    lane = lax.broadcasted_iota(jnp.int32, (all_rows, LANES), 1) % GROUP

    def clear(g):
        first = first_of(g)

        def one(lt):
            whole[g, :, pl.ds(pl.multiple_of(lt * LANES, LANES), LANES)] = jnp.zeros((2 * half, LANES), whole.dtype)

        span(first // 2 * 2, first, one)

    loop(groups, clear)

    def produce(g):
        @pl.when(lax.rem(g, chunk) == 0)
        def _():
            for source in range(n_cons):

                @pl.when(c != source)
                def _():
                    there_copy(0, g // chunk, source).wait_recv()

        table_copy(g).wait()
        for fold in range(folds):
            parts = [taken[source, g, fold].astype(jnp.float32) for source in range(n_cons)]
            gathered = jnp.concatenate(parts, axis=0).astype(jnp.bfloat16)
            ordered = jnp.dot(order[...], gathered, preferred_element_type=jnp.float32)
            for m in range(GROUP):
                spread_s[pl.ds(m * all_rows, all_rows), pl.ds(fold * LANES, LANES)] = jnp.where(
                    lane == m, ordered, 0.0
                ).astype(spread_s.dtype)

        def one(lp):
            values = table[g, :, :, lane_pair(lp)].reshape(cycles * GROUP, 2 * LANES)
            part[g, :, lane_pair(lp)] = jnp.dot(
                spread_s[...], values, preferred_element_type=jnp.float32
            ).astype(part.dtype)

        span(first_of(g) // 2, pairs, one)

        @pl.when(plan.merged(c, g))
        def _():
            here = pl.ds(pl.multiple_of(first_of(g) * LANES, LANES), LANES)
            moved = LANES - GROUP * plan.turn(c, g)
            lanes = lax.broadcasted_iota(jnp.int32, (2 * half, LANES), 1)
            low = pltpu.roll(part[g, :, here].astype(jnp.float32), moved, 1)
            high = part[plan.mate(c, g), :, here].astype(jnp.float32)
            part[g, :, here] = jnp.where(lanes < moved, low, high).astype(part.dtype)

        span(start_of(g), start_of(g + 1), lambda t: pair_copy(t, plan.place(c, listed, t)).start())

    width = folds * LANES
    order_lane = lax.broadcasted_iota(jnp.int32, (rows, LANES), 1) % GROUP

    def restore(g):
        def take(t):
            fin_copy(t, corner).wait_recv()

        span(start_of(g), start_of(g + 1), take)
        joined = plan.merged(c, g)

        @pl.when(joined)
        def _():
            here = pl.ds(pl.multiple_of(first_of(g) * LANES, LANES), LANES)
            fin_copy(start_of(g), corner).wait_send()
            both = whole[g, :, here]
            whole[plan.mate(c, g), :, here] = both
            back_by = GROUP * plan.turn(c, g)
            whole[g, :, here] = pltpu.roll(both.astype(jnp.float32), back_by, 1).astype(whole.dtype)

        count = jnp.where(plan.lost(c, g), 0, jnp.where(joined, 2, 1))
        span(0, count, lambda n: synthesise(jnp.where(n == 0, g, plan.mate(c, g))))

    def synthesise(g):
        def one(lp, total):
            values = table[g, :, :, lane_pair(lp)].reshape(cycles * GROUP, 2 * LANES)
            full = lax.dot_general(
                whole[g, :, lane_pair(lp)], values, (((1,), (1,)), ((), ())), preferred_element_type=jnp.float32
            )
            wide = lax.broadcasted_iota(jnp.int32, (all_rows, width), 1) % GROUP
            for m in range(GROUP):
                total = total + jnp.where(wide == m, full[m * all_rows : (m + 1) * all_rows], 0.0)
            return total

        total = lax.fori_loop(first_of(g) // 2, pairs, one, jnp.zeros((all_rows, width), jnp.float32))
        zero_order = (c * groups + g) * GROUP + order_lane == 0
        factor = jnp.where(zero_order, 1.0, 2.0)
        for peer in range(n_cons):
            for fold in range(folds):
                piece = total[peer * rows : (peer + 1) * rows, fold * LANES : (fold + 1) * LANES]
                back[g, peer, fold] = (piece * factor).astype(back.dtype)
        for k in range(n_cons - 1):
            home_copy(k, g, c).start()
        returned[c * groups + g] = back[g, c]

    def give(e):
        spot = plan.place(c, listed, 2 * e)
        pair_copy(2 * e, spot).wait_recv()
        given[e] = add(at(part, spot, mine)[...], pair_in[2 * e]).astype(given.dtype)
        give_copy(e).start()

    def gather(q):
        native = jnp.logical_not(is_import(q))

        @pl.when(native)
        def _():
            t = tile_of(q)
            spot = plan.place(c, listed, t)
            pair_copy(t, spot).wait_recv()
            acc[q] = add(at(part, spot, mine)[...], pair_in[t]).astype(acc.dtype)

        @pl.when(is_import(q))
        def _():
            give_copy(q - LEAD).wait_recv()

        @pl.when(depth < last)
        def _():
            in_copy(q).wait_recv()
            acc[q] = add(acc[q], inward_in[q]).astype(acc.dtype)

        @pl.when(depth > 0)
        def _():
            in_copy(q).start()

        @pl.when((depth == 0) & (lax.rem(q, 2) != side))
        def _():
            cross_copy(q).start()

    def spread(q):
        @pl.when(depth < last)
        def _():
            out_copy(q).start()

        @pl.when(is_import(q))
        def _():
            e = q - LEAD
            ret_copy(q, e, plan.place(other_c, other_starts, 2 * e)).start()

        @pl.when(jnp.logical_not(is_import(q)))
        def _():
            t = tile_of(q)
            spot = plan.place(c, listed, t)
            at(whole, spot, mine)[...] = coef[q]
            fin_copy(t, spot).start()

    def finish(q):
        @pl.when((depth == 0) & (lax.rem(q, 2) == side))
        def _():
            cross_copy(q).wait_recv()
            own = plan.place(c, listed, tile_of(q))
            lent = plan.place(other_c, other_starts, 2 * (q - LEAD))
            lt = jnp.where(is_import(q), lent[1], own[1])
            moved = jnp.where(is_import(q), plan.shift(other_c, lent), plan.shift(c, own))
            scale = jnp.broadcast_to(love[pl.ds(lt, 1), :], (8, LANES))
            ahead_of = lax.broadcasted_iota(jnp.int32, (8, LANES), 1) < moved
            scale = jnp.where(ahead_of, pltpu.roll(scale, moved, 1), scale)[:1]
            total = add(acc[q], cross_in[q // 2]) * scale
            coef[q] = total.astype(coef.dtype)
            mid_copy(q).start()
            spread(q)

    def relay(q):
        @pl.when((depth > 0) | (lax.rem(q, 2) != side))
        def _():
            out_copy(q).wait_recv()
            spread(q)

    def take_back(e):
        spot = plan.place(c, listed, 2 * e)
        ret_copy(0, e, spot).wait_recv()
        fin_copy(2 * e, spot).start()

    relay_gap = jnp.where(depth == 0, REL0, REL1 + (depth - 1) * RELN)
    back_gap = LEAD + relay_gap + BACK

    def ready(g):
        t = start_of(g + 1) - 1
        q = jnp.where(t < 2 * exports, t // 2, t - exports) + jnp.where(t >= LEAD, imports, 0)
        e = jnp.where(start_of(g) < 2 * exports, jnp.minimum(t // 2, exports - 1) + back_gap, 0)
        return jnp.maximum(q + relay_gap, e) + SLACK

    fine_rows = fine.shape[1]
    wave_blocks = waves.shape[1] // fine_rows

    def wave_copy(b):
        rows_here = pl.ds(pl.multiple_of(b * fine_rows, fine_rows), fine_rows)
        return pltpu.make_async_copy(waves.at[:, rows_here, :], wave.at[:, rows_here, :], wave_sem.at[b])

    def turn(row):
        lon = lax.broadcasted_iota(jnp.int32, row.shape, 1).astype(jnp.float32)
        return circle(row.astype(jnp.float32) * lon)

    def make_fine():
        fine[0], fine[1] = turn(lax.broadcasted_iota(jnp.int32, (fine_rows, quarter), 0))

    def make_wave(b):
        cos_a, sin_a = turn(jnp.full((8, quarter), b * fine_rows, jnp.int32))
        cos_a, sin_a = cos_a[:1], sin_a[:1]
        here = pl.ds(pl.multiple_of(b * fine_rows, fine_rows), fine_rows)
        waves[0, here, :] = (cos_a * fine[0] - sin_a * fine[1]).astype(waves.dtype)
        waves[1, here, :] = (-sin_a * fine[0] - cos_a * fine[1]).astype(waves.dtype)
        wave_copy(b).start()

    for g in range(AHEAD):
        produce(g)

    def step(i, done):
        for h in range(EARLY, CHUNKS):

            @pl.when(i == CHUNK_AT + (h - EARLY) * 4)
            def _(h=h):
                send_chunk(h)

        @pl.when(i == WAVE_AT)
        def _():
            make_fine()

        b = i - WAVE_AT - 1

        @pl.when((b >= 0) & (b < wave_blocks))
        def _():
            make_wave(b)

        ahead = AHEAD + i // PACE

        @pl.when((lax.rem(i, PACE) == 0) & (ahead < groups))
        def _():
            produce(ahead)

        @pl.when(i < exports)
        def _():
            give(i)

        @pl.when(i < queue)
        def _():
            gather(i)

        q = i - FIN

        @pl.when((q >= 0) & (q < queue))
        def _():
            finish(q)

        r = i - relay_gap

        @pl.when((r >= 0) & (r < queue))
        def _():
            relay(r)

        e = i - back_gap

        @pl.when((e >= 0) & (e < exports))
        def _():
            take_back(e)

        now = (done < groups) & (i >= ready(done))

        @pl.when(now)
        def _():
            restore(done)

        return done + jnp.where(now, 1, 0)

    count = plan.max_queue + LEAD + REL1 + mid * RELN + BACK
    done = lax.fori_loop(0, count, step, 0)
    span(done, groups, restore)

    def unpack(tile):
        def heard_from(k):
            index = tile * blocks + k

            @pl.when(index // groups != c)
            def _():
                home_copy(0, lax.rem(index, groups), index // groups).wait_recv()

        loop(blocks, heard_from)

        swapped = swap_blocks([returned[tile * blocks + k].astype(jnp.float32) for k in range(blocks)])
        merged = jnp.stack(swapped, axis=1).reshape(cycles * rows, LANES)
        out[pl.ds(pl.multiple_of(tile * cycles * rows, 8), cycles * rows), :] = merged

    loop(order_tiles, unpack)

    def drain_tile(t):
        pair_copy(t, corner).wait_send()

    loop(tiles, drain_tile)

    def drain_group(g):
        begin = start_of(g) + jnp.where(plan.merged(c, g), 1, 0)
        span(begin, start_of(g + 1), lambda t: fin_copy(t, corner).wait_send())

    loop(groups, drain_group)
    loop(exports, lambda e: give_copy(e).wait_send())

    def drain_queue(q):
        @pl.when(depth > 0)
        def _():
            in_copy(q).wait_send()

        @pl.when((depth == 0) & (lax.rem(q, 2) != side))
        def _():
            cross_copy(q).wait_send()

        @pl.when((depth == 0) & (lax.rem(q, 2) == side))
        def _():
            mid_copy(q).wait_send()

        @pl.when(depth < last)
        def _():
            out_copy(q).wait_send()

        @pl.when(is_import(q))
        def _():
            e = q - LEAD
            ret_copy(q, e, corner).wait_send()

    loop(queue, drain_queue)
    loop(wave_blocks, lambda b: wave_copy(b).wait())
    for k in range(n_cons - 1):
        for h in range(CHUNKS):
            there_copy(k, h, c).wait_send()

        loop(groups, lambda g, k=k: home_copy(k, g, c).wait_send())


def exchange(elevation, weight, assignment, love, legendre, n_cons, n_blk):
    cycles, orders_dev, degrees = legendre.shape
    fields, _, longitudes = elevation.shape
    quarter, rows = longitudes // 4, 2 * fields
    all_rows, orders = n_cons * rows, n_cons * orders_dev
    plan = Plan(n_cons, n_blk, orders_dev, degrees)
    groups, folds = plan.groups, cycles * GROUP // LANES
    half = (GROUP * all_rows // 2, LANES)
    kind = elevation.dtype
    tiles, queue, moved = plan.max_tiles, plan.max_queue, plan.max_moved
    halves = (queue + 1) // 2
    sems = [(n,) for n in [tiles] * 2 + [moved] * 2 + [queue] * 2 + [halves] * 2 + [halves, queue, queue] + [moved] * 2 + [tiles] * 2]
    sems += [(n_cons - 1, CHUNKS), (n_cons, CHUNKS), (n_cons - 1, groups), (n_cons * groups,)]
    lane_tiles = (folds, rows, LANES)
    waves = (2, orders, quarter)
    chunk_lanes = orders // CHUNKS
    vmem = pl.BlockSpec(memory_space=pltpu.VMEM)
    scalars = pl.BlockSpec(memory_space=pltpu.SMEM)
    anywhere = pl.BlockSpec(memory_space=pl.ANY)
    return pl.pallas_call(
        functools.partial(sum_kernel, plan),
        out_shape=[
            jax.ShapeDtypeStruct((orders // LANES * cycles * rows, LANES), jnp.float32),
            jax.ShapeDtypeStruct(waves, kind),
        ],
        in_specs=[anywhere, scalars, scalars, vmem, anywhere],
        out_specs=[vmem, anywhere],
        scratch_shapes=[
            pltpu.VMEM((groups, cycles, GROUP, degrees), kind),
            pltpu.SemaphoreType.DMA((groups,)),
            pltpu.VMEM((groups, GROUP * all_rows, degrees), kind),
            pltpu.VMEM((GROUP * all_rows, folds * LANES), kind),
            pltpu.VMEM((groups, GROUP * all_rows, degrees), kind),
            pltpu.VMEM((n_cons * groups,) + lane_tiles, kind),
            pltpu.VMEM((n_cons, groups) + lane_tiles, kind),
            pltpu.VMEM((groups, n_cons) + lane_tiles, kind),
            pltpu.VMEM((n_cons * groups,) + lane_tiles, kind),
            pltpu.VMEM((tiles,) + half, kind),
            pltpu.VMEM((queue,) + half, kind),
            pltpu.VMEM((moved,) + half, kind),
            pltpu.VMEM((queue,) + half, kind),
            pltpu.VMEM((halves,) + half, kind),
            pltpu.VMEM((queue,) + half, kind),
            pltpu.VMEM((2, FINE, quarter), jnp.float32),
            pltpu.VMEM(waves, kind),
            pltpu.SemaphoreType.DMA((waves[1] // FINE,)),
            pltpu.SemaphoreType.DMA((longitudes // degrees,)),
            pltpu.VMEM((2, quarter // FINE, chunk_lanes), jnp.float32),
            pltpu.VMEM((2, FINE, chunk_lanes), jnp.float32),
            pltpu.VMEM((quarter, 2 * chunk_lanes), kind),
            pltpu.VMEM((cycles, LANES), jnp.float32),
            pltpu.VMEM((all_rows, all_rows), kind),
            pltpu.VMEM((chunk_lanes // LANES, cycles * rows, LANES), jnp.float32),
        ]
        + [pltpu.SemaphoreType.DMA(n) for n in sems],
        compiler_params=pltpu.CompilerParams(
            collective_id=0, has_side_effects=True, vmem_limit_bytes=VMEM_MIB * 2**20
        ),
    )(
        elevation.reshape(fields * cycles, longitudes),
        weight,
        assignment,
        love.reshape(degrees // LANES, LANES),
        legendre,
    )


def inverse_kernel(y, wave, loading, lhs, held, result, wave_sem, out_sem):
    fields, cycles, longitudes = loading.shape
    quarter, tiles = longitudes // 4, lhs.shape[1] // LANES
    width, parts = held.shape[3], held.shape[0]
    rows = 2 * fields

    def columns(n):
        return pl.ds(pl.multiple_of(n * width, width), width)

    def wave_copy(n):
        return pltpu.make_async_copy(wave.at[:, :, columns(n)], held.at[n], wave_sem.at[n])

    def out_copy(n, q):
        place = pl.ds(pl.multiple_of(q * quarter + n * width, width), width)
        return pltpu.make_async_copy(
            result.at[n, pl.ds(q * fields, fields)], loading.at[:, :, place], out_sem.at[n, q]
        )

    for n in range(parts):
        wave_copy(n).start()
    residue = lax.broadcasted_iota(jnp.int32, (2 * cycles, LANES), 1) % 4
    turn_re = jnp.where(residue == 0, 1.0, jnp.where(residue == 2, -1.0, 0.0))
    turn_im = jnp.where(residue == 1, 1.0, jnp.where(residue == 3, -1.0, 0.0))
    sign = turn_re * turn_re - turn_im * turn_im
    orders = tiles * LANES // 2
    for tile in range(tiles // 2):

        def load(piece, pair):
            at = [tile * cycles * rows + piece * fields + 2 * pair + k for k in range(2)]
            return jnp.concatenate([y[pl.ds(a, cycles, stride=rows), :] for a in at], axis=0)

        for pair in range(fields // 2):
            re, im = load(0, pair), load(1, pair)
            turned = (
                (re, im),
                (turn_re * re - turn_im * im, turn_re * im + turn_im * re),
                (sign * re, sign * im),
                (turn_re * re + turn_im * im, turn_re * im - turn_im * re),
            )
            for q in range(4):
                here = pl.ds((q * (fields // 2) + pair) * 2 * cycles, 2 * cycles)
                for piece in range(2):
                    lanes = pl.ds(piece * orders + tile * LANES, LANES)
                    lhs[here, lanes] = turned[q][piece].astype(lhs.dtype)

    def one(n, carry):
        wave_copy(n).wait()
        table = held[n].reshape(2 * orders, width)
        product = jnp.dot(lhs[...], table, preferred_element_type=jnp.float32)
        result[n] = product.reshape(4 * fields, cycles, width)
        for q in range(4):
            out_copy(n, q).start()
        return carry

    lax.fori_loop(0, parts, one, 0)
    for n in range(parts):
        for q in range(4):
            out_copy(n, q).wait()


def inverse(y, wave, fields, cycles):
    orders, quarter = wave.shape[1:]
    parts = quarter // (2 * LANES)
    anywhere = pl.BlockSpec(memory_space=pl.ANY)
    return pl.pallas_call(
        inverse_kernel,
        out_shape=jax.ShapeDtypeStruct((fields, cycles, 4 * quarter), jnp.float32),
        in_specs=[pl.BlockSpec(memory_space=pltpu.VMEM), anywhere],
        out_specs=anywhere,
        scratch_shapes=[
            pltpu.VMEM((4 * fields * cycles, 2 * orders), jnp.bfloat16),
            pltpu.VMEM((parts, 2, orders, 2 * LANES), jnp.bfloat16),
            pltpu.VMEM((parts, 4 * fields, cycles, 2 * LANES), jnp.float32),
            pltpu.SemaphoreType.DMA((parts,)),
            pltpu.SemaphoreType.DMA((parts, 4)),
        ],
        compiler_params=pltpu.CompilerParams(vmem_limit_bytes=60 * 2**20),
    )(y, wave)


def local(elevation, legendre, cycle_weight, love_factor, assignment):
    n_cons, n_blk = lax.axis_size("cons"), lax.axis_size("blk")
    y, wave = exchange(elevation, cycle_weight, assignment, love_factor, legendre, n_cons, n_blk)
    return inverse(y, wave, *elevation.shape[:2])


def solution(mesh):
    placed = (P("cons", "blk", None), P("blk", "cons", None), P("blk"), P(), P())
    return jax.shard_map(
        local, mesh=mesh, in_specs=placed, out_specs=P("cons", "blk", None), check_vma=False
    )
```

```python
import functools

import jax
import jax.numpy as jnp
from jax import lax
from jax.experimental import pallas as pl
from jax.experimental.pallas import tpu as pltpu
from jax.sharding import PartitionSpec as P

GROUP = 16
LANES = 128
LEAD = 4
FIN = 4
REL0 = 8
REL1 = 14
RELN = 5
BACK = 4
SLACK = 2
AHEAD = 1
PACE = 2
EARLY = 3
CHUNK_AT = 3
CHUNK_EVERY = 1
CHUNKS = 3
WIDE = 6
VMEM_MIB = 60
WAVE_AT = 5
FINE = 32
MESH = pl.DeviceIdType.MESH


class Plan:
    def __init__(self, n_cons, n_blk, orders_dev, degrees):
        self.n_cons, self.chips = n_cons, n_blk // 2
        self.groups, self.columns = orders_dev // GROUP, degrees // LANES
        counts = [sum(self.width(c, g) for g in range(self.groups)) for c in range(n_cons)]
        self.counts = counts
        moved = [max(0, (counts[c] - counts[n_cons - 1 - c]) // 2) for c in range(n_cons)]
        self.moved = moved
        self.max_tiles = max(counts)
        self.max_moved = max(1, max(moved))
        self.queues = [counts[c] - moved[c] + moved[n_cons - 1 - c] for c in range(n_cons)]
        self.max_queue = max(self.queues)

    def first(self, c, g):
        return (c * self.groups + g) * GROUP // LANES

    def turn(self, c, g):
        return (c * self.groups + g) % (LANES // GROUP)

    def mate(self, c, g):
        return g + LANES // GROUP - 2 * self.turn(c, g)

    def merged(self, c, g):
        return (self.turn(c, g) > LANES // GROUP // 2) & (self.mate(c, g) >= 0)

    def lost(self, c, g):
        place = self.turn(c, g)
        return (place > 0) & (place < LANES // GROUP // 2) & (self.mate(c, g) < self.groups)

    def width(self, c, g):
        return self.columns - self.first(c, g) - (1 if self.lost(c, g) else 0)

    def starts(self, c):
        sums = []
        for k in range(self.groups + 1):
            sums.append(pick(c, [sum(self.width(b, g) for g in range(k)) for b in range(self.n_cons)]))
        return sums[:-1], sums[-1]

    def place(self, c, starts, t):
        starts, tiles = starts
        g, end = 0, starts[1]
        for k in range(1, self.groups):
            after = starts[k + 1] if k + 1 < self.groups else tiles
            g = g + jnp.where(t >= starts[k], 1, 0)
            end = jnp.where(t >= starts[k], after, end)
        return g, self.columns - end + t

    def shift(self, c, spot):
        g, lt = spot
        joined = self.merged(c, g) & (lt == self.first(c, g))
        return jnp.where(joined, LANES - GROUP * self.turn(c, g), 0)


def pick(c, values):
    out = values[-1]
    for k in range(len(values) - 1):
        out = jnp.where(c == k, values[k], out)
    return out


def swap_blocks(tiles):
    count = LANES // GROUP
    block = lax.broadcasted_iota(jnp.int32, tiles[0].shape, len(tiles[0].shape) - 1) // GROUP
    step = count // 2
    while step:
        high = (block // step) % 2 == 1
        new = list(tiles)
        for a in range(count):
            if (a // step) % 2 == 0:
                low_t, high_t = tiles[a], tiles[a + step]
                up = pltpu.roll(high_t, GROUP * step, high_t.ndim - 1)
                down = pltpu.roll(low_t, LANES - GROUP * step, low_t.ndim - 1)
                new[a] = jnp.where(high, up, low_t)
                new[a + step] = jnp.where(high, high_t, down)
        tiles = new
        step //= 2
    return tiles


def sum_kernel(
    plan, elevation, weight, assignment, love, legendre, y, wave, table, table_sem, part, spread_s, whole, sent, taken, back, returned,
    pair_in, acc, given, inward_in, cross_in, coef, fine, waves, wave_sem,
    out, out_sem, field_sem, coarse, near, forward, weights, order, split_s, *sems
):
    (pair_s, pair_r, give_s, give_r, in_s, in_r, cross_s, cross_r, mid_s, out_s, coef_r, ret_s, ret_r, fin_s, fin_r) = sems[:15]
    there_s, there_r, home_s, home_r = sems[15:]
    me, c = lax.axis_index("blk"), lax.axis_index("cons")
    chips, half = plan.chips, part.shape[1] // 2
    n_cons, groups = plan.n_cons, plan.groups
    cycles = weight.shape[0]
    blocks = LANES // GROUP
    folds = cycles // blocks
    fields = elevation.shape[0] // cycles
    rows = 2 * fields
    order_tiles = n_cons * groups // blocks
    all_rows = n_cons * rows
    pairs = plan.columns // 2
    p, core = me // 2, lax.rem(me, 2)
    mid = chips // 2
    left = p < mid
    depth = jnp.where(left, mid - 1 - p, p - mid)
    side = jnp.where(left, 0, 1)
    inner = jnp.where(left, me + 2, me - 2)
    outer = jnp.where(left, me - 2, me + 2)
    partner = me + 1 - 2 * core
    other_c = n_cons - 1 - c
    last = mid - 1

    listed, other_starts = plan.starts(c), plan.starts(other_c)
    starts, tiles = listed
    exports, imports = pick(c, plan.moved), pick(other_c, plan.moved)
    queue = pick(c, plan.queues)

    barrier = pltpu.get_barrier_semaphore()

    def greet(where):
        pl.semaphore_signal(barrier, inc=1, device_id=where, device_id_type=MESH)

    greet({"blk": partner})

    @pl.when(p > 0)
    def _():
        greet({"blk": me - 2})

    @pl.when(p < chips - 1)
    def _():
        greet({"blk": me + 2})

    peers = [lax.rem(c + k, n_cons) for k in range(1, n_cons)]
    for peer in peers:
        greet({"cons": peer})

    def loop(count, body):
        def step(i, carry):
            body(i)
            return carry

        lax.fori_loop(0, count, step, 0)

    def table_copy(g):
        return pltpu.make_async_copy(
            legendre.at[:, pl.ds(pl.multiple_of(g * GROUP, GROUP), GROUP), :], table.at[g], table_sem.at[g]
        )

    def copy(src, dst, send, recv, where):
        return pltpu.make_async_remote_copy(
            src_ref=src, dst_ref=dst, send_sem=send, recv_sem=recv, device_id=where, device_id_type=MESH
        )

    chunk = groups // CHUNKS

    def there_copy(k, h, source):
        peer = peers[k]
        return copy(
            sent.at[pl.ds(peer * groups + h * chunk, chunk)],
            taken.at[source, pl.ds(h * chunk, chunk)],
            there_s.at[k, h],
            there_r.at[source, h],
            {"cons": peer},
        )

    quarter = waves.shape[2]
    period = 4.0 * quarter
    slot_lanes = whole.shape[2]
    per_quarter = quarter // slot_lanes
    base, field_rows = groups - 2 * per_quarter, elevation.shape[0]
    chunk_orders = chunk * GROUP
    half_lanes = n_cons * chunk_orders
    lens = coarse.shape[1]

    def circle(phase):
        phase = phase - jnp.floor(phase * (1.0 / period)) * period
        angle = phase * (2.0 * 3.141592653589793 / period)
        return jnp.cos(angle), jnp.sin(angle)

    def field_copy(i):
        lanes = pl.ds(i * slot_lanes, slot_lanes)
        q, piece = i // per_quarter, i % per_quarter
        here = pl.ds(q % 2 * field_rows, field_rows)
        return pltpu.make_async_copy(
            elevation.at[:, lanes], part.at[base + q // 2 * per_quarter + piece, here, :], field_sem.at[i]
        )

    for i in range(4 * per_quarter):
        field_copy(i).start()
    loop(groups, lambda g: table_copy(g).start())

    def set_weight(j):
        weights[pl.ds(j, 1), :] = jnp.full((1, LANES), weight[j], jnp.float32)

    loop(cycles, set_weight)
    out_row = lax.broadcasted_iota(jnp.int32, order.shape, 0)
    in_row = lax.broadcasted_iota(jnp.int32, order.shape, 1)
    out_slot = out_row // rows * fields + out_row % fields
    wanted = jnp.zeros(order.shape, jnp.int32)
    for k in range(n_cons * fields):
        wanted = jnp.where(out_slot == k, assignment[k], wanted)
    in_field = in_row // rows * fields + in_row % fields
    same = (wanted == in_field) & (out_row // fields % 2 == in_row // fields % 2)
    order[...] = jnp.where(same, 1.0, 0.0).astype(order.dtype)

    def analyse(h):
        def orders_of(shape):
            at_lane = lax.broadcasted_iota(jnp.int32, shape, 1)
            return at_lane // chunk_orders * (groups * GROUP) + h * chunk_orders + at_lane % chunk_orders

        for ref, stride in ((coarse, near.shape[1]), (near, 1)):
            shape = ref.shape[1:]
            lon = lax.broadcasted_iota(jnp.int32, shape, 0) * stride
            ref[0], ref[1] = circle((lon * orders_of(shape)).astype(jnp.float32))

        def make_rows(a, carry):
            cos_a, sin_a = coarse[0, pl.ds(a, 1), :], coarse[1, pl.ds(a, 1), :]
            here = pl.ds(pl.multiple_of(a * near.shape[1], near.shape[1]), near.shape[1])
            forward[here, :half_lanes] = (cos_a * near[0] - sin_a * near[1]).astype(forward.dtype)
            forward[here, half_lanes:] = (-sin_a * near[0] - cos_a * near[1]).astype(forward.dtype)
            return carry

        lax.fori_loop(0, lens, make_rows, 0, unroll=8)
        if h == 0:
            for i in range(4 * per_quarter):
                field_copy(i).wait()
        parts = []
        for q in range(2):
            total = 0.0
            for i in range(per_quarter):
                total = total + jnp.dot(
                    part[base + q * per_quarter + i, : 2 * field_rows, :],
                    forward[i * slot_lanes : (i + 1) * slot_lanes, :],
                    preferred_element_type=jnp.float32,
                )
            for piece in (total[:field_rows], total[field_rows:]):
                parts.append((piece[:, :half_lanes], piece[:, half_lanes:]))
        (re0, im0), (re1, im1), (re2, im2), (re3, im3) = parts
        residue = lax.broadcasted_iota(jnp.int32, re0.shape, 1) % 4
        turn_re = jnp.where(residue == 0, 1.0, jnp.where(residue == 2, -1.0, 0.0))
        turn_im = jnp.where(residue == 1, 1.0, jnp.where(residue == 3, -1.0, 0.0))
        sign = turn_re * turn_re - turn_im * turn_im
        even_re, even_im = re0 + sign * re2, im0 + sign * im2
        odd_re, odd_im = re1 + sign * re3, im1 + sign * im3
        sums = (even_re + turn_re * odd_re + turn_im * odd_im, even_im + turn_re * odd_im - turn_im * odd_re)
        per_tile = LANES // chunk_orders
        for u in range(half_lanes // LANES):
            for piece in range(2):
                for f in range(fields):
                    value = sums[piece][f * cycles : (f + 1) * cycles, u * LANES : (u + 1) * LANES]
                    split_s[u, pl.ds(piece * fields + f, cycles, stride=rows), :] = value * weights[...]
            split = split_s[u].reshape(folds, blocks, rows, LANES)
            swapped = swap_blocks([split[:, k] for k in range(blocks)])
            for k in range(blocks):
                owner = u * per_tile + k // chunk
                sent[owner * groups + h * chunk + k % chunk] = swapped[k].astype(sent.dtype)

    heard = n_cons + jnp.where(p > 0, 1, 0) + jnp.where(p < chips - 1, 1, 0)

    def send_chunk(h):
        analyse(h)
        if h == 0:
            pl.semaphore_wait(barrier, heard)
        for k in range(n_cons - 1):
            there_copy(k, h, c).start()
        for g in range(h * chunk, (h + 1) * chunk):
            taken[c, g] = sent[c * groups + g]

    for h in range(min(EARLY, CHUNKS)):
        send_chunk(h)

    def home_copy(k, g, source):
        return copy(
            back.at[g, peers[k]],
            returned.at[source * groups + g],
            home_s.at[k, g],
            home_r.at[source * groups + g],
            {"cons": peers[k]},
        )

    corner = (0, plan.columns - 1)

    def rows_of(k):
        return pl.ds(pl.multiple_of(k * half, half), half)

    mine, theirs = rows_of(core), rows_of(1 - core)

    def at(ref, spot, rows):
        g, lt = spot
        return ref.at[g, rows, pl.ds(pl.multiple_of(lt * LANES, LANES), LANES)]

    def pair_copy(t, spot):
        return copy(at(part, spot, theirs), pair_in.at[t], pair_s.at[t], pair_r.at[t], {"blk": partner})

    def give_copy(e):
        return copy(given.at[e], acc.at[LEAD + e], give_s.at[e], give_r.at[e], {"cons": other_c})

    def in_copy(q):
        return copy(acc.at[q], inward_in.at[q], in_s.at[q], in_r.at[q], {"blk": inner})

    def cross_copy(q):
        h = q // 2
        return copy(acc.at[q], cross_in.at[h], cross_s.at[h], cross_r.at[h], {"blk": inner})

    def mid_copy(q):
        return copy(coef.at[q], coef.at[q], mid_s.at[q // 2], coef_r.at[q], {"blk": inner})

    def out_copy(q):
        return copy(coef.at[q], coef.at[q], out_s.at[q], coef_r.at[q], {"blk": outer})

    def ret_copy(q, e, spot):
        return copy(coef.at[q], at(whole, spot, mine), ret_s.at[e], ret_r.at[e], {"cons": other_c})

    def fin_copy(t, spot):
        part_of = at(whole, spot, mine)
        return copy(part_of, part_of, fin_s.at[t], fin_r.at[t], {"blk": partner})

    def add(x, y):
        return x.astype(jnp.float32) + y.astype(jnp.float32)

    def is_import(q):
        return (q >= LEAD) & (q < LEAD + imports)

    def tile_of(q):
        return q + jnp.minimum(q + 1, exports) - jnp.where(q >= LEAD, imports, 0)

    def first_of(g):
        return (c * groups + g) * GROUP // LANES

    def start_of(g):
        out = tiles
        for k in range(groups - 1, -1, -1):
            out = jnp.where(g == k, starts[k], out)
        return out

    def lane_pair(lp):
        return pl.ds(pl.multiple_of(lp * 2 * LANES, 2 * LANES), 2 * LANES)

    def span(begin, end, body):
        def step(i, carry):
            body(i)
            return carry

        lax.fori_loop(begin, end, step, 0)

    lane = lax.broadcasted_iota(jnp.int32, (all_rows, folds * LANES), 1) % GROUP

    def clear(g):
        first = first_of(g)

        def one(lt):
            whole[g, :, pl.ds(pl.multiple_of(lt * LANES, LANES), LANES)] = jnp.zeros((2 * half, LANES), whole.dtype)

        span(first // 2 * 2, first, one)

    loop(groups, clear)

    def produce(g):
        @pl.when(lax.rem(g, chunk) == 0)
        def _():
            for source in range(n_cons):

                @pl.when(c != source)
                def _():
                    there_copy(0, g // chunk, source).wait_recv()

        table_copy(g).wait()
        lists = [
            jnp.concatenate([taken[source, g, fold] for source in range(n_cons)], axis=0) for fold in range(folds)
        ]
        gathered = jnp.concatenate(lists, axis=1)
        ordered = jnp.dot(order[...], gathered, preferred_element_type=jnp.float32)
        for m in range(GROUP):
            spread_s[pl.ds(m * all_rows, all_rows), :] = jnp.where(lane == m, ordered, 0.0).astype(spread_s.dtype)

        def one(lp):
            values = table[g, :, :, lane_pair(lp)].reshape(cycles * GROUP, 2 * LANES)
            part[g, :, lane_pair(lp)] = jnp.dot(
                spread_s[...], values, preferred_element_type=jnp.float32
            ).astype(part.dtype)

        span(first_of(g) // 2, pairs, one)

        @pl.when(plan.merged(c, g))
        def _():
            here = pl.ds(pl.multiple_of(first_of(g) * LANES, LANES), LANES)
            moved = LANES - GROUP * plan.turn(c, g)
            lanes = lax.broadcasted_iota(jnp.int32, (2 * half, LANES), 1)
            low = pltpu.roll(part[g, :, here].astype(jnp.float32), moved, 1)
            high = part[plan.mate(c, g), :, here].astype(jnp.float32)
            part[g, :, here] = jnp.where(lanes < moved, low, high).astype(part.dtype)

        span(start_of(g), start_of(g + 1), lambda t: pair_copy(t, plan.place(c, listed, t)).start())

    width = folds * LANES
    order_lane = lax.broadcasted_iota(jnp.int32, (rows, LANES), 1) % GROUP

    def restore(g):
        def take(t):
            fin_copy(t, corner).wait_recv()

        span(start_of(g), start_of(g + 1), take)
        joined = plan.merged(c, g)

        @pl.when(joined)
        def _():
            here = pl.ds(pl.multiple_of(first_of(g) * LANES, LANES), LANES)
            fin_copy(start_of(g), corner).wait_send()
            both = whole[g, :, here]
            whole[plan.mate(c, g), :, here] = both
            back_by = GROUP * plan.turn(c, g)
            whole[g, :, here] = pltpu.roll(both.astype(jnp.float32), back_by, 1).astype(whole.dtype)

        count = jnp.where(plan.lost(c, g), 0, jnp.where(joined, 2, 1))
        span(0, count, lambda n: synthesise(jnp.where(n == 0, g, plan.mate(c, g))))

    def synthesise(g):
        def one(lp, total):
            values = table[g, :, :, lane_pair(lp)].reshape(cycles * GROUP, 2 * LANES)
            full = lax.dot_general(
                whole[g, :, lane_pair(lp)], values, (((1,), (1,)), ((), ())), preferred_element_type=jnp.float32
            )
            wide = lax.broadcasted_iota(jnp.int32, (all_rows, width), 1) % GROUP
            for m in range(GROUP):
                total = total + jnp.where(wide == m, full[m * all_rows : (m + 1) * all_rows], 0.0)
            return total

        total = lax.fori_loop(first_of(g) // 2, pairs, one, jnp.zeros((all_rows, width), jnp.float32))
        zero_order = (c * groups + g) * GROUP + order_lane == 0
        factor = jnp.where(zero_order, 1.0, 2.0)
        for peer in range(n_cons):
            for fold in range(folds):
                piece = total[peer * rows : (peer + 1) * rows, fold * LANES : (fold + 1) * LANES]
                back[g, peer, fold] = (piece * factor).astype(back.dtype)
        for k in range(n_cons - 1):
            home_copy(k, g, c).start()
        returned[c * groups + g] = back[g, c]

    def give(e):
        spot = plan.place(c, listed, 2 * e)
        pair_copy(2 * e, spot).wait_recv()
        given[e] = add(at(part, spot, mine)[...], pair_in[2 * e]).astype(given.dtype)
        give_copy(e).start()

    def gather(q):
        native = jnp.logical_not(is_import(q))

        @pl.when(native)
        def _():
            t = tile_of(q)
            spot = plan.place(c, listed, t)
            pair_copy(t, spot).wait_recv()
            acc[q] = add(at(part, spot, mine)[...], pair_in[t]).astype(acc.dtype)

        @pl.when(is_import(q))
        def _():
            give_copy(q - LEAD).wait_recv()

        @pl.when(depth < last)
        def _():
            in_copy(q).wait_recv()
            acc[q] = add(acc[q], inward_in[q]).astype(acc.dtype)

        @pl.when(depth > 0)
        def _():
            in_copy(q).start()

        @pl.when((depth == 0) & (lax.rem(q, 2) != side))
        def _():
            cross_copy(q).start()

    def spread(q):
        @pl.when(depth < last)
        def _():
            out_copy(q).start()

        @pl.when(is_import(q))
        def _():
            e = q - LEAD
            ret_copy(q, e, plan.place(other_c, other_starts, 2 * e)).start()

        @pl.when(jnp.logical_not(is_import(q)))
        def _():
            t = tile_of(q)
            spot = plan.place(c, listed, t)
            at(whole, spot, mine)[...] = coef[q]
            fin_copy(t, spot).start()

    def finish(q):
        @pl.when((depth == 0) & (lax.rem(q, 2) == side))
        def _():
            cross_copy(q).wait_recv()
            own = plan.place(c, listed, tile_of(q))
            lent = plan.place(other_c, other_starts, 2 * (q - LEAD))
            lt = jnp.where(is_import(q), lent[1], own[1])
            moved = jnp.where(is_import(q), plan.shift(other_c, lent), plan.shift(c, own))
            scale = jnp.broadcast_to(love[pl.ds(lt, 1), :], (8, LANES))
            ahead_of = lax.broadcasted_iota(jnp.int32, (8, LANES), 1) < moved
            scale = jnp.where(ahead_of, pltpu.roll(scale, moved, 1), scale)[:1]
            total = add(acc[q], cross_in[q // 2]) * scale
            coef[q] = total.astype(coef.dtype)
            mid_copy(q).start()
            spread(q)

    def relay(q):
        @pl.when((depth > 0) | (lax.rem(q, 2) != side))
        def _():
            out_copy(q).wait_recv()
            spread(q)

    def take_back(e):
        spot = plan.place(c, listed, 2 * e)
        ret_copy(0, e, spot).wait_recv()
        fin_copy(2 * e, spot).start()

    relay_gap = jnp.where(depth == 0, REL0, REL1 + (depth - 1) * RELN)
    back_gap = LEAD + relay_gap + BACK

    def ready(g):
        t = start_of(g + 1) - 1
        q = jnp.where(t < 2 * exports, t // 2, t - exports) + jnp.where(t >= LEAD, imports, 0)
        e = jnp.where(start_of(g) < 2 * exports, jnp.minimum(t // 2, exports - 1) + back_gap, 0)
        return jnp.maximum(q + relay_gap, e) + SLACK

    fine_rows = fine.shape[1]
    wave_blocks = waves.shape[1] // fine_rows

    def wave_copy(b):
        rows_here = pl.ds(pl.multiple_of(b * fine_rows, fine_rows), fine_rows)
        return pltpu.make_async_copy(waves.at[:, rows_here, :], wave.at[:, rows_here, :], wave_sem.at[b])

    def turn(row):
        lon = lax.broadcasted_iota(jnp.int32, row.shape, 1).astype(jnp.float32)
        return circle(row.astype(jnp.float32) * lon)

    def make_fine():
        fine[0], fine[1] = turn(lax.broadcasted_iota(jnp.int32, (fine_rows, quarter), 0))

    def make_wave(b):
        cos_a, sin_a = turn(jnp.full((8, quarter), b * fine_rows, jnp.int32))
        cos_a, sin_a = cos_a[:1], sin_a[:1]
        here = pl.ds(pl.multiple_of(b * fine_rows, fine_rows), fine_rows)
        waves[0, here, :] = (cos_a * fine[0] - sin_a * fine[1]).astype(waves.dtype)
        waves[1, here, :] = (-sin_a * fine[0] - cos_a * fine[1]).astype(waves.dtype)
        wave_copy(b).start()

    for g in range(AHEAD):
        produce(g)

    def step(i, done):
        @pl.when(i < exports)
        def _():
            give(i)

        @pl.when(i < queue)
        def _():
            gather(i)

        q = i - FIN

        @pl.when((q >= 0) & (q < queue))
        def _():
            finish(q)

        r = i - relay_gap

        @pl.when((r >= 0) & (r < queue))
        def _():
            relay(r)

        e = i - back_gap

        @pl.when((e >= 0) & (e < exports))
        def _():
            take_back(e)

        for h in range(EARLY, CHUNKS):

            @pl.when(i == CHUNK_AT + (h - EARLY) * CHUNK_EVERY)
            def _(h=h):
                send_chunk(h)

        @pl.when(i == WAVE_AT)
        def _():
            make_fine()

        b = i - WAVE_AT - 1

        @pl.when((b >= 0) & (b < wave_blocks))
        def _():
            make_wave(b)

        ahead = AHEAD + i // PACE

        @pl.when((lax.rem(i, PACE) == 0) & (ahead < groups))
        def _():
            produce(ahead)

        now = (done < groups) & (i >= ready(done)) & ((lax.rem(i, PACE) > 0) | (i > PACE * groups))

        @pl.when(now)
        def _():
            restore(done)

        return done + jnp.where(now, 1, 0)

    count = plan.max_queue + LEAD + REL1 + mid * RELN + BACK
    done = lax.fori_loop(0, count, step, 0)
    span(done, groups, restore)

    def drain_tile(t):
        pair_copy(t, corner).wait_send()

    loop(tiles, drain_tile)

    def drain_group(g):
        begin = start_of(g) + jnp.where(plan.merged(c, g), 1, 0)
        span(begin, start_of(g + 1), lambda t: fin_copy(t, corner).wait_send())

    loop(groups, drain_group)
    loop(exports, lambda e: give_copy(e).wait_send())

    def drain_queue(q):
        @pl.when(depth > 0)
        def _():
            in_copy(q).wait_send()

        @pl.when((depth == 0) & (lax.rem(q, 2) != side))
        def _():
            cross_copy(q).wait_send()

        @pl.when((depth == 0) & (lax.rem(q, 2) == side))
        def _():
            mid_copy(q).wait_send()

        @pl.when(depth < last)
        def _():
            out_copy(q).wait_send()

        @pl.when(is_import(q))
        def _():
            e = q - LEAD
            ret_copy(q, e, corner).wait_send()

    loop(queue, drain_queue)
    loop(wave_blocks, lambda b: wave_copy(b).wait())
    for k in range(n_cons - 1):
        for h in range(CHUNKS):
            there_copy(k, h, c).wait_send()

        loop(groups, lambda g, k=k: home_copy(k, g, c).wait_send())

    def tile_rows(tile):
        return pl.ds(pl.multiple_of(tile * cycles * rows, 8), cycles * rows)

    def y_copy(tile):
        return pltpu.make_async_copy(out.at[tile_rows(tile), :], y.at[tile_rows(tile), :], out_sem.at[tile])

    def unpack(tile):
        def heard_from(k):
            index = tile * blocks + k

            @pl.when(index // groups != c)
            def _():
                home_copy(0, lax.rem(index, groups), index // groups).wait_recv()

        loop(blocks, heard_from)

        swapped = swap_blocks([returned[tile * blocks + k].astype(jnp.float32) for k in range(blocks)])
        merged = jnp.stack(swapped, axis=1).reshape(cycles * rows, LANES)
        out[tile_rows(tile), :] = merged
        y_copy(tile).start()

    latest = [max(k % groups for k in range(t * blocks, (t + 1) * blocks)) for t in range(order_tiles)]
    turns = sorted(range(order_tiles), key=lambda t: latest[t])
    loop(order_tiles, lambda n: unpack(pick(n, turns)))
    loop(order_tiles, lambda t: y_copy(t).wait())


def exchange(elevation, weight, assignment, love, legendre, n_cons, n_blk):
    cycles, orders_dev, degrees = legendre.shape
    fields, _, longitudes = elevation.shape
    quarter, rows = longitudes // 4, 2 * fields
    all_rows, orders = n_cons * rows, n_cons * orders_dev
    plan = Plan(n_cons, n_blk, orders_dev, degrees)
    groups, folds = plan.groups, cycles * GROUP // LANES
    half = (GROUP * all_rows // 2, LANES)
    kind = elevation.dtype
    tiles, queue, moved = plan.max_tiles, plan.max_queue, plan.max_moved
    halves = (queue + 1) // 2
    sems = [(n,) for n in [tiles] * 2 + [moved] * 2 + [queue] * 2 + [halves] * 2 + [halves, queue, queue] + [moved] * 2 + [tiles] * 2]
    sems += [(n_cons - 1, CHUNKS), (n_cons, CHUNKS), (n_cons - 1, groups), (n_cons * groups,)]
    lane_tiles = (folds, rows, LANES)
    waves = (2, orders, quarter)
    chunk_lanes = orders // CHUNKS
    vmem = pl.BlockSpec(memory_space=pltpu.VMEM)
    scalars = pl.BlockSpec(memory_space=pltpu.SMEM)
    anywhere = pl.BlockSpec(memory_space=pl.ANY)
    return pl.pallas_call(
        functools.partial(sum_kernel, plan),
        out_shape=[
            jax.ShapeDtypeStruct((orders // LANES * cycles * rows, LANES), jnp.float32),
            jax.ShapeDtypeStruct(waves, kind),
        ],
        in_specs=[anywhere, scalars, scalars, vmem, anywhere],
        out_specs=[anywhere, anywhere],
        scratch_shapes=[
            pltpu.VMEM((groups, cycles, GROUP, degrees), kind),
            pltpu.SemaphoreType.DMA((groups,)),
            pltpu.VMEM((groups, GROUP * all_rows, degrees), kind),
            pltpu.VMEM((GROUP * all_rows, folds * LANES), kind),
            pltpu.VMEM((groups, GROUP * all_rows, degrees), kind),
            pltpu.VMEM((n_cons * groups,) + lane_tiles, kind),
            pltpu.VMEM((n_cons, groups) + lane_tiles, kind),
            pltpu.VMEM((groups, n_cons) + lane_tiles, kind),
            pltpu.VMEM((n_cons * groups,) + lane_tiles, kind),
            pltpu.VMEM((tiles,) + half, kind),
            pltpu.VMEM((queue,) + half, kind),
            pltpu.VMEM((moved,) + half, kind),
            pltpu.VMEM((queue,) + half, kind),
            pltpu.VMEM((halves,) + half, kind),
            pltpu.VMEM((queue,) + half, kind),
            pltpu.VMEM((2, FINE, quarter), jnp.float32),
            pltpu.VMEM(waves, kind),
            pltpu.SemaphoreType.DMA((waves[1] // FINE,)),
            pltpu.VMEM((orders // LANES * cycles * rows, LANES), jnp.float32),
            pltpu.SemaphoreType.DMA((orders // LANES,)),
            pltpu.SemaphoreType.DMA((longitudes // degrees,)),
            pltpu.VMEM((2, quarter // FINE, chunk_lanes), jnp.float32),
            pltpu.VMEM((2, FINE, chunk_lanes), jnp.float32),
            pltpu.VMEM((quarter, 2 * chunk_lanes), kind),
            pltpu.VMEM((cycles, LANES), jnp.float32),
            pltpu.VMEM((all_rows, all_rows), kind),
            pltpu.VMEM((chunk_lanes // LANES, cycles * rows, LANES), jnp.float32),
        ]
        + [pltpu.SemaphoreType.DMA(n) for n in sems],
        compiler_params=pltpu.CompilerParams(
            collective_id=0, has_side_effects=True, vmem_limit_bytes=VMEM_MIB * 2**20
        ),
    )(
        elevation.reshape(fields * cycles, longitudes),
        weight,
        assignment,
        love.reshape(degrees // LANES, LANES),
        legendre,
    )


def inverse_kernel(given, wave, loading, y, lhs, held, result, y_sem, wave_sem, out_sem):
    fields, cycles, longitudes = loading.shape
    quarter, tiles = longitudes // 4, lhs.shape[1] // LANES
    width, parts = held.shape[3], held.shape[0]
    rows = 2 * fields

    def columns(n):
        return pl.ds(pl.multiple_of(n * width, width), width)

    def wave_copy(n):
        return pltpu.make_async_copy(wave.at[:, :, columns(n)], held.at[n], wave_sem.at[n])

    def out_copy(n, q):
        place = pl.ds(pl.multiple_of(q * quarter + n * width, width), width)
        return pltpu.make_async_copy(
            result.at[n, pl.ds(q * fields, fields)], loading.at[:, :, place], out_sem.at[n, q]
        )

    def y_copy(tile):
        here = pl.ds(tile * cycles * rows, cycles * rows)
        return pltpu.make_async_copy(given.at[here, :], y.at[here, :], y_sem.at[tile])

    for tile in range(tiles // 2):
        y_copy(tile).start()
    for n in range(parts):
        wave_copy(n).start()
    residue = lax.broadcasted_iota(jnp.int32, (2 * cycles, LANES), 1) % 4
    turn_re = jnp.where(residue == 0, 1.0, jnp.where(residue == 2, -1.0, 0.0))
    turn_im = jnp.where(residue == 1, 1.0, jnp.where(residue == 3, -1.0, 0.0))
    sign = turn_re * turn_re - turn_im * turn_im
    orders = tiles * LANES // 2
    for tile in range(tiles // 2):
        y_copy(tile).wait()

        def load(piece, pair):
            at = [tile * cycles * rows + piece * fields + 2 * pair + k for k in range(2)]
            return jnp.concatenate([y[pl.ds(a, cycles, stride=rows), :] for a in at], axis=0)

        for pair in range(fields // 2):
            re, im = load(0, pair), load(1, pair)
            turned = (
                (re, im),
                (turn_re * re - turn_im * im, turn_re * im + turn_im * re),
                (sign * re, sign * im),
                (turn_re * re + turn_im * im, turn_re * im - turn_im * re),
            )
            for q in range(4):
                here = pl.ds((q * (fields // 2) + pair) * 2 * cycles, 2 * cycles)
                for piece in range(2):
                    lanes = pl.ds(piece * orders + tile * LANES, LANES)
                    lhs[here, lanes] = turned[q][piece].astype(lhs.dtype)

    def one(n, carry):
        wave_copy(n).wait()
        table = held[n].reshape(2 * orders, width)
        product = jnp.dot(lhs[...], table, preferred_element_type=jnp.float32)
        result[n] = product.reshape(4 * fields, cycles, width)
        for q in range(4):
            out_copy(n, q).start()
        return carry

    lax.fori_loop(0, parts, one, 0)
    for n in range(parts):
        for q in range(4):
            out_copy(n, q).wait()


def inverse(y, wave, fields, cycles):
    orders, quarter = wave.shape[1:]
    width = WIDE * LANES
    parts = quarter // width
    anywhere = pl.BlockSpec(memory_space=pl.ANY)
    return pl.pallas_call(
        inverse_kernel,
        out_shape=jax.ShapeDtypeStruct((fields, cycles, 4 * quarter), jnp.float32),
        in_specs=[anywhere, anywhere],
        out_specs=anywhere,
        scratch_shapes=[
            pltpu.VMEM(y.shape, jnp.float32),
            pltpu.VMEM((4 * fields * cycles, 2 * orders), jnp.bfloat16),
            pltpu.VMEM((parts, 2, orders, width), jnp.bfloat16),
            pltpu.VMEM((parts, 4 * fields, cycles, width), jnp.float32),
            pltpu.SemaphoreType.DMA((orders // LANES,)),
            pltpu.SemaphoreType.DMA((parts,)),
            pltpu.SemaphoreType.DMA((parts, 4)),
        ],
        compiler_params=pltpu.CompilerParams(vmem_limit_bytes=60 * 2**20),
    )(y, wave)


def local(elevation, legendre, cycle_weight, love_factor, assignment):
    n_cons, n_blk = lax.axis_size("cons"), lax.axis_size("blk")
    y, wave = exchange(elevation, cycle_weight, assignment, love_factor, legendre, n_cons, n_blk)
    return inverse(y, wave, *elevation.shape[:2])


def solution(mesh):
    placed = (P("cons", "blk", None), P("blk", "cons", None), P("blk"), P(), P())
    return jax.shard_map(
        local, mesh=mesh, in_specs=placed, out_specs=P("cons", "blk", None), check_vma=False
    )
```

```python
import functools

import jax
import jax.numpy as jnp
from jax import lax
from jax.experimental import pallas as pl
from jax.experimental.pallas import tpu as pltpu
from jax.sharding import PartitionSpec as P

GROUP = 16
LANES = 128
LEAD = 4
FIN = 4
REL0 = 8
REL1 = 14
RELN = 5
BACK = 3
SLACK = 1
AHEAD = 1
PACE = 2
EARLY = 3
CHUNK_AT = 3
CHUNK_EVERY = 1
CHUNKS = 3
WIDE = 6
VMEM_MIB = 60
WAVE_AT = 5
FINE = 32
MESH = pl.DeviceIdType.MESH


class Plan:
    def __init__(self, n_cons, n_blk, orders_dev, degrees):
        self.n_cons, self.chips = n_cons, n_blk // 2
        self.groups, self.columns = orders_dev // GROUP, degrees // LANES
        counts = [sum(self.width(c, g) for g in range(self.groups)) for c in range(n_cons)]
        self.counts = counts
        moved = [max(0, (counts[c] - counts[n_cons - 1 - c]) // 2) for c in range(n_cons)]
        self.moved = moved
        self.max_tiles = max(counts)
        self.max_moved = max(1, max(moved))
        self.queues = [counts[c] - moved[c] + moved[n_cons - 1 - c] for c in range(n_cons)]
        self.max_queue = max(self.queues)

    def first(self, c, g):
        return (c * self.groups + g) * GROUP // LANES

    def turn(self, c, g):
        return (c * self.groups + g) % (LANES // GROUP)

    def mate(self, c, g):
        return g + LANES // GROUP - 2 * self.turn(c, g)

    def merged(self, c, g):
        return (self.turn(c, g) > LANES // GROUP // 2) & (self.mate(c, g) >= 0)

    def lost(self, c, g):
        place = self.turn(c, g)
        return (place > 0) & (place < LANES // GROUP // 2) & (self.mate(c, g) < self.groups)

    def width(self, c, g):
        return self.columns - self.first(c, g) - (1 if self.lost(c, g) else 0)

    def starts(self, c):
        sums = []
        for k in range(self.groups + 1):
            sums.append(pick(c, [sum(self.width(b, g) for g in range(k)) for b in range(self.n_cons)]))
        return sums[:-1], sums[-1]

    def place(self, c, starts, t):
        starts, tiles = starts
        g, end = 0, starts[1]
        for k in range(1, self.groups):
            after = starts[k + 1] if k + 1 < self.groups else tiles
            g = g + jnp.where(t >= starts[k], 1, 0)
            end = jnp.where(t >= starts[k], after, end)
        return g, self.columns - end + t

    def shift(self, c, spot):
        g, lt = spot
        joined = self.merged(c, g) & (lt == self.first(c, g))
        return jnp.where(joined, LANES - GROUP * self.turn(c, g), 0)


def pick(c, values):
    out = values[-1]
    for k in range(len(values) - 1):
        out = jnp.where(c == k, values[k], out)
    return out


def swap_blocks(tiles):
    count = LANES // GROUP
    block = lax.broadcasted_iota(jnp.int32, tiles[0].shape, len(tiles[0].shape) - 1) // GROUP
    step = count // 2
    while step:
        high = (block // step) % 2 == 1
        new = list(tiles)
        for a in range(count):
            if (a // step) % 2 == 0:
                low_t, high_t = tiles[a], tiles[a + step]
                up = pltpu.roll(high_t, GROUP * step, high_t.ndim - 1)
                down = pltpu.roll(low_t, LANES - GROUP * step, low_t.ndim - 1)
                new[a] = jnp.where(high, up, low_t)
                new[a + step] = jnp.where(high, high_t, down)
        tiles = new
        step //= 2
    return tiles


def sum_kernel(
    plan, elevation, weight, assignment, love, legendre, y, wave, table, table_sem, part, spread_s, whole, sent, taken, back, returned,
    pair_in, acc, given, inward_in, cross_in, coef, fine, waves, wave_sem,
    out, out_sem, field_sem, coarse, near, forward, weights, order, split_s, *sems
):
    (pair_s, pair_r, give_s, give_r, in_s, in_r, cross_s, cross_r, mid_s, out_s, coef_r, ret_s, ret_r, fin_s, fin_r) = sems[:15]
    there_s, there_r, home_s, home_r = sems[15:]
    me, c = lax.axis_index("blk"), lax.axis_index("cons")
    chips, half = plan.chips, part.shape[1] // 2
    n_cons, groups = plan.n_cons, plan.groups
    cycles = weight.shape[0]
    blocks = LANES // GROUP
    folds = cycles // blocks
    fields = elevation.shape[0] // cycles
    rows = 2 * fields
    order_tiles = n_cons * groups // blocks
    all_rows = n_cons * rows
    pairs = plan.columns // 2
    p, core = me // 2, lax.rem(me, 2)
    mid = chips // 2
    left = p < mid
    depth = jnp.where(left, mid - 1 - p, p - mid)
    side = jnp.where(left, 0, 1)
    inner = jnp.where(left, me + 2, me - 2)
    outer = jnp.where(left, me - 2, me + 2)
    partner = me + 1 - 2 * core
    other_c = n_cons - 1 - c
    last = mid - 1

    listed, other_starts = plan.starts(c), plan.starts(other_c)
    starts, tiles = listed
    exports, imports = pick(c, plan.moved), pick(other_c, plan.moved)
    queue = pick(c, plan.queues)

    barrier = pltpu.get_barrier_semaphore()

    def greet(where):
        pl.semaphore_signal(barrier, inc=1, device_id=where, device_id_type=MESH)

    greet({"blk": partner})

    @pl.when(p > 0)
    def _():
        greet({"blk": me - 2})

    @pl.when(p < chips - 1)
    def _():
        greet({"blk": me + 2})

    peers = [lax.rem(c + k, n_cons) for k in range(1, n_cons)]
    for peer in peers:
        greet({"cons": peer})

    def loop(count, body):
        def step(i, carry):
            body(i)
            return carry

        lax.fori_loop(0, count, step, 0)

    def table_copy(g):
        return pltpu.make_async_copy(
            legendre.at[:, pl.ds(pl.multiple_of(g * GROUP, GROUP), GROUP), :], table.at[g], table_sem.at[g]
        )

    def copy(src, dst, send, recv, where):
        return pltpu.make_async_remote_copy(
            src_ref=src, dst_ref=dst, send_sem=send, recv_sem=recv, device_id=where, device_id_type=MESH
        )

    chunk = groups // CHUNKS

    def there_copy(k, h, source):
        peer = peers[k]
        return copy(
            sent.at[pl.ds(peer * groups + h * chunk, chunk)],
            taken.at[source, pl.ds(h * chunk, chunk)],
            there_s.at[k, h],
            there_r.at[source, h],
            {"cons": peer},
        )

    quarter = waves.shape[2]
    period = 4.0 * quarter
    slot_lanes = whole.shape[2]
    per_quarter = quarter // slot_lanes
    base, field_rows = groups - 2 * per_quarter, elevation.shape[0]
    chunk_orders = chunk * GROUP
    half_lanes = n_cons * chunk_orders
    lens = coarse.shape[1]

    def circle(phase):
        phase = phase - jnp.floor(phase * (1.0 / period)) * period
        angle = phase * (2.0 * 3.141592653589793 / period)
        return jnp.cos(angle), jnp.sin(angle)

    def field_copy(i):
        lanes = pl.ds(i * slot_lanes, slot_lanes)
        q, piece = i // per_quarter, i % per_quarter
        here = pl.ds(q % 2 * field_rows, field_rows)
        return pltpu.make_async_copy(
            elevation.at[:, lanes], part.at[base + q // 2 * per_quarter + piece, here, :], field_sem.at[i]
        )

    for i in range(4 * per_quarter):
        field_copy(i).start()
    loop(groups, lambda g: table_copy(g).start())

    def set_weight(j):
        weights[pl.ds(j, 1), :] = jnp.full((1, LANES), weight[j], jnp.float32)

    loop(cycles, set_weight)
    out_row = lax.broadcasted_iota(jnp.int32, order.shape, 0)
    in_row = lax.broadcasted_iota(jnp.int32, order.shape, 1)
    out_slot = out_row // rows * fields + out_row % fields
    wanted = jnp.zeros(order.shape, jnp.int32)
    for k in range(n_cons * fields):
        wanted = jnp.where(out_slot == k, assignment[k], wanted)
    in_field = in_row // rows * fields + in_row % fields
    same = (wanted == in_field) & (out_row // fields % 2 == in_row // fields % 2)
    order[...] = jnp.where(same, 1.0, 0.0).astype(order.dtype)

    def analyse(h):
        def orders_of(shape):
            at_lane = lax.broadcasted_iota(jnp.int32, shape, 1)
            return at_lane // chunk_orders * (groups * GROUP) + h * chunk_orders + at_lane % chunk_orders

        for ref, stride in ((coarse, near.shape[1]), (near, 1)):
            shape = ref.shape[1:]
            lon = lax.broadcasted_iota(jnp.int32, shape, 0) * stride
            ref[0], ref[1] = circle((lon * orders_of(shape)).astype(jnp.float32))

        def make_rows(a, carry):
            cos_a, sin_a = coarse[0, pl.ds(a, 1), :], coarse[1, pl.ds(a, 1), :]
            here = pl.ds(pl.multiple_of(a * near.shape[1], near.shape[1]), near.shape[1])
            forward[here, :half_lanes] = (cos_a * near[0] - sin_a * near[1]).astype(forward.dtype)
            forward[here, half_lanes:] = (-sin_a * near[0] - cos_a * near[1]).astype(forward.dtype)
            return carry

        lax.fori_loop(0, lens, make_rows, 0, unroll=8)
        if h == 0:
            for i in range(4 * per_quarter):
                field_copy(i).wait()
        parts = []
        for q in range(2):
            total = 0.0
            for i in range(per_quarter):
                total = total + jnp.dot(
                    part[base + q * per_quarter + i, : 2 * field_rows, :],
                    forward[i * slot_lanes : (i + 1) * slot_lanes, :],
                    preferred_element_type=jnp.float32,
                )
            for piece in (total[:field_rows], total[field_rows:]):
                parts.append((piece[:, :half_lanes], piece[:, half_lanes:]))
        (re0, im0), (re1, im1), (re2, im2), (re3, im3) = parts
        residue = lax.broadcasted_iota(jnp.int32, re0.shape, 1) % 4
        turn_re = jnp.where(residue == 0, 1.0, jnp.where(residue == 2, -1.0, 0.0))
        turn_im = jnp.where(residue == 1, 1.0, jnp.where(residue == 3, -1.0, 0.0))
        sign = turn_re * turn_re - turn_im * turn_im
        even_re, even_im = re0 + sign * re2, im0 + sign * im2
        odd_re, odd_im = re1 + sign * re3, im1 + sign * im3
        sums = (even_re + turn_re * odd_re + turn_im * odd_im, even_im + turn_re * odd_im - turn_im * odd_re)
        per_tile = LANES // chunk_orders
        for u in range(half_lanes // LANES):
            for piece in range(2):
                for f in range(fields):
                    value = sums[piece][f * cycles : (f + 1) * cycles, u * LANES : (u + 1) * LANES]
                    split_s[u, pl.ds(piece * fields + f, cycles, stride=rows), :] = value * weights[...]
            split = split_s[u].reshape(folds, blocks, rows, LANES)
            swapped = swap_blocks([split[:, k] for k in range(blocks)])
            for k in range(blocks):
                owner = u * per_tile + k // chunk
                sent[owner * groups + h * chunk + k % chunk] = swapped[k].astype(sent.dtype)

    heard = n_cons + jnp.where(p > 0, 1, 0) + jnp.where(p < chips - 1, 1, 0)

    def send_chunk(h):
        analyse(h)
        if h == 0:
            pl.semaphore_wait(barrier, heard)
        for k in range(n_cons - 1):
            there_copy(k, h, c).start()
        for g in range(h * chunk, (h + 1) * chunk):
            taken[c, g] = sent[c * groups + g]

    for h in range(min(EARLY, CHUNKS)):
        send_chunk(h)

    def home_copy(k, g, source):
        return copy(
            back.at[g, peers[k]],
            returned.at[source * groups + g],
            home_s.at[k, g],
            home_r.at[source * groups + g],
            {"cons": peers[k]},
        )

    corner = (0, plan.columns - 1)

    def rows_of(k):
        return pl.ds(pl.multiple_of(k * half, half), half)

    mine, theirs = rows_of(core), rows_of(1 - core)

    def at(ref, spot, rows):
        g, lt = spot
        return ref.at[g, rows, pl.ds(pl.multiple_of(lt * LANES, LANES), LANES)]

    def pair_copy(t, spot):
        return copy(at(part, spot, theirs), pair_in.at[t], pair_s.at[t], pair_r.at[t], {"blk": partner})

    def give_copy(e):
        return copy(given.at[e], acc.at[LEAD + e], give_s.at[e], give_r.at[e], {"cons": other_c})

    def in_copy(q):
        return copy(acc.at[q], inward_in.at[q], in_s.at[q], in_r.at[q], {"blk": inner})

    def cross_copy(q):
        h = q // 2
        return copy(acc.at[q], cross_in.at[h], cross_s.at[h], cross_r.at[h], {"blk": inner})

    def mid_copy(q):
        return copy(coef.at[q], coef.at[q], mid_s.at[q // 2], coef_r.at[q], {"blk": inner})

    def out_copy(q):
        return copy(coef.at[q], coef.at[q], out_s.at[q], coef_r.at[q], {"blk": outer})

    def ret_copy(q, e, spot):
        return copy(coef.at[q], at(whole, spot, mine), ret_s.at[e], ret_r.at[e], {"cons": other_c})

    def fin_copy(t, spot):
        part_of = at(whole, spot, mine)
        return copy(part_of, part_of, fin_s.at[t], fin_r.at[t], {"blk": partner})

    def add(x, y):
        return x.astype(jnp.float32) + y.astype(jnp.float32)

    def is_import(q):
        return (q >= LEAD) & (q < LEAD + imports)

    def tile_of(q):
        return q + jnp.minimum(q + 1, exports) - jnp.where(q >= LEAD, imports, 0)

    def first_of(g):
        return (c * groups + g) * GROUP // LANES

    def start_of(g):
        out = tiles
        for k in range(groups - 1, -1, -1):
            out = jnp.where(g == k, starts[k], out)
        return out

    def lane_pair(lp):
        return pl.ds(pl.multiple_of(lp * 2 * LANES, 2 * LANES), 2 * LANES)

    def span(begin, end, body):
        def step(i, carry):
            body(i)
            return carry

        lax.fori_loop(begin, end, step, 0)

    lane = lax.broadcasted_iota(jnp.int32, (all_rows, folds * LANES), 1) % GROUP

    def clear(g):
        first = first_of(g)

        def one(lt):
            whole[g, :, pl.ds(pl.multiple_of(lt * LANES, LANES), LANES)] = jnp.zeros((2 * half, LANES), whole.dtype)

        span(first // 2 * 2, first, one)

    loop(groups, clear)

    def produce(g):
        @pl.when(lax.rem(g, chunk) == 0)
        def _():
            for source in range(n_cons):

                @pl.when(c != source)
                def _():
                    there_copy(0, g // chunk, source).wait_recv()

        table_copy(g).wait()
        lists = [
            jnp.concatenate([taken[source, g, fold] for source in range(n_cons)], axis=0) for fold in range(folds)
        ]
        gathered = jnp.concatenate(lists, axis=1)
        ordered = jnp.dot(order[...], gathered, preferred_element_type=jnp.float32)
        for m in range(GROUP):
            spread_s[pl.ds(m * all_rows, all_rows), :] = jnp.where(lane == m, ordered, 0.0).astype(spread_s.dtype)

        def one(lp):
            values = table[g, :, :, lane_pair(lp)].reshape(cycles * GROUP, 2 * LANES)
            part[g, :, lane_pair(lp)] = jnp.dot(
                spread_s[...], values, preferred_element_type=jnp.float32
            ).astype(part.dtype)

        span(first_of(g) // 2, pairs, one)

        @pl.when(plan.merged(c, g))
        def _():
            here = pl.ds(pl.multiple_of(first_of(g) * LANES, LANES), LANES)
            moved = LANES - GROUP * plan.turn(c, g)
            lanes = lax.broadcasted_iota(jnp.int32, (2 * half, LANES), 1)
            low = pltpu.roll(part[g, :, here].astype(jnp.float32), moved, 1)
            high = part[plan.mate(c, g), :, here].astype(jnp.float32)
            part[g, :, here] = jnp.where(lanes < moved, low, high).astype(part.dtype)

        span(start_of(g), start_of(g + 1), lambda t: pair_copy(t, plan.place(c, listed, t)).start())

    width = folds * LANES
    order_lane = lax.broadcasted_iota(jnp.int32, (rows, LANES), 1) % GROUP

    def restore(g):
        def take(t):
            fin_copy(t, corner).wait_recv()

        span(start_of(g), start_of(g + 1), take)
        joined = plan.merged(c, g)

        @pl.when(joined)
        def _():
            here = pl.ds(pl.multiple_of(first_of(g) * LANES, LANES), LANES)
            fin_copy(start_of(g), corner).wait_send()
            both = whole[g, :, here]
            whole[plan.mate(c, g), :, here] = both
            back_by = GROUP * plan.turn(c, g)
            whole[g, :, here] = pltpu.roll(both.astype(jnp.float32), back_by, 1).astype(whole.dtype)

        count = jnp.where(plan.lost(c, g), 0, jnp.where(joined, 2, 1))
        span(0, count, lambda n: synthesise(jnp.where(n == 0, g, plan.mate(c, g))))

    def synthesise(g):
        def one(lp, total):
            values = table[g, :, :, lane_pair(lp)].reshape(cycles * GROUP, 2 * LANES)
            full = lax.dot_general(
                whole[g, :, lane_pair(lp)], values, (((1,), (1,)), ((), ())), preferred_element_type=jnp.float32
            )
            wide = lax.broadcasted_iota(jnp.int32, (all_rows, width), 1) % GROUP
            for m in range(GROUP):
                total = total + jnp.where(wide == m, full[m * all_rows : (m + 1) * all_rows], 0.0)
            return total

        total = lax.fori_loop(first_of(g) // 2, pairs, one, jnp.zeros((all_rows, width), jnp.float32))
        zero_order = (c * groups + g) * GROUP + order_lane == 0
        factor = jnp.where(zero_order, 1.0, 2.0)
        for peer in range(n_cons):
            for fold in range(folds):
                piece = total[peer * rows : (peer + 1) * rows, fold * LANES : (fold + 1) * LANES]
                back[g, peer, fold] = (piece * factor).astype(back.dtype)
        for k in range(n_cons - 1):
            home_copy(k, g, c).start()
        returned[c * groups + g] = back[g, c]

    def give(e):
        spot = plan.place(c, listed, 2 * e)
        pair_copy(2 * e, spot).wait_recv()
        given[e] = add(at(part, spot, mine)[...], pair_in[2 * e]).astype(given.dtype)
        give_copy(e).start()

    def gather(q):
        native = jnp.logical_not(is_import(q))

        @pl.when(native)
        def _():
            t = tile_of(q)
            spot = plan.place(c, listed, t)
            pair_copy(t, spot).wait_recv()
            acc[q] = add(at(part, spot, mine)[...], pair_in[t]).astype(acc.dtype)

        @pl.when(is_import(q))
        def _():
            give_copy(q - LEAD).wait_recv()

        @pl.when(depth < last)
        def _():
            in_copy(q).wait_recv()
            acc[q] = add(acc[q], inward_in[q]).astype(acc.dtype)

        @pl.when(depth > 0)
        def _():
            in_copy(q).start()

        @pl.when((depth == 0) & (lax.rem(q, 2) != side))
        def _():
            cross_copy(q).start()

    def spread(q):
        @pl.when(depth < last)
        def _():
            out_copy(q).start()

        @pl.when(is_import(q))
        def _():
            e = q - LEAD
            ret_copy(q, e, plan.place(other_c, other_starts, 2 * e)).start()

        @pl.when(jnp.logical_not(is_import(q)))
        def _():
            t = tile_of(q)
            spot = plan.place(c, listed, t)
            at(whole, spot, mine)[...] = coef[q]
            fin_copy(t, spot).start()

    def finish(q):
        @pl.when((depth == 0) & (lax.rem(q, 2) == side))
        def _():
            cross_copy(q).wait_recv()
            own = plan.place(c, listed, tile_of(q))
            lent = plan.place(other_c, other_starts, 2 * (q - LEAD))
            lt = jnp.where(is_import(q), lent[1], own[1])
            moved = jnp.where(is_import(q), plan.shift(other_c, lent), plan.shift(c, own))
            scale = jnp.broadcast_to(love[pl.ds(lt, 1), :], (8, LANES))
            ahead_of = lax.broadcasted_iota(jnp.int32, (8, LANES), 1) < moved
            scale = jnp.where(ahead_of, pltpu.roll(scale, moved, 1), scale)[:1]
            total = add(acc[q], cross_in[q // 2]) * scale
            coef[q] = total.astype(coef.dtype)
            mid_copy(q).start()
            spread(q)

    def relay(q):
        @pl.when((depth > 0) | (lax.rem(q, 2) != side))
        def _():
            out_copy(q).wait_recv()
            spread(q)

    def take_back(e):
        spot = plan.place(c, listed, 2 * e)
        ret_copy(0, e, spot).wait_recv()
        fin_copy(2 * e, spot).start()

    relay_gap = jnp.where(depth == 0, REL0, REL1 + (depth - 1) * RELN)
    back_gap = LEAD + relay_gap + BACK

    def ready(g):
        t = start_of(g + 1) - 1
        q = jnp.where(t < 2 * exports, t // 2, t - exports) + jnp.where(t >= LEAD, imports, 0)
        e = jnp.where(start_of(g) < 2 * exports, jnp.minimum(t // 2, exports - 1) + back_gap, 0)
        return jnp.maximum(q + relay_gap, e) + SLACK

    fine_rows = fine.shape[1]
    wave_blocks = waves.shape[1] // fine_rows

    def wave_copy(b):
        rows_here = pl.ds(pl.multiple_of(b * fine_rows, fine_rows), fine_rows)
        return pltpu.make_async_copy(waves.at[:, rows_here, :], wave.at[:, rows_here, :], wave_sem.at[b])

    def turn(row):
        lon = lax.broadcasted_iota(jnp.int32, row.shape, 1).astype(jnp.float32)
        return circle(row.astype(jnp.float32) * lon)

    def make_fine():
        fine[0], fine[1] = turn(lax.broadcasted_iota(jnp.int32, (fine_rows, quarter), 0))

    def make_wave(b):
        cos_a, sin_a = turn(jnp.full((8, quarter), b * fine_rows, jnp.int32))
        cos_a, sin_a = cos_a[:1], sin_a[:1]
        here = pl.ds(pl.multiple_of(b * fine_rows, fine_rows), fine_rows)
        waves[0, here, :] = (cos_a * fine[0] - sin_a * fine[1]).astype(waves.dtype)
        waves[1, here, :] = (-sin_a * fine[0] - cos_a * fine[1]).astype(waves.dtype)
        wave_copy(b).start()

    for g in range(AHEAD):
        produce(g)

    def step(i, done):
        @pl.when(i < exports)
        def _():
            give(i)

        @pl.when(i < queue)
        def _():
            gather(i)

        q = i - FIN

        @pl.when((q >= 0) & (q < queue))
        def _():
            finish(q)

        r = i - relay_gap

        @pl.when((r >= 0) & (r < queue))
        def _():
            relay(r)

        e = i - back_gap

        @pl.when((e >= 0) & (e < exports))
        def _():
            take_back(e)

        for h in range(EARLY, CHUNKS):

            @pl.when(i == CHUNK_AT + (h - EARLY) * CHUNK_EVERY)
            def _(h=h):
                send_chunk(h)

        @pl.when(i == WAVE_AT)
        def _():
            make_fine()

        b = i - WAVE_AT - 1

        @pl.when((b >= 0) & (b < wave_blocks))
        def _():
            make_wave(b)

        ahead = AHEAD + i // PACE

        @pl.when((lax.rem(i, PACE) == 0) & (ahead < groups))
        def _():
            produce(ahead)

        now = (done < groups) & (i >= ready(done)) & ((lax.rem(i, PACE) > 0) | (i > PACE * groups))

        @pl.when(now)
        def _():
            restore(done)

        return done + jnp.where(now, 1, 0)

    count = plan.max_queue + LEAD + REL1 + mid * RELN + BACK
    done = lax.fori_loop(0, count, step, 0)
    span(done, groups, restore)

    def drain_tile(t):
        pair_copy(t, corner).wait_send()

    loop(tiles, drain_tile)

    def drain_group(g):
        begin = start_of(g) + jnp.where(plan.merged(c, g), 1, 0)
        span(begin, start_of(g + 1), lambda t: fin_copy(t, corner).wait_send())

    loop(groups, drain_group)
    loop(exports, lambda e: give_copy(e).wait_send())

    def drain_queue(q):
        @pl.when(depth > 0)
        def _():
            in_copy(q).wait_send()

        @pl.when((depth == 0) & (lax.rem(q, 2) != side))
        def _():
            cross_copy(q).wait_send()

        @pl.when((depth == 0) & (lax.rem(q, 2) == side))
        def _():
            mid_copy(q).wait_send()

        @pl.when(depth < last)
        def _():
            out_copy(q).wait_send()

        @pl.when(is_import(q))
        def _():
            e = q - LEAD
            ret_copy(q, e, corner).wait_send()

    loop(queue, drain_queue)
    loop(wave_blocks, lambda b: wave_copy(b).wait())
    for k in range(n_cons - 1):
        for h in range(CHUNKS):
            there_copy(k, h, c).wait_send()

        loop(groups, lambda g, k=k: home_copy(k, g, c).wait_send())

    def tile_rows(tile):
        return pl.ds(pl.multiple_of(tile * cycles * rows, 8), cycles * rows)

    def y_copy(tile):
        return pltpu.make_async_copy(out.at[tile_rows(tile), :], y.at[tile_rows(tile), :], out_sem.at[tile])

    def unpack(tile):
        def heard_from(k):
            index = tile * blocks + k

            @pl.when(index // groups != c)
            def _():
                home_copy(0, lax.rem(index, groups), index // groups).wait_recv()

        loop(blocks, heard_from)

        swapped = swap_blocks([returned[tile * blocks + k].astype(jnp.float32) for k in range(blocks)])
        merged = jnp.stack(swapped, axis=1).reshape(cycles * rows, LANES)
        out[tile_rows(tile), :] = merged
        y_copy(tile).start()

    latest = [max(k % groups for k in range(t * blocks, (t + 1) * blocks)) for t in range(order_tiles)]
    turns = sorted(range(order_tiles), key=lambda t: latest[t])
    loop(order_tiles, lambda n: unpack(pick(n, turns)))
    loop(order_tiles, lambda t: y_copy(t).wait())


def exchange(elevation, weight, assignment, love, legendre, n_cons, n_blk):
    cycles, orders_dev, degrees = legendre.shape
    fields, _, longitudes = elevation.shape
    quarter, rows = longitudes // 4, 2 * fields
    all_rows, orders = n_cons * rows, n_cons * orders_dev
    plan = Plan(n_cons, n_blk, orders_dev, degrees)
    groups, folds = plan.groups, cycles * GROUP // LANES
    half = (GROUP * all_rows // 2, LANES)
    kind = elevation.dtype
    tiles, queue, moved = plan.max_tiles, plan.max_queue, plan.max_moved
    halves = (queue + 1) // 2
    sems = [(n,) for n in [tiles] * 2 + [moved] * 2 + [queue] * 2 + [halves] * 2 + [halves, queue, queue] + [moved] * 2 + [tiles] * 2]
    sems += [(n_cons - 1, CHUNKS), (n_cons, CHUNKS), (n_cons - 1, groups), (n_cons * groups,)]
    lane_tiles = (folds, rows, LANES)
    waves = (2, orders, quarter)
    chunk_lanes = orders // CHUNKS
    vmem = pl.BlockSpec(memory_space=pltpu.VMEM)
    scalars = pl.BlockSpec(memory_space=pltpu.SMEM)
    anywhere = pl.BlockSpec(memory_space=pl.ANY)
    return pl.pallas_call(
        functools.partial(sum_kernel, plan),
        out_shape=[
            jax.ShapeDtypeStruct((orders // LANES * cycles * rows, LANES), jnp.float32),
            jax.ShapeDtypeStruct(waves, kind),
        ],
        in_specs=[anywhere, scalars, scalars, vmem, anywhere],
        out_specs=[anywhere, anywhere],
        scratch_shapes=[
            pltpu.VMEM((groups, cycles, GROUP, degrees), kind),
            pltpu.SemaphoreType.DMA((groups,)),
            pltpu.VMEM((groups, GROUP * all_rows, degrees), kind),
            pltpu.VMEM((GROUP * all_rows, folds * LANES), kind),
            pltpu.VMEM((groups, GROUP * all_rows, degrees), kind),
            pltpu.VMEM((n_cons * groups,) + lane_tiles, kind),
            pltpu.VMEM((n_cons, groups) + lane_tiles, kind),
            pltpu.VMEM((groups, n_cons) + lane_tiles, kind),
            pltpu.VMEM((n_cons * groups,) + lane_tiles, kind),
            pltpu.VMEM((tiles,) + half, kind),
            pltpu.VMEM((queue,) + half, kind),
            pltpu.VMEM((moved,) + half, kind),
            pltpu.VMEM((queue,) + half, kind),
            pltpu.VMEM((halves,) + half, kind),
            pltpu.VMEM((queue,) + half, kind),
            pltpu.VMEM((2, FINE, quarter), jnp.float32),
            pltpu.VMEM(waves, kind),
            pltpu.SemaphoreType.DMA((waves[1] // FINE,)),
            pltpu.VMEM((orders // LANES * cycles * rows, LANES), jnp.float32),
            pltpu.SemaphoreType.DMA((orders // LANES,)),
            pltpu.SemaphoreType.DMA((longitudes // degrees,)),
            pltpu.VMEM((2, quarter // FINE, chunk_lanes), jnp.float32),
            pltpu.VMEM((2, FINE, chunk_lanes), jnp.float32),
            pltpu.VMEM((quarter, 2 * chunk_lanes), kind),
            pltpu.VMEM((cycles, LANES), jnp.float32),
            pltpu.VMEM((all_rows, all_rows), kind),
            pltpu.VMEM((chunk_lanes // LANES, cycles * rows, LANES), jnp.float32),
        ]
        + [pltpu.SemaphoreType.DMA(n) for n in sems],
        compiler_params=pltpu.CompilerParams(
            collective_id=0, has_side_effects=True, vmem_limit_bytes=VMEM_MIB * 2**20
        ),
    )(
        elevation.reshape(fields * cycles, longitudes),
        weight,
        assignment,
        love.reshape(degrees // LANES, LANES),
        legendre,
    )


def inverse_kernel(given, wave, loading, y, lhs, held, result, y_sem, wave_sem, out_sem):
    fields, cycles, longitudes = loading.shape
    quarter, tiles = longitudes // 4, lhs.shape[1] // LANES
    width, parts = held.shape[3], held.shape[0]
    rows = 2 * fields

    def columns(n):
        return pl.ds(pl.multiple_of(n * width, width), width)

    def wave_copy(n):
        return pltpu.make_async_copy(wave.at[:, :, columns(n)], held.at[n], wave_sem.at[n])

    def out_copy(n, q):
        place = pl.ds(pl.multiple_of(q * quarter + n * width, width), width)
        return pltpu.make_async_copy(
            result.at[n, pl.ds(q * fields, fields)], loading.at[:, :, place], out_sem.at[n, q]
        )

    def y_copy(tile):
        here = pl.ds(tile * cycles * rows, cycles * rows)
        return pltpu.make_async_copy(given.at[here, :], y.at[here, :], y_sem.at[tile])

    for tile in range(tiles // 2):
        y_copy(tile).start()
    for n in range(parts):
        wave_copy(n).start()
    residue = lax.broadcasted_iota(jnp.int32, (2 * cycles, LANES), 1) % 4
    turn_re = jnp.where(residue == 0, 1.0, jnp.where(residue == 2, -1.0, 0.0))
    turn_im = jnp.where(residue == 1, 1.0, jnp.where(residue == 3, -1.0, 0.0))
    sign = turn_re * turn_re - turn_im * turn_im
    orders = tiles * LANES // 2
    for tile in range(tiles // 2):
        y_copy(tile).wait()

        def load(piece, pair):
            at = [tile * cycles * rows + piece * fields + 2 * pair + k for k in range(2)]
            return jnp.concatenate([y[pl.ds(a, cycles, stride=rows), :] for a in at], axis=0)

        for pair in range(fields // 2):
            re, im = load(0, pair), load(1, pair)
            turned = (
                (re, im),
                (turn_re * re - turn_im * im, turn_re * im + turn_im * re),
                (sign * re, sign * im),
                (turn_re * re + turn_im * im, turn_re * im - turn_im * re),
            )
            for q in range(4):
                here = pl.ds((q * (fields // 2) + pair) * 2 * cycles, 2 * cycles)
                for piece in range(2):
                    lanes = pl.ds(piece * orders + tile * LANES, LANES)
                    lhs[here, lanes] = turned[q][piece].astype(lhs.dtype)

    def one(n, carry):
        wave_copy(n).wait()
        table = held[n].reshape(2 * orders, width)
        product = jnp.dot(lhs[...], table, preferred_element_type=jnp.float32)
        result[n] = product.reshape(4 * fields, cycles, width)
        for q in range(4):
            out_copy(n, q).start()
        return carry

    lax.fori_loop(0, parts, one, 0)
    for n in range(parts):
        for q in range(4):
            out_copy(n, q).wait()


def inverse(y, wave, fields, cycles):
    orders, quarter = wave.shape[1:]
    width = WIDE * LANES
    parts = quarter // width
    anywhere = pl.BlockSpec(memory_space=pl.ANY)
    return pl.pallas_call(
        inverse_kernel,
        out_shape=jax.ShapeDtypeStruct((fields, cycles, 4 * quarter), jnp.float32),
        in_specs=[anywhere, anywhere],
        out_specs=anywhere,
        scratch_shapes=[
            pltpu.VMEM(y.shape, jnp.float32),
            pltpu.VMEM((4 * fields * cycles, 2 * orders), jnp.bfloat16),
            pltpu.VMEM((parts, 2, orders, width), jnp.bfloat16),
            pltpu.VMEM((parts, 4 * fields, cycles, width), jnp.float32),
            pltpu.SemaphoreType.DMA((orders // LANES,)),
            pltpu.SemaphoreType.DMA((parts,)),
            pltpu.SemaphoreType.DMA((parts, 4)),
        ],
        compiler_params=pltpu.CompilerParams(vmem_limit_bytes=60 * 2**20),
    )(y, wave)


def local(elevation, legendre, cycle_weight, love_factor, assignment):
    n_cons, n_blk = lax.axis_size("cons"), lax.axis_size("blk")
    y, wave = exchange(elevation, cycle_weight, assignment, love_factor, legendre, n_cons, n_blk)
    return inverse(y, wave, *elevation.shape[:2])


def solution(mesh):
    placed = (P("cons", "blk", None), P("blk", "cons", None), P("blk"), P(), P())
    return jax.shard_map(
        local, mesh=mesh, in_specs=placed, out_specs=P("cons", "blk", None), check_vma=False
    )
```
